8 devices in a mesh: dp: 1 (over z), tp: 2 (over y), ep: 4 (over x, core).
Axes of the slice: x: 2, y: 2, z: 1, core: 2. Of those that a mesh axis runs over, the one named last changes fastest.
Arguments:
- tokens: bfloat16 [1024, 1536], P(('dp', 'ep', 'tp'))
- expert_ids: int32 [1024, 4], P(('dp', 'ep', 'tp'))
- gate_vals: float32 [1024, 4], P(('dp', 'ep', 'tp'))
- w_one: bfloat16 [32, 1536, 768], P('ep', None, 'tp')
- w_three: bfloat16 [32, 1536, 768], P('ep', None, 'tp')
- w_two: bfloat16 [32, 768, 1536], P('ep', 'tp')
- d_out: bfloat16 [1024, 1536], P(('dp', 'ep', 'tp'))
Outputs:
- output 1: bfloat16 [1024, 1536], P(('dp', 'ep', 'tp'))
- output 2: bfloat16 [1024, 1536], P(('dp', 'ep', 'tp'))
- output 3: bfloat16 [32, 1536, 768], P(('dp', 'ep'), None, 'tp')
- output 4: bfloat16 [32, 1536, 768], P(('dp', 'ep'), None, 'tp')
- output 5: bfloat16 [32, 768, 1536], P(('dp', 'ep'), 'tp')
All inputs are finite; a program needn't handle non-finite values.
Results may differ from the reference program's by a relative error of at most 0.00857034.
Values are sent between devices in bfloat16 or wider.
A program may use at most 1 GiB of HBM per device.

```python
import math
import jax
import jax.numpy as jnp
from jax import lax

D = 1536
FF = 768
EXPERTS = 32
TOP = 4
TOK = 128
CAP = 24
BLOCKS = 8
TOKENS = TOK * BLOCKS


def draw_routes(route_key):
    score_key, hot_key = jax.random.split(route_key)
    score_span = 2 ** 20
    bonus_size = 2 ** 29
    scores = jax.random.randint(score_key, (BLOCKS, TOK, EXPERTS), 0, score_span, dtype=jnp.int32) * EXPERTS + jnp.arange(EXPERTS, dtype=jnp.int32)
    hot_ids = jax.random.randint(hot_key, (BLOCKS, 1, 1), 0, EXPERTS, dtype=jnp.int32)
    hot_rows = CAP + CAP // 16 + 1
    is_hot = jnp.arange(EXPERTS, dtype=jnp.int32)[None, None, :] == hot_ids
    lead_rows = (jnp.arange(TOK, dtype=jnp.int32) < hot_rows)[None, :, None]
    bonus = jnp.where(is_hot, jnp.where(lead_rows, bonus_size, -bonus_size), 0)
    chosen = lax.top_k(scores + bonus, TOP)[1]
    return chosen.astype(jnp.int32).reshape(BLOCKS * TOK, TOP)


def setup_inputs(seed: int = 0, part: int = 0) -> dict:
    base_key = jax.random.key(seed)
    key_one, key_three, key_two = jax.random.split(jax.random.fold_in(base_key, 1), 3)
    part_key = jax.random.fold_in(jax.random.fold_in(base_key, 2), part)
    key_tok, key_route, key_gate, key_grad = jax.random.split(part_key, 4)
    tokens = jax.random.normal(key_tok, (TOKENS, D), jnp.float32).astype(jnp.bfloat16)
    expert_ids = draw_routes(key_route)
    gate_vals = jax.random.uniform(key_gate, (TOKENS, TOP), jnp.float32, 0.5, 1.5) / math.sqrt(TOP)
    in_scale = D ** -0.5
    mid_scale = FF ** -0.5
    w_one = (jax.random.normal(key_one, (EXPERTS, D, FF), jnp.float32) * in_scale).astype(jnp.bfloat16)
    w_three = (jax.random.normal(key_three, (EXPERTS, D, FF), jnp.float32) * in_scale).astype(jnp.bfloat16)
    w_two = (jax.random.normal(key_two, (EXPERTS, FF, D), jnp.float32) * mid_scale).astype(jnp.bfloat16)
    d_out = jax.random.normal(key_grad, (TOKENS, D), jnp.float32).astype(jnp.bfloat16)
    return {"tokens": tokens, "expert_ids": expert_ids, "gate_vals": gate_vals, "w_one": w_one, "w_three": w_three, "w_two": w_two, "d_out": d_out}


def route_tables(block_ids):
    hit_mask = block_ids[:, :, None] == jnp.arange(EXPERTS, dtype=jnp.int32)
    per_row = jnp.sum(hit_mask, axis=1, dtype=jnp.int32)
    before = jnp.cumsum(per_row, axis=0) - per_row
    slot_pos = jnp.sum(jnp.where(hit_mask, before[:, None, :], 0), axis=2)
    copy_slot = jnp.where(slot_pos < CAP, block_ids * CAP + slot_pos, EXPERTS * CAP)
    slot_copy = jnp.full((EXPERTS * CAP,), TOK * TOP, jnp.int32)
    slot_copy = slot_copy.at[copy_slot.reshape(-1)].set(jnp.arange(TOK * TOP, dtype=jnp.int32), mode="drop")
    return slot_copy, copy_slot


def take_rows(source, index_list):
    return jnp.take(source, index_list, axis=0, mode="fill", fill_value=0)


def by_expert(slot_rows):
    return slot_rows.reshape(BLOCKS, EXPERTS, CAP, D).transpose(1, 0, 2, 3).reshape(EXPERTS, BLOCKS * CAP, D)


def by_block(expert_rows):
    return expert_rows.reshape(EXPERTS, BLOCKS, CAP, D).transpose(1, 0, 2, 3).reshape(BLOCKS, EXPERTS * CAP, D)


def expert_pass(operands):
    slot_in, slot_grad, w_a, w_b, w_c = operands
    act_one = jnp.dot(slot_in, w_a, preferred_element_type=jnp.float32)
    act_three = jnp.dot(slot_in, w_b, preferred_element_type=jnp.float32)
    sig_one = jax.nn.sigmoid(act_one)
    silu_one = act_one * sig_one
    hidden = (silu_one * act_three).astype(jnp.bfloat16)
    slot_out = jnp.dot(hidden, w_c, preferred_element_type=jnp.float32).astype(jnp.bfloat16)
    d_hidden = jnp.dot(slot_grad, w_c.T, preferred_element_type=jnp.float32)
    grad_c = jnp.dot(hidden.T, slot_grad, preferred_element_type=jnp.float32).astype(jnp.bfloat16)
    d_one = (d_hidden * act_three * sig_one * (1.0 + act_one * (1.0 - sig_one))).astype(jnp.bfloat16)
    d_three = (d_hidden * silu_one).astype(jnp.bfloat16)
    grad_a = jnp.dot(slot_in.T, d_one, preferred_element_type=jnp.float32).astype(jnp.bfloat16)
    grad_b = jnp.dot(slot_in.T, d_three, preferred_element_type=jnp.float32).astype(jnp.bfloat16)
    slot_dx = (jnp.dot(d_one, w_a.T, preferred_element_type=jnp.float32) + jnp.dot(d_three, w_b.T, preferred_element_type=jnp.float32)).astype(jnp.bfloat16)
    return slot_out, slot_dx, grad_a, grad_b, grad_c


def reference(tokens, expert_ids, gate_vals, w_one, w_three, w_two, d_out):
    slot_copy, copy_slot = jax.vmap(route_tables)(expert_ids.reshape(BLOCKS, TOK, TOP))
    gather_rows = jax.vmap(take_rows)
    slot_in = gather_rows(tokens.reshape(BLOCKS, TOK, D), slot_copy // TOP)
    grad_copies = (gate_vals[:, :, None] * d_out.astype(jnp.float32)[:, None, :]).astype(jnp.bfloat16)
    slot_grad = gather_rows(grad_copies.reshape(BLOCKS, TOK * TOP, D), slot_copy)
    slot_out, slot_dx, grad_one, grad_three, grad_two = lax.map(expert_pass, (by_expert(slot_in), by_expert(slot_grad), w_one, w_three, w_two))
    out_copies = gather_rows(by_block(slot_out), copy_slot)
    block_gates = gate_vals.reshape(BLOCKS, TOK, TOP)
    out_rows = jnp.sum(block_gates[:, :, :, None] * out_copies.astype(jnp.float32), axis=2).astype(jnp.bfloat16)
    dx_copies = gather_rows(by_block(slot_dx), copy_slot)
    dx_rows = jnp.sum(dx_copies.astype(jnp.float32), axis=2).astype(jnp.bfloat16)
    return out_rows.reshape(TOKENS, D), dx_rows.reshape(TOKENS, D), grad_one, grad_three, grad_two
```

```python
import functools

import jax
import jax.numpy as jnp
from jax import lax
from jax.experimental import pallas as pl
from jax.experimental.pallas import tpu as pltpu
from jax.sharding import PartitionSpec as P

BF = jnp.bfloat16
F32 = jnp.float32


def slot_count(num_top, tok_dev, experts):
    return 8 * ((5 * num_top * tok_dev + 32 * experts - 1) // (32 * experts))


def dot(a, b, ca, cb):
    return lax.dot_general(a, b, (((ca,), (cb,)), ((), ())), preferred_element_type=F32)


def fwd_kernel(half, x_ref, w1_ref, w3_ref, w2_ref, a_ref, b_ref, h_ref, yo_ref, ym_ref):
    x = x_ref[0]
    a = dot(x, w1_ref[0], 1, 0)
    b = dot(x, w3_ref[0], 1, 0)
    h = (a * jax.nn.sigmoid(a) * b).astype(BF)
    a_ref[0] = a
    b_ref[0] = b
    h_ref[0] = h
    y = dot(h, w2_ref[0], 1, 0)
    yo_ref[0] = y[:half]
    ym_ref[0] = y[half:]


def bwd_kernel(half, u_ref, w1_ref, w3_ref, w2_ref, a_ref, b_ref, da_ref, db_ref, vo_ref, vm_ref):
    dh = dot(u_ref[0], w2_ref[0], 1, 1)
    a = a_ref[0]
    s = jax.nn.sigmoid(a)
    da = (dh * b_ref[0] * s * (1.0 + a * (1.0 - s))).astype(BF)
    db = (dh * (a * s)).astype(BF)
    da_ref[0] = da
    db_ref[0] = db
    v = dot(da, w1_ref[0], 1, 1) + dot(db, w3_ref[0], 1, 1)
    vo_ref[0] = v[:half]
    vm_ref[0] = v[half:]


def grad_kernel(x_ref, u_ref, h_ref, da_ref, db_ref, g1_ref, g3_ref, g2_ref):
    x = x_ref[0]
    g1_ref[0] = dot(x, da_ref[0], 0, 0).astype(BF)
    g3_ref[0] = dot(x, db_ref[0], 0, 0).astype(BF)
    g2_ref[0] = dot(h_ref[0], u_ref[0], 0, 0).astype(BF)


def spec(shape, first):
    return pl.BlockSpec((1,) + shape, lambda i: (i + first, 0, 0))


def cost(flops, nbytes):
    return pl.CostEstimate(flops=flops, bytes_accessed=nbytes, transcendentals=0)


PARAMS = pltpu.CompilerParams(dimension_semantics=("arbitrary",), vmem_limit_bytes=48 * 2**20)


def fwd_call(first, count, xs, w1, w3, w2):
    rows, d, f = xs.shape[1], w1.shape[1], w1.shape[2]
    half = rows // 2
    outs = [((rows, f), F32), ((rows, f), F32), ((rows, f), BF), ((half, d), F32), ((half, d), F32)]
    return pl.pallas_call(
        functools.partial(fwd_kernel, half), grid=(count,), name=f"fwd{first}",
        in_specs=[spec((rows, d), first), spec((d, f), first), spec((d, f), first), spec((f, d), first)],
        out_specs=[spec(s, 0) for s, _ in outs],
        out_shape=[jax.ShapeDtypeStruct((count,) + s, t) for s, t in outs],
        compiler_params=PARAMS, cost_estimate=cost(count * 6 * rows * d * f, count * (6 * d * f + 6 * rows * d)),
    )(xs, w1, w3, w2)


def bwd_call(first, count, us, w1, w3, w2, a, b):
    rows, d, f = us.shape[1], w1.shape[1], w1.shape[2]
    half = rows // 2
    outs = [((rows, f), BF), ((rows, f), BF), ((half, d), F32), ((half, d), F32)]
    return pl.pallas_call(
        functools.partial(bwd_kernel, half), grid=(count,), name=f"bwd{first}",
        in_specs=[spec((rows, d), first), spec((d, f), first), spec((d, f), first), spec((f, d), first),
                  spec((rows, f), 0), spec((rows, f), 0)],
        out_specs=[spec(s, 0) for s, _ in outs],
        out_shape=[jax.ShapeDtypeStruct((count,) + s, t) for s, t in outs],
        compiler_params=PARAMS, cost_estimate=cost(count * 6 * rows * d * f, count * (6 * d * f + 6 * rows * d)),
    )(us, w1, w3, w2, a, b)


def grad_call(xs, us, h, da, db):
    count, rows, d = xs.shape
    f = h.shape[2]
    outs = [((d, f), BF), ((d, f), BF), ((f, d), BF)]
    return pl.pallas_call(
        grad_kernel, grid=(count,), name="wgrad",
        in_specs=[spec((rows, d), 0), spec((rows, d), 0)] + [spec((rows, f), 0)] * 3,
        out_specs=[spec(s, 0) for s, _ in outs],
        out_shape=[jax.ShapeDtypeStruct((count,) + s, t) for s, t in outs],
        compiler_params=PARAMS, cost_estimate=cost(count * 6 * rows * d * f, count * (6 * d * f + 4 * rows * d)),
    )(xs, us, h, da, db)


def solution(mesh):
    tp_size, ep_size = mesh.shape["tp"], mesh.shape["ep"]
    row_spec = P(("dp", "ep", "tp"), None)
    col_spec = P("ep", None, "tp")
    down_spec = P("ep", "tp", None)
    grad_col = P(("dp", "ep"), None, "tp")
    grad_down = P(("dp", "ep"), "tp", None)

    def swap(z, tp_bit, ep_bits):
        pairs = [(t * ep_size + e, (t ^ tp_bit) * ep_size + (e ^ ep_bits)) for t in range(tp_size) for e in range(ep_size)]
        return lax.ppermute(z, ("tp", "ep"), pairs)

    def gather_all(z):
        zy, zd, zx = swap(z, 1, 0), swap(z, 1, 2), swap(z, 0, 2)
        mine = jnp.stack([zy, zd, z, zx])
        core = swap(mine, 0, 1)
        return jnp.stack([zy, zd, core[0], core[1], z, zx, core[2], core[3]])

    def local_step(tokens, expert_ids, gate_vals, w_one, w_three, w_two, d_out):
        tok_dev, width = tokens.shape
        num_top = expert_ids.shape[1]
        local = w_one.shape[0]
        experts = local * ep_size
        slot_cap = slot_count(num_top, tok_dev, experts)
        blocks = tp_size * ep_size
        rows = blocks * slot_cap
        ep_here = lax.axis_index("ep")

        aux = jnp.concatenate([expert_ids.astype(F32), gate_vals], axis=1)
        aux_all = gather_all(aux)
        tok_all = gather_all(tokens)
        dout_all = gather_all(d_out)

        lower = (jnp.arange(tok_dev)[:, None] > jnp.arange(tok_dev)[None, :]).astype(BF)

        def keys(aux_in, ids):
            eq = aux_in[..., :num_top, None] == ids.astype(F32)
            hit = jnp.any(eq, axis=-2)
            pos = jnp.einsum("ts,bse->bte", lower, hit.astype(BF), preferred_element_type=F32)
            gate = jnp.sum(jnp.where(eq, aux_in[..., num_top:, None], 0.0), axis=-2)
            return jnp.where(hit & (pos < slot_cap), pos, -1.0), gate

        key, gate = keys(aux_all, ep_here * local + jnp.arange(local))
        shift = (slot_cap * jnp.arange(blocks, dtype=F32))[:, None, None]
        row_key = jnp.where(key >= 0, key + shift, -1.0)
        row_key = row_key.transpose(2, 0, 1).reshape(local, 1, blocks * tok_dev)
        gate_e = gate.transpose(2, 0, 1).reshape(local, 1, blocks * tok_dev)
        pick = row_key == jnp.arange(rows, dtype=F32)[None, :, None]
        slot_gate = jnp.sum(jnp.where(pick, gate_e, 0.0), axis=2)
        pick = pick.astype(BF).reshape(local * rows, blocks * tok_dev)
        xs = jnp.dot(pick, tok_all.reshape(-1, width), preferred_element_type=F32).astype(BF).reshape(local, rows, width)

        chunks = 4
        count = local // chunks
        fwd = [fwd_call(c * count, count, xs, w_one, w_three, w_two) for c in range(chunks)]
        y_recv = [swap(f[3], 1, 0) for f in fwd]

        us = jnp.dot(pick, dout_all.reshape(-1, width), preferred_element_type=F32)
        us = (us.reshape(local, rows, width) * slot_gate[:, :, None]).astype(BF)
        bwd = [bwd_call(c * count, count, us, w_one, w_three, w_two, fwd[c][0], fwd[c][1]) for c in range(chunks)]
        v_recv = [swap(b[2], 1, 0) for b in bwd]

        hid = jnp.concatenate([f[2] for f in fwd])
        d_one = jnp.concatenate([b[0] for b in bwd])
        d_three = jnp.concatenate([b[1] for b in bwd])
        grads = grad_call(xs, us, hid, d_one, d_three)

        def finish(own, recv):
            done = (own + recv).astype(BF).reshape(count, ep_size, slot_cap, width)
            return [done[:, 0], swap(done[:, 1], 0, 2), swap(done[:, 2], 0, 1), swap(done[:, 3], 0, 3)]

        y_back = [finish(f[4], r) for f, r in zip(fwd, y_recv)]
        v_back = [finish(b[3], r) for b, r in zip(bwd, v_recv)]

        sources = jnp.stack([ep_here, ep_here ^ 2, ep_here ^ 1, ep_here ^ 3])
        all_ids = (sources[:, None] * local + jnp.arange(local)).reshape(-1)
        own_key, own_gate = keys(aux[None], all_ids)
        own_pick = own_key[0][:, :, None] == jnp.arange(slot_cap, dtype=F32)
        own_mul = jnp.where(own_pick, own_gate[0][:, :, None], 0.0)

        def collect(back):
            return jnp.stack([jnp.concatenate([b[s] for b in back]) for s in range(ep_size)]).reshape(-1, width)

        out_rows = jnp.dot(own_mul.reshape(tok_dev, -1), collect(y_back).astype(F32), precision=lax.Precision.HIGHEST).astype(BF)
        dx_rows = jnp.dot(own_pick.astype(BF).reshape(tok_dev, -1), collect(v_back), preferred_element_type=F32).astype(BF)
        return out_rows, dx_rows, *grads

    return jax.shard_map(local_step, mesh=mesh,
                         in_specs=(row_spec, row_spec, row_spec, col_spec, col_spec, down_spec, row_spec),
                         out_specs=(row_spec, row_spec, grad_col, grad_col, grad_down), check_vma=False)
```

```python
import functools

import jax
import jax.numpy as jnp
from jax import lax
from jax.experimental import pallas as pl
from jax.experimental.pallas import tpu as pltpu
from jax.sharding import PartitionSpec as P


BF = jnp.bfloat16
F32 = jnp.float32
MESH = pl.DeviceIdType.MESH

LEAD = 2
CAPS = (168, 448)


def slot_count(num_top, tok_dev, experts):
    return 8 * ((5 * num_top * tok_dev + 32 * experts - 1) // (32 * experts))


def dot(a, b, ca, cb):
    return lax.dot_general(a, b, (((ca,), (cb,)), ((), ())), preferred_element_type=F32)


def place(rows, keys, cap):
    pick = lax.broadcasted_iota(jnp.int32, (cap, keys.shape[1]), 0).astype(F32) == keys
    pick = jnp.where(pick, 1.0, 0.0).astype(BF)
    high = rows.astype(BF)
    rest = rows - high.astype(F32)
    mid = rest.astype(BF)
    low = (rest - mid.astype(F32)).astype(BF)
    return (dot(pick, high, 1, 0) + dot(pick, mid, 1, 0)) + dot(pick, low, 1, 0)


def put_packed(y, half, cap, key_ref, other_ref, mine_ref):
    for part, ref in ((0, other_ref), (1, mine_ref)):
        placed = place(y[part * half:(part + 1) * half], key_ref[0, part:part + 1, :], cap)

        @pl.when(pl.program_id(0) == 0)
        def _():
            ref[...] = placed

        @pl.when(pl.program_id(0) > 0)
        def _():
            ref[...] += placed


def fwd_kernel(half, cap, x_ref, w1_ref, w3_ref, w2_ref, key_ref, a_ref, b_ref, h_ref, yo_ref, ym_ref):
    x = x_ref[0]
    a = dot(x, w1_ref[0], 1, 0)
    b = dot(x, w3_ref[0], 1, 0)
    h = (a * jax.nn.sigmoid(a) * b).astype(BF)
    a_ref[0] = a
    b_ref[0] = b
    h_ref[0] = h
    put_packed(dot(h, w2_ref[0], 1, 0), half, cap, key_ref, yo_ref, ym_ref)


def bwd_kernel(half, cap, u_ref, w1_ref, w3_ref, w2_ref, key_ref, a_ref, b_ref, da_ref, db_ref, vo_ref, vm_ref):
    dh = dot(u_ref[0], w2_ref[0], 1, 1)
    a = a_ref[0]
    s = jax.nn.sigmoid(a)
    da = (dh * b_ref[0] * s * (1.0 + a * (1.0 - s))).astype(BF)
    db = (dh * (a * s)).astype(BF)
    da_ref[0] = da
    db_ref[0] = db
    put_packed(dot(da, w1_ref[0], 1, 1) + dot(db, w3_ref[0], 1, 1), half, cap, key_ref, vo_ref, vm_ref)


def finish_kernel(own_ref, recv_ref, key_ref, *out_refs):
    done = (own_ref[...] + recv_ref[...]).astype(BF)
    rows = key_ref.shape[0] // len(out_refs)
    for i, out_ref in enumerate(out_refs):
        keys = key_ref[i * rows:(i + 1) * rows, :]
        pick = lax.broadcasted_iota(jnp.int32, (rows, done.shape[0]), 1).astype(F32) == keys
        out_ref[...] = dot(jnp.where(pick, 1.0, 0.0).astype(BF), done, 1, 0).astype(BF)


def grad_kernel(x_ref, u_ref, h_ref, da_ref, db_ref, g1_ref, g3_ref, g2_ref):
    x = x_ref[0]
    g1_ref[0] = dot(x, da_ref[0], 0, 0).astype(BF)
    g3_ref[0] = dot(x, db_ref[0], 0, 0).astype(BF)
    g2_ref[0] = dot(h_ref[0], u_ref[0], 0, 0).astype(BF)


def spec(shape, first):
    return pl.BlockSpec((1,) + shape, lambda i: (i + first, 0, 0))


def whole(shape):
    return pl.BlockSpec(shape, lambda i: (0,) * len(shape))


def cost(flops, nbytes):
    return pl.CostEstimate(flops=flops, bytes_accessed=nbytes, transcendentals=0)


PARAMS = pltpu.CompilerParams(dimension_semantics=("arbitrary",), vmem_limit_bytes=48 * 2**20)


def expert_call(body, first, count, cap, rows_in, w1, w3, w2, keys, saved, kinds):
    rows, d, f = rows_in.shape[1], w1.shape[1], w1.shape[2]
    half = rows // 2
    outs = [((count, rows, f), t) for t in kinds] + [((cap, d), F32)] * 2
    return pl.pallas_call(
        functools.partial(body, half, cap), grid=(count,),
        in_specs=[spec((rows, d), first), spec((d, f), first), spec((d, f), first), spec((f, d), first),
                  spec((2, half), first)] + [spec((rows, f), 0)] * len(saved),
        out_specs=[spec(s[1:], 0) if len(s) == 3 else whole(s) for s, _ in outs],
        out_shape=[jax.ShapeDtypeStruct(s, t) for s, t in outs],
        compiler_params=PARAMS, cost_estimate=cost(count * 8 * rows * d * f, count * (6 * d * f + 6 * rows * d)),
    )(rows_in, w1, w3, w2, keys, *saved)


def grad_call(xs, us, h, da, db):
    count, rows, d = xs.shape
    f = h.shape[2]
    outs = [((d, f), BF), ((d, f), BF), ((f, d), BF)]
    return pl.pallas_call(
        grad_kernel, grid=(count,), name="wgrad",
        in_specs=[spec((rows, d), 0), spec((rows, d), 0)] + [spec((rows, f), 0)] * 3,
        out_specs=[spec(s, 0) for s, _ in outs],
        out_shape=[jax.ShapeDtypeStruct((count,) + s, t) for s, t in outs],
        compiler_params=PARAMS, cost_estimate=cost(count * 6 * rows * d * f, count * (6 * d * f + 4 * rows * d)),
    )(xs, us, h, da, db)


def finish_call(own, recv, keys, parts):
    rows, d = keys.shape[0] // parts, own.shape[1]
    return pl.pallas_call(
        finish_kernel, name="finish",
        out_shape=[jax.ShapeDtypeStruct((rows, d), BF)] * parts,
        compiler_params=pltpu.CompilerParams(vmem_limit_bytes=40 * 2**20),
        cost_estimate=cost(2 * parts * rows * d * own.shape[0], 8 * own.shape[0] * d),
    )(own, recv, keys)


ACROSS_Y, ACROSS_XY, OWN, ACROSS_X, CORE = 0, 1, 4, 5, 6
STEPS = ((1, 0), (1, 2), (1, 1), (1, 3), (0, 0), (0, 2), (0, 1), (0, 3))


def gather_kernel(slot_cap, num_top, tok_ref, aux_ref, xs_ref, key_ref, gate_ref, place_ref, aux_all_ref,
                  tok_all, aux_all, tok_send, tok_recv, aux_send, aux_recv):
    tp, ep = lax.axis_index("tp"), lax.axis_index("ep")
    eps = {0: ep, 2: lax.rem(ep + 2, 4), 1: ep + 1 - 2 * lax.rem(ep, 2), 3: 3 - ep}
    peers = [{"tp": 1 - tp if a else tp, "ep": eps[b]} for a, b in STEPS]
    others = [k for k in range(8) if k != OWN]

    barrier = pltpu.get_barrier_semaphore()
    for k in others:
        pl.semaphore_signal(barrier, inc=1, device_id=peers[k], device_id_type=MESH)
    pl.semaphore_wait(barrier, len(others))

    aux_copies = [pltpu.make_async_remote_copy(aux_ref, aux_all.at[k], aux_send.at[k], aux_recv.at[k],
                                               device_id=peers[k], device_id_type=MESH) for k in others]
    for c in aux_copies:
        c.start()

    copies = {}

    def send(source, slot, part, peer):
        c = pltpu.make_async_remote_copy(source, tok_all.at[slot, part], tok_send.at[slot, part], tok_recv.at[slot, part],
                                         device_id=peers[peer], device_id_type=MESH)
        c.start()
        copies[slot, part] = c

    def relay(slot, part):
        copies[slot, part].wait_recv()
        if slot == ACROSS_Y and part == 0:
            send(tok_all.at[slot, part], ACROSS_XY, 0, ACROSS_X)
        if slot == ACROSS_X and part == 1:
            send(tok_all.at[slot, part], ACROSS_XY, 1, ACROSS_Y)
        send(tok_all.at[slot, part], slot + 2, part, CORE)

    send(tok_ref.at[0], ACROSS_Y, 0, ACROSS_Y)
    send(tok_ref.at[1], ACROSS_X, 1, ACROSS_X)
    send(tok_ref.at[1], ACROSS_Y, 1, ACROSS_Y)
    send(tok_ref.at[0], ACROSS_X, 0, ACROSS_X)
    send(tok_ref.at[0], CORE, 0, CORE)
    send(tok_ref.at[1], CORE, 1, CORE)
    tok_all[OWN] = tok_ref[...]
    aux_all[OWN] = aux_ref[...]

    for c in aux_copies:
        c.wait_recv()
    aux_all_ref[...] = aux_all[...]
    local = key_ref.shape[1]
    width = aux_ref.shape[1]
    expert = (lax.broadcasted_iota(jnp.int32, (local, width), 0) + ep * local).astype(F32)
    hits = []
    for k in range(8):
        a = aux_all[k]
        hit, gate = jnp.zeros((local, width), F32), jnp.zeros((local, width), F32)
        for j in range(num_top):
            eq = a[j:j + 1, :] == expert
            hit = jnp.where(eq, 1.0, hit)
            gate = jnp.where(eq, a[num_top + j:num_top + j + 1, :], gate)
        hits.append(hit)
        gate_ref[k] = gate
    hit = jnp.concatenate(hits, axis=0)
    upper = lax.broadcasted_iota(jnp.int32, (width, width), 0) < lax.broadcasted_iota(jnp.int32, (width, width), 1)
    pos = dot(hit.astype(BF), jnp.where(upper, 1.0, 0.0).astype(BF), 1, 0)
    kept = jnp.where(pos < slot_cap, hit, 0.0)
    key = jnp.where(kept > 0.0, pos, -1.0)
    number = jnp.broadcast_to(jnp.sum(kept, axis=1, keepdims=True), key.shape)
    total = 8 * local
    row = lax.broadcasted_iota(jnp.int32, (total, total), 0)
    col = lax.broadcasted_iota(jnp.int32, (total, total), 1)
    rb, re, cb, ce = row // local, lax.rem(row, local), col // local, lax.rem(col, local)
    before = jnp.logical_and(rb // 4 == cb // 4, (re < LEAD) == (ce < LEAD))
    before = jnp.logical_and(before, jnp.logical_or(ce < re, jnp.logical_and(ce == re, cb < rb)))
    base = dot(jnp.where(before, 1.0, 0.0).astype(BF), number.astype(BF), 1, 0)
    lane = lax.broadcasted_iota(jnp.int32, key.shape, 1).astype(F32)
    place = jnp.where(lane < number, base + lane, -1.0)
    for k in range(8):
        key_ref[k] = key[k * local:(k + 1) * local]
        place_ref[k] = place[k * local:(k + 1) * local]

    def dispatch(first):
        one = key[first * local:(first + 1) * local]
        two = key[(first + 1) * local:(first + 2) * local]
        pair = jnp.concatenate([one, jnp.where(two >= 0.0, two + slot_cap, -1.0)], axis=1)
        slot = lax.broadcasted_iota(jnp.int32, (2 * slot_cap, 2 * width), 0).astype(F32)
        pick = jnp.concatenate([jnp.where(slot == pair[e:e + 1, :], 1.0, 0.0) for e in range(local)], axis=0).astype(BF)
        rows = dot(pick, tok_all[first:first + 2].reshape(2 * width, tok_ref.shape[2]), 1, 0).astype(BF)
        for e in range(local):
            xs_ref[e, first * slot_cap:(first + 2) * slot_cap, :] = rows[e * 2 * slot_cap:(e + 1) * 2 * slot_cap]

    relay(ACROSS_Y, 0)
    relay(ACROSS_X, 1)
    relay(ACROSS_Y, 1)
    relay(ACROSS_X, 0)
    dispatch(OWN)
    relay(ACROSS_XY, 0)
    relay(ACROSS_XY, 1)
    dispatch(ACROSS_Y)
    for slot in (CORE, CORE + 1):
        for part in (0, 1):
            copies[slot, part].wait_recv()
    dispatch(CORE)
    for slot in (2, 3):
        for part in (0, 1):
            copies[slot, part].wait_recv()
    dispatch(2)
    for c in aux_copies:
        c.wait_send()
    for c in copies.values():
        c.wait_send()


def gather_call(tokens, aux, local, slot_cap, num_top):
    tok_dev, width = tokens.shape
    tok = tokens.reshape(2, tok_dev // 2, width)
    table = jax.ShapeDtypeStruct((8, local, tok_dev), F32)
    return pl.pallas_call(
        functools.partial(gather_kernel, slot_cap, num_top), name="gather",
        in_specs=[pl.BlockSpec(memory_space=pltpu.VMEM)] * 2,
        out_specs=[pl.BlockSpec(memory_space=pltpu.VMEM)] * 5,
        out_shape=[jax.ShapeDtypeStruct((local, 8 * slot_cap, width), BF), table, table, table,
                   jax.ShapeDtypeStruct((8,) + aux.shape, F32)],
        scratch_shapes=[pltpu.VMEM((8,) + tok.shape, BF), pltpu.VMEM((8,) + aux.shape, F32),
                        pltpu.SemaphoreType.DMA((8, 2)), pltpu.SemaphoreType.DMA((8, 2)),
                        pltpu.SemaphoreType.DMA((8,)), pltpu.SemaphoreType.DMA((8,))],
        compiler_params=pltpu.CompilerParams(collective_id=0, has_side_effects=True, vmem_limit_bytes=40 * 2**20),
        cost_estimate=cost(5 * 10**9, 10**7),
    )(tok, aux)


def solution(mesh):
    tp_size, ep_size = mesh.shape["tp"], mesh.shape["ep"]
    row_spec = P(("dp", "ep", "tp"), None)
    col_spec = P("ep", None, "tp")
    down_spec = P("ep", "tp", None)
    grad_col = P(("dp", "ep"), None, "tp")
    grad_down = P(("dp", "ep"), "tp", None)

    def swap(z, tp_bit, ep_bits):
        pairs = [(t * ep_size + e, (t ^ tp_bit) * ep_size + (e ^ ep_bits)) for t in range(tp_size) for e in range(ep_size)]
        return lax.ppermute(z, ("tp", "ep"), pairs)

    def local_step(tokens, expert_ids, gate_vals, w_one, w_three, w_two, d_out):
        tok_dev, width = tokens.shape
        num_top = expert_ids.shape[1]
        local = w_one.shape[0]
        experts = local * ep_size
        slot_cap = slot_count(num_top, tok_dev, experts)
        blocks = tp_size * ep_size
        rows = blocks * slot_cap
        half = rows // 2
        ep_here = lax.axis_index("ep")

        aux = jnp.concatenate([expert_ids.astype(F32).T, gate_vals.T])
        xs, key, gate, place_all, aux_all = gather_call(tokens, aux, local, slot_cap, num_top)
        pack = place_all[:, :, :slot_cap].reshape(2, ep_size, local, slot_cap).transpose(2, 0, 1, 3).reshape(local, 2, half)

        d_here = lax.optimization_barrier((d_out, xs))[0]
        zy = swap(d_here, 1, 0)
        zx = swap(d_here, 0, 2)

        def fwd(first, count, cap):
            return expert_call(fwd_kernel, first, count, cap, xs, w_one, w_three, w_two, pack, [], [F32, F32, BF])

        rest = local - LEAD
        f0 = fwd(0, LEAD, CAPS[0])
        y0 = swap(f0[3], 1, 0)
        f1 = fwd(LEAD, rest, CAPS[1])
        y1 = swap(f1[3], 1, 0)

        zd = swap(zy, 0, 2)
        mine = jnp.stack([zy, zd, d_here, zx])
        core = swap(mine, 0, 1)
        dout_all = jnp.concatenate([mine[:2], core[:2], mine[2:], core[2:]])

        shift = (slot_cap * jnp.arange(blocks, dtype=F32))[:, None, None]
        row_key = jnp.where(key >= 0, key + shift, -1.0).transpose(1, 0, 2).reshape(local, 1, blocks * tok_dev)
        gate_e = gate.transpose(1, 0, 2).reshape(local, 1, blocks * tok_dev)
        pick = row_key == jnp.arange(rows, dtype=F32)[None, :, None]
        slot_gate = jnp.sum(jnp.where(pick, gate_e, 0.0), axis=2)
        pick = pick.astype(BF).reshape(local * rows, blocks * tok_dev)
        us = jnp.dot(pick, dout_all.reshape(-1, width), preferred_element_type=F32)
        us = (us.reshape(local, rows, width) * slot_gate[:, :, None]).astype(BF)

        def bwd(first, count, cap, saved):
            return expert_call(bwd_kernel, first, count, cap, us, w_one, w_three, w_two, pack, saved, [BF, BF])

        b1 = bwd(LEAD, rest, CAPS[1], f1[:2])
        v1 = swap(b1[2], 1, 0)
        b0 = bwd(0, LEAD, CAPS[0], f0[:2])
        v0 = swap(b0[2], 1, 0)

        hid = jnp.concatenate([f0[2], f1[2]])
        d_one = jnp.concatenate([b0[0], b1[0]])
        d_three = jnp.concatenate([b0[1], b1[1]])
        grads = grad_call(xs, us, hid, d_one, d_three)

        sources = jnp.stack([ep_here, ep_here ^ 2, ep_here ^ 1, ep_here ^ 3])
        all_ids = (sources[:, None] * local + jnp.arange(local)).reshape(-1).astype(F32)
        eq = aux[:num_top, :, None] == all_ids
        hit = jnp.any(eq, axis=0)
        lower = (jnp.arange(tok_dev)[:, None] > jnp.arange(tok_dev)[None, :]).astype(BF)
        pos = jnp.dot(lower, hit.astype(BF), preferred_element_type=F32)
        own_gate = jnp.sum(jnp.where(eq, aux[num_top:, :, None], 0.0), axis=0)
        own_pick = hit[:, :, None] & (pos[:, :, None] == jnp.arange(slot_cap, dtype=F32))
        own_mul = jnp.where(own_pick, own_gate[:, :, None], 0.0).reshape(tok_dev, ep_size, local, slot_cap)
        own_pick = own_pick.astype(BF).reshape(tok_dev, ep_size, local, slot_cap)

        def send_back(parts):
            return [parts[0], swap(parts[1], 0, 2), swap(parts[2], 0, 1), swap(parts[3], 0, 3)]

        def mix(weights, back, first, count):
            flat = jnp.concatenate(back)
            weights = weights[:, :, first:first + count].reshape(tok_dev, -1)
            if weights.dtype == BF:
                return jnp.dot(weights, flat, preferred_element_type=F32)
            return jnp.dot(weights, flat.astype(F32), precision=lax.Precision.HIGHEST)

        def finish(first, count, own, recv, weights):
            keys = pack[first:first + count, 1].reshape(count, ep_size, slot_cap).transpose(1, 0, 2).reshape(-1, 1)
            back = send_back(finish_call(own, recv, keys, ep_size))
            return back[0], mix(weights, back, first, count)

        out_sum = finish(0, LEAD, f0[4], y0, own_mul)[1] + finish(LEAD, rest, f1[4], y1, own_mul)[1]
        ahead, dx_sum = finish(LEAD, rest, b1[3], v1, own_pick)
        own_last = lax.optimization_barrier((b0[3], ahead))[0]
        dx_sum = finish(0, LEAD, own_last, v0, own_pick)[1] + dx_sum

        every = jnp.arange(experts, dtype=F32)[None, :, None]
        count_all = sum(jnp.sum(aux_all[:, j:j + 1, :] == every, axis=2, dtype=jnp.int32) for j in range(num_top))
        kept = jnp.minimum(count_all, slot_cap).reshape(2, ep_size, ep_size, local).sum(axis=1)
        full = jnp.any(kept[:, :, :LEAD].sum(axis=2) > CAPS[0]) | jnp.any(kept[:, :, LEAD:].sum(axis=2) > CAPS[1])

        def exchange_all(args):
            hid, d_one, d_three, own_mul, own_pick = args

            def back(part):
                recv = swap(part[:, :half], 1, 0)
                done = (part[:, half:] + recv).astype(BF).reshape(local, ep_size, slot_cap, width)
                return send_back([done[:, s].reshape(-1, width) for s in range(ep_size)])

            part_out = jnp.einsum("enf,efd->end", hid, w_two, preferred_element_type=F32)
            part_dx = jnp.einsum("enf,edf->end", d_one, w_one, preferred_element_type=F32)
            part_dx += jnp.einsum("enf,edf->end", d_three, w_three, preferred_element_type=F32)
            return mix(own_mul, back(part_out), 0, local), mix(own_pick, back(part_dx), 0, local)

        def exchange_none(args):
            zero = jnp.zeros((tok_dev, width), F32)
            return zero, zero

        out_full, dx_full = lax.cond(full, exchange_all, exchange_none, (hid, d_one, d_three, own_mul, own_pick))
        out_rows = jnp.where(full, out_full, out_sum).astype(BF)
        dx_rows = jnp.where(full, dx_full, dx_sum).astype(BF)
        return out_rows, dx_rows, *grads

    return jax.shard_map(local_step, mesh=mesh,
                         in_specs=(row_spec, row_spec, row_spec, col_spec, col_spec, down_spec, row_spec),
                         out_specs=(row_spec, row_spec, grad_col, grad_col, grad_down), check_vma=False)
```

```python
import functools

import jax
import jax.numpy as jnp
from jax import lax
from jax.experimental import pallas as pl
from jax.experimental.pallas import tpu as pltpu
from jax.sharding import PartitionSpec as P


BF = jnp.bfloat16
F32 = jnp.float32
MESH = pl.DeviceIdType.MESH

LEAD = 3
CAPS = (240, 376)
VMEM_LIMIT = 62 * 2**20


def slot_count(num_top, tok_dev, experts):
    return 8 * ((5 * num_top * tok_dev + 32 * experts - 1) // (32 * experts))


def dot(a, b, ca, cb):
    return lax.dot_general(a, b, (((ca,), (cb,)), ((), ())), preferred_element_type=F32)


def place(rows, keys, cap):
    pick = lax.broadcasted_iota(jnp.int32, (cap, keys.shape[1]), 0).astype(F32) == keys
    pick = jnp.where(pick, 1.0, 0.0).astype(BF)
    high = rows.astype(BF)
    rest = rows - high.astype(F32)
    mid = rest.astype(BF)
    low = (rest - mid.astype(F32)).astype(BF)
    return (dot(pick, high, 1, 0) + dot(pick, mid, 1, 0)) + dot(pick, low, 1, 0)


def put_packed(y, half, cap, key_ref, other_ref, mine_ref):
    for part, ref in ((0, other_ref), (1, mine_ref)):
        placed = place(y[part * half:(part + 1) * half], key_ref[0, part:part + 1, :], cap)

        @pl.when(pl.program_id(0) == 0)
        def _():
            ref[...] = placed

        @pl.when(pl.program_id(0) > 0)
        def _():
            ref[...] += placed


def fwd_kernel(half, cap, x_ref, w1_ref, w3_ref, w2_ref, key_ref, a_ref, b_ref, h_ref, yo_ref, ym_ref):
    x = x_ref[0]
    a = dot(x, w1_ref[0], 1, 0)
    b = dot(x, w3_ref[0], 1, 0)
    h = (a * jax.nn.sigmoid(a) * b).astype(BF)
    a_ref[0] = a
    b_ref[0] = b
    h_ref[0] = h
    put_packed(dot(h, w2_ref[0], 1, 0), half, cap, key_ref, yo_ref, ym_ref)


def bwd_kernel(half, cap, u_ref, w1_ref, w3_ref, w2_ref, key_ref, a_ref, b_ref, da_ref, db_ref, vo_ref, vm_ref):
    dh = dot(u_ref[0], w2_ref[0], 1, 1)
    a = a_ref[0]
    s = jax.nn.sigmoid(a)
    da = (dh * b_ref[0] * s * (1.0 + a * (1.0 - s))).astype(BF)
    db = (dh * (a * s)).astype(BF)
    da_ref[0] = da
    db_ref[0] = db
    put_packed(dot(da, w1_ref[0], 1, 1) + dot(db, w3_ref[0], 1, 1), half, cap, key_ref, vo_ref, vm_ref)


def finish_kernel(own_ref, recv_ref, key_ref, *out_refs):
    done = (own_ref[...] + recv_ref[...]).astype(BF)
    rows = key_ref.shape[0] // len(out_refs)
    for i, out_ref in enumerate(out_refs):
        keys = key_ref[i * rows:(i + 1) * rows, :]
        pick = lax.broadcasted_iota(jnp.int32, (rows, done.shape[0]), 1).astype(F32) == keys
        out_ref[...] = dot(jnp.where(pick, 1.0, 0.0).astype(BF), done, 1, 0).astype(BF)


def grad_kernel(x_ref, u_ref, h_ref, da_ref, db_ref, g1_ref, g3_ref, g2_ref):
    x = x_ref[0]
    g1_ref[0] = dot(x, da_ref[0], 0, 0).astype(BF)
    g3_ref[0] = dot(x, db_ref[0], 0, 0).astype(BF)
    g2_ref[0] = dot(h_ref[0], u_ref[0], 0, 0).astype(BF)


def spec(shape, first):
    return pl.BlockSpec((1,) + shape, lambda i: (i + first, 0, 0))


def whole(shape):
    return pl.BlockSpec(shape, lambda i: (0,) * len(shape))


def cost(flops, nbytes):
    return pl.CostEstimate(flops=flops, bytes_accessed=nbytes, transcendentals=0)


PARAMS = pltpu.CompilerParams(dimension_semantics=("arbitrary",), vmem_limit_bytes=VMEM_LIMIT)


def expert_call(body, first, count, cap, rows_in, w1, w3, w2, keys, saved, kinds):
    rows, d, f = rows_in.shape[1], w1.shape[1], w1.shape[2]
    half = rows // 2
    outs = [((count, rows, f), t) for t in kinds] + [((cap, d), F32)] * 2
    return pl.pallas_call(
        functools.partial(body, half, cap), grid=(count,),
        in_specs=[spec((rows, d), first), spec((d, f), first), spec((d, f), first), spec((f, d), first),
                  spec((2, half), first)] + [spec((rows, f), 0)] * len(saved),
        out_specs=[spec(s[1:], 0) if len(s) == 3 else whole(s) for s, _ in outs],
        out_shape=[jax.ShapeDtypeStruct(s, t) for s, t in outs],
        compiler_params=PARAMS, cost_estimate=cost(count * 8 * rows * d * f, count * (6 * d * f + 6 * rows * d)),
    )(rows_in, w1, w3, w2, keys, *saved)


def grad_call(xs, us, h, da, db):
    count, rows, d = xs.shape
    f = h.shape[2]
    outs = [((d, f), BF), ((d, f), BF), ((f, d), BF)]
    return pl.pallas_call(
        grad_kernel, grid=(count,), name="wgrad",
        in_specs=[spec((rows, d), 0), spec((rows, d), 0)] + [spec((rows, f), 0)] * 3,
        out_specs=[spec(s, 0) for s, _ in outs],
        out_shape=[jax.ShapeDtypeStruct((count,) + s, t) for s, t in outs],
        compiler_params=PARAMS, cost_estimate=cost(count * 6 * rows * d * f, count * (6 * d * f + 4 * rows * d)),
    )(xs, us, h, da, db)


def finish_call(own, recv, keys, parts):
    rows, d = keys.shape[0] // parts, own.shape[1]
    return pl.pallas_call(
        finish_kernel, name="finish",
        out_shape=[jax.ShapeDtypeStruct((rows, d), BF)] * parts,
        compiler_params=pltpu.CompilerParams(vmem_limit_bytes=VMEM_LIMIT),
        cost_estimate=cost(2 * parts * rows * d * own.shape[0], 8 * own.shape[0] * d),
    )(own, recv, keys)


ACROSS_Y, ACROSS_XY, OWN, ACROSS_X, CORE = 0, 1, 4, 5, 6
STEPS = ((1, 0), (1, 2), (1, 1), (1, 3), (0, 0), (0, 2), (0, 1), (0, 3))


def prologue_kernel(slot_cap, num_top, cap, tok_ref, dout_ref, aux_ref, w1_hbm, w3_hbm, w2_hbm,
                    xs_hbm, us_hbm, a_hbm, b_hbm, h_hbm, yo_hbm, ym_hbm, pack_ref, aux_all_ref,
                    gathered, aux_all, xs, us, w1, w3, w2, a_buf, b_buf, h_buf, yo, ym, key_buf, gate_buf,
                    row_send, row_recv, aux_send, aux_recv, in_sem, out_sem):
    tp, ep = lax.axis_index("tp"), lax.axis_index("ep")
    eps = {0: ep, 2: lax.rem(ep + 2, 4), 1: ep + 1 - 2 * lax.rem(ep, 2), 3: 3 - ep}
    peers = [{"tp": 1 - tp if a else tp, "ep": eps[b]} for a, b in STEPS]
    others = [k for k in range(8) if k != OWN]
    local, width = key_buf.shape[1], key_buf.shape[2]
    half = 4 * slot_cap

    barrier = pltpu.get_barrier_semaphore()
    for k in others:
        pl.semaphore_signal(barrier, inc=1, device_id=peers[k], device_id_type=MESH)
    pl.semaphore_wait(barrier, len(others))

    def aux_copy(k):
        return pltpu.make_async_remote_copy(aux_ref, aux_all.at[k], aux_send.at[k], aux_recv.at[k],
                                            device_id=peers[k], device_id_type=MESH)

    def copy(i, slot, part):
        if slot in (ACROSS_Y, ACROSS_X, CORE):
            source, peer = (tok_ref, dout_ref)[i].at[part], slot
        elif slot == ACROSS_XY:
            source, peer = (gathered.at[i, ACROSS_Y, 0], ACROSS_X) if part == 0 else (gathered.at[i, ACROSS_X, 1], ACROSS_Y)
        else:
            source, peer = gathered.at[i, slot - 2, part], CORE
        return pltpu.make_async_remote_copy(source, gathered.at[i, slot, part], row_send.at[i, slot, part],
                                            row_recv.at[i, slot, part], device_id=peers[peer], device_id_type=MESH)

    def send_own(i):
        for slot, part in ((ACROSS_Y, 0), (ACROSS_X, 1), (ACROSS_Y, 1), (ACROSS_X, 0), (CORE, 0), (CORE, 1)):
            copy(i, slot, part).start()

    def relay(i, slot, part):
        copy(i, slot, part).wait_recv()
        if (slot, part) in ((ACROSS_Y, 0), (ACROSS_X, 1)):
            copy(i, ACROSS_XY, part).start()
        copy(i, slot + 2, part).start()

    def arrive(i):
        for slot in (CORE, CORE + 1, 2, 3):
            for part in (0, 1):
                copy(i, slot, part).wait_recv()

    for k in others:
        aux_copy(k).start()
    send_own(0)
    lead = w1.shape[0]
    loads = [pltpu.make_async_copy(w.at[pl.ds(0, lead)], buf, in_sem.at[n])
             for n, (w, buf) in enumerate(((w1_hbm, w1), (w3_hbm, w3), (w2_hbm, w2)))]
    for c in loads:
        c.start()
    gathered[0, OWN] = tok_ref[...]
    gathered[1, OWN] = dout_ref[...]
    aux_all[OWN] = aux_ref[...]

    for k in others:
        aux_copy(k).wait_recv()
    aux_all_ref[...] = aux_all[...]
    expert = (lax.broadcasted_iota(jnp.int32, (local, width), 0) + ep * local).astype(F32)
    hits = []
    for k in range(8):
        a = aux_all[k]
        hit, gate = jnp.zeros((local, width), F32), jnp.zeros((local, width), F32)
        for j in range(num_top):
            eq = a[j:j + 1, :] == expert
            hit = jnp.where(eq, 1.0, hit)
            gate = jnp.where(eq, a[num_top + j:num_top + j + 1, :], gate)
        hits.append(hit)
        gate_buf[k] = gate
    hit = jnp.concatenate(hits, axis=0)
    upper = lax.broadcasted_iota(jnp.int32, (width, width), 0) < lax.broadcasted_iota(jnp.int32, (width, width), 1)
    pos = dot(hit.astype(BF), jnp.where(upper, 1.0, 0.0).astype(BF), 1, 0)
    kept = jnp.where(pos < slot_cap, hit, 0.0)
    key = jnp.where(kept > 0.0, pos, -1.0)
    number = jnp.broadcast_to(jnp.sum(kept, axis=1, keepdims=True), key.shape)
    total = 8 * local
    row = lax.broadcasted_iota(jnp.int32, (total, total), 0)
    col = lax.broadcasted_iota(jnp.int32, (total, total), 1)
    rb, re, cb, ce = row // local, lax.rem(row, local), col // local, lax.rem(col, local)
    before = jnp.logical_and(rb // 4 == cb // 4, (re < LEAD) == (ce < LEAD))
    before = jnp.logical_and(before, jnp.logical_or(ce < re, jnp.logical_and(ce == re, cb < rb)))
    base = dot(jnp.where(before, 1.0, 0.0).astype(BF), number.astype(BF), 1, 0)
    lane = lax.broadcasted_iota(jnp.int32, (local, half), 1)
    slot, block = lax.rem(lane, slot_cap).astype(F32), lane // slot_cap
    for k in range(8):
        key_buf[k] = key[k * local:(k + 1) * local]
    for part in range(2):
        count, start = jnp.zeros((local, half), F32), jnp.zeros((local, half), F32)
        for n in range(4):
            k = (4 * part + n) * local
            count = jnp.where(block == n, number[k:k + local, :half], count)
            start = jnp.where(block == n, base[k:k + local, :half], start)
        packed = jnp.where(slot < count, start + slot, -1.0)
        for e in range(local):
            pack_ref[e, part:part + 1, :] = packed[e:e + 1]

    def dispatch(i, out):
        @pl.loop(0, 4)
        def _(n):
            first = 2 * n
            one, two = key_buf[first], key_buf[first + 1]
            pair = jnp.concatenate([one, jnp.where(two >= 0.0, two + slot_cap, -1.0)], axis=1)
            gates = jnp.concatenate([gate_buf[first], gate_buf[first + 1]], axis=1)
            index = lax.broadcasted_iota(jnp.int32, (2 * slot_cap, 2 * width), 0).astype(F32)
            picks = [index == pair[e:e + 1, :] for e in range(local)]
            pick = jnp.concatenate([jnp.where(p, 1.0, 0.0) for p in picks], axis=0).astype(BF)
            rows = dot(pick, gathered[i, pl.ds(first, 2)].reshape(2 * width, tok_ref.shape[2]), 1, 0)
            if i == 1:
                scale = jnp.concatenate([jnp.where(p, gates[e:e + 1, :], 0.0) for e, p in enumerate(picks)], axis=0)
                rows = rows * jnp.sum(scale, axis=1, keepdims=True)
            rows = rows.astype(BF)
            at = pl.ds(pl.multiple_of(first * slot_cap, 2 * slot_cap), 2 * slot_cap)
            for e in range(local):
                out[e, at, :] = rows[e * 2 * slot_cap:(e + 1) * 2 * slot_cap]

    relay(0, ACROSS_Y, 0)
    relay(0, ACROSS_X, 1)
    send_own(1)
    relay(0, ACROSS_Y, 1)
    relay(0, ACROSS_X, 0)
    relay(0, ACROSS_XY, 0)
    relay(0, ACROSS_XY, 1)
    arrive(0)
    dispatch(0, xs)
    stores = [pltpu.make_async_copy(xs, xs_hbm, out_sem.at[0])]
    stores[0].start()
    relay(1, ACROSS_Y, 0)
    relay(1, ACROSS_X, 1)
    for c in loads:
        c.wait()

    @pl.loop(0, lead)
    def _(e):
        x = xs[e]
        a = dot(x, w1[e], 1, 0)
        b = dot(x, w3[e], 1, 0)
        h = (a * jax.nn.sigmoid(a) * b).astype(BF)
        a_buf[e] = a
        b_buf[e] = b
        h_buf[e] = h
        y = dot(h, w2[e], 1, 0)
        keys = pack_ref[e]
        for part, out in ((0, yo), (1, ym)):
            placed = place(y[part * half:(part + 1) * half], keys[part:part + 1, :], cap)

            @pl.when(e == 0)
            def _():
                out[...] = placed

            @pl.when(e > 0)
            def _():
                out[...] += placed

        @pl.when(e == 0)
        def _():
            relay(1, ACROSS_Y, 1)
            relay(1, ACROSS_X, 0)

        @pl.when(e == 1)
        def _():
            relay(1, ACROSS_XY, 0)
            relay(1, ACROSS_XY, 1)

    for n, (buf, out) in enumerate(((yo, yo_hbm), (ym, ym_hbm), (a_buf, a_hbm), (b_buf, b_hbm), (h_buf, h_hbm))):
        stores.append(pltpu.make_async_copy(buf, out, out_sem.at[n + 1]))
        stores[-1].start()
    arrive(1)
    dispatch(1, us)
    stores.append(pltpu.make_async_copy(us, us_hbm, out_sem.at[6]))
    stores[-1].start()
    for k in others:
        aux_copy(k).wait_send()
        for i in (0, 1):
            for part in (0, 1):
                copy(i, k, part).wait_send()
    for c in stores:
        c.wait()


def prologue_call(tokens, d_out, aux, w1, w3, w2, slot_cap, num_top):
    tok_dev, width = tokens.shape
    local, f = w1.shape[0], w1.shape[2]
    rows, cap = 8 * slot_cap, CAPS[0]
    blocked = (2, tok_dev // 2, width)
    table = ((8, local, tok_dev), F32)
    acts = [((LEAD, rows, f), F32), ((LEAD, rows, f), F32), ((LEAD, rows, f), BF)]
    outs = [((local, rows, width), BF)] * 2 + acts + [((cap, width), F32)] * 2
    small = [((local, 2, rows // 2), F32), ((8,) + aux.shape, F32)]
    vmem = pl.BlockSpec(memory_space=pltpu.VMEM)
    anywhere = pl.BlockSpec(memory_space=pl.ANY)
    scratch = [((2, 8) + blocked, BF), ((8,) + aux.shape, F32)] + outs[:2]
    scratch += [((LEAD, width, f), BF)] * 2 + [((LEAD, f, width), BF)] + outs[2:] + [table] * 2
    dma = pltpu.SemaphoreType.DMA
    return pl.pallas_call(
        functools.partial(prologue_kernel, slot_cap, num_top, cap), name="prologue",
        in_specs=[vmem] * 3 + [anywhere] * 3,
        out_specs=[anywhere] * len(outs) + [vmem] * len(small),
        out_shape=[jax.ShapeDtypeStruct(s, t) for s, t in outs + small],
        scratch_shapes=[pltpu.VMEM(s, t) for s, t in scratch]
        + [dma((2, 8, 2)), dma((2, 8, 2)), dma((8,)), dma((8,)), dma((3,)), dma((7,))],
        compiler_params=pltpu.CompilerParams(collective_id=0, has_side_effects=True, vmem_limit_bytes=VMEM_LIMIT),
        cost_estimate=cost(15 * 10**9, 3 * 10**7),
    )(tokens.reshape(blocked), d_out.reshape(blocked), aux, w1, w3, w2)


def solution(mesh):
    tp_size, ep_size = mesh.shape["tp"], mesh.shape["ep"]
    row_spec = P(("dp", "ep", "tp"), None)
    col_spec = P("ep", None, "tp")
    down_spec = P("ep", "tp", None)
    grad_col = P(("dp", "ep"), None, "tp")
    grad_down = P(("dp", "ep"), "tp", None)

    def swap(z, tp_bit, ep_bits):
        pairs = [(t * ep_size + e, (t ^ tp_bit) * ep_size + (e ^ ep_bits)) for t in range(tp_size) for e in range(ep_size)]
        return lax.ppermute(z, ("tp", "ep"), pairs)

    def local_step(tokens, expert_ids, gate_vals, w_one, w_three, w_two, d_out):
        tok_dev, width = tokens.shape
        num_top = expert_ids.shape[1]
        local = w_one.shape[0]
        experts = local * ep_size
        slot_cap = slot_count(num_top, tok_dev, experts)
        half = tp_size * ep_size * slot_cap // 2
        ep_here = lax.axis_index("ep")

        aux = jnp.concatenate([expert_ids.astype(F32).T, gate_vals.T])
        xs, us, *f0, pack, aux_all = prologue_call(tokens, d_out, aux, w_one, w_three, w_two, slot_cap, num_top)

        def fwd(first, count, cap):
            return expert_call(fwd_kernel, first, count, cap, xs, w_one, w_three, w_two, pack, [], [F32, F32, BF])

        rest = local - LEAD
        y0 = swap(f0[3], 1, 0)
        f1 = fwd(LEAD, rest, CAPS[1])
        y1 = swap(f1[3], 1, 0)

        def bwd(first, count, cap, saved):
            return expert_call(bwd_kernel, first, count, cap, us, w_one, w_three, w_two, pack, saved, [BF, BF])

        b1 = bwd(LEAD, rest, CAPS[1], f1[:2])
        v1 = swap(b1[2], 1, 0)
        b0 = bwd(0, LEAD, CAPS[0], f0[:2])
        v0 = swap(b0[2], 1, 0)

        hid = jnp.concatenate([f0[2], f1[2]])
        d_one = jnp.concatenate([b0[0], b1[0]])
        d_three = jnp.concatenate([b0[1], b1[1]])
        grads = grad_call(xs, us, hid, d_one, d_three)

        sources = jnp.stack([ep_here, ep_here ^ 2, ep_here ^ 1, ep_here ^ 3])
        all_ids = (sources[:, None] * local + jnp.arange(local)).reshape(-1).astype(F32)
        eq = aux[:num_top, :, None] == all_ids
        hit = jnp.any(eq, axis=0)
        lower = (jnp.arange(tok_dev)[:, None] > jnp.arange(tok_dev)[None, :]).astype(BF)
        pos = jnp.dot(lower, hit.astype(BF), preferred_element_type=F32)
        own_gate = jnp.sum(jnp.where(eq, aux[num_top:, :, None], 0.0), axis=0)
        own_pick = hit[:, :, None] & (pos[:, :, None] == jnp.arange(slot_cap, dtype=F32))
        own_mul = jnp.where(own_pick, own_gate[:, :, None], 0.0).reshape(tok_dev, ep_size, local, slot_cap)
        own_pick = own_pick.astype(BF).reshape(tok_dev, ep_size, local, slot_cap)

        def send_back(parts):
            return [parts[0], swap(parts[1], 0, 2), swap(parts[2], 0, 1), swap(parts[3], 0, 3)]

        def mix(weights, back, first, count):
            flat = jnp.concatenate(back)
            weights = weights[:, :, first:first + count].reshape(tok_dev, -1)
            if weights.dtype == BF:
                return jnp.dot(weights, flat, preferred_element_type=F32)
            return jnp.dot(weights, flat.astype(F32), precision=lax.Precision.HIGHEST)

        def finish(first, count, own, recv, weights):
            keys = pack[first:first + count, 1].reshape(count, ep_size, slot_cap).transpose(1, 0, 2).reshape(-1, 1)
            back = send_back(finish_call(own, recv, keys, ep_size))
            return back[0], mix(weights, back, first, count)

        out_sum = finish(0, LEAD, f0[4], y0, own_mul)[1] + finish(LEAD, rest, f1[4], y1, own_mul)[1]
        ahead, dx_sum = finish(LEAD, rest, b1[3], v1, own_pick)
        own_last = lax.optimization_barrier((b0[3], ahead))[0]
        dx_sum = finish(0, LEAD, own_last, v0, own_pick)[1] + dx_sum

        every = jnp.arange(experts, dtype=F32)[None, :, None]
        count_all = sum(jnp.sum(aux_all[:, j:j + 1, :] == every, axis=2, dtype=jnp.int32) for j in range(num_top))
        kept = jnp.minimum(count_all, slot_cap).reshape(2, ep_size, ep_size, local).sum(axis=1)
        full = jnp.any(kept[:, :, :LEAD].sum(axis=2) > CAPS[0]) | jnp.any(kept[:, :, LEAD:].sum(axis=2) > CAPS[1])

        def exchange_all(args):
            hid, d_one, d_three, own_mul, own_pick = args

            def back(part):
                recv = swap(part[:, :half], 1, 0)
                done = (part[:, half:] + recv).astype(BF).reshape(local, ep_size, slot_cap, width)
                return send_back([done[:, s].reshape(-1, width) for s in range(ep_size)])

            part_out = jnp.einsum("enf,efd->end", hid, w_two, preferred_element_type=F32)
            part_dx = jnp.einsum("enf,edf->end", d_one, w_one, preferred_element_type=F32)
            part_dx += jnp.einsum("enf,edf->end", d_three, w_three, preferred_element_type=F32)
            return mix(own_mul, back(part_out), 0, local), mix(own_pick, back(part_dx), 0, local)

        def exchange_none(args):
            zero = jnp.zeros((tok_dev, width), F32)
            return zero, zero

        out_full, dx_full = lax.cond(full, exchange_all, exchange_none, (hid, d_one, d_three, own_mul, own_pick))
        out_rows = jnp.where(full, out_full, out_sum).astype(BF)
        dx_rows = jnp.where(full, dx_full, dx_sum).astype(BF)
        return out_rows, dx_rows, *grads

    return jax.shard_map(local_step, mesh=mesh,
                         in_specs=(row_spec, row_spec, row_spec, col_spec, col_spec, down_spec, row_spec),
                         out_specs=(row_spec, row_spec, grad_col, grad_col, grad_down), check_vma=False)
```

```python
import functools

import jax
import jax.numpy as jnp
from jax import lax
from jax.experimental import pallas as pl
from jax.experimental.pallas import tpu as pltpu
from jax.sharding import PartitionSpec as P


BF = jnp.bfloat16
F32 = jnp.float32
MESH = pl.DeviceIdType.MESH

LEAD = 3
CAPS = (240, 376)
VMEM_LIMIT = 62 * 2**20


def slot_count(num_top, tok_dev, experts):
    return 8 * ((5 * num_top * tok_dev + 32 * experts - 1) // (32 * experts))


def dot(a, b, ca, cb):
    return lax.dot_general(a, b, (((ca,), (cb,)), ((), ())), preferred_element_type=F32)


def place(rows, keys, cap):
    pick = lax.broadcasted_iota(jnp.int32, (cap, keys.shape[1]), 0).astype(F32) == keys
    return dot(jnp.where(pick, 1.0, 0.0).astype(BF), rows, 1, 0).astype(BF)


def put_packed(step, half, cap, keys, terms, refs):
    for part, ref in enumerate(refs):
        rows = slice(part * half, (part + 1) * half)
        packed = sum(dot(place(left[rows], keys[part:part + 1, :], cap), right, 1, dim) for left, right, dim in terms)

        @pl.when(step == 0)
        def _():
            ref[...] = packed

        @pl.when(step > 0)
        def _():
            ref[...] += packed


def fwd_kernel(half, cap, x_ref, w1_ref, w3_ref, w2_ref, key_ref, a_ref, b_ref, h_ref, yo_ref, ym_ref):
    x = x_ref[0]
    a = dot(x, w1_ref[0], 1, 0)
    b = dot(x, w3_ref[0], 1, 0)
    h = (a * jax.nn.sigmoid(a) * b).astype(BF)
    a_ref[0] = a
    b_ref[0] = b
    h_ref[0] = h
    put_packed(pl.program_id(0), half, cap, key_ref[0], [(h, w2_ref[0], 0)], (yo_ref, ym_ref))


def bwd_kernel(half, cap, u_ref, w1_ref, w3_ref, w2_ref, key_ref, a_ref, b_ref, da_ref, db_ref, vo_ref, vm_ref):
    dh = dot(u_ref[0], w2_ref[0], 1, 1)
    a = a_ref[0]
    s = jax.nn.sigmoid(a)
    da = (dh * b_ref[0] * s * (1.0 + a * (1.0 - s))).astype(BF)
    db = (dh * (a * s)).astype(BF)
    da_ref[0] = da
    db_ref[0] = db
    put_packed(pl.program_id(0), half, cap, key_ref[0], [(da, w1_ref[0], 1), (db, w3_ref[0], 1)], (vo_ref, vm_ref))


def finish_kernel(own_ref, recv_ref, key_ref, *out_refs):
    done = (own_ref[...] + recv_ref[...]).astype(BF)
    rows = key_ref.shape[0] // len(out_refs)
    for i, out_ref in enumerate(out_refs):
        keys = key_ref[i * rows:(i + 1) * rows, :]
        pick = lax.broadcasted_iota(jnp.int32, (rows, done.shape[0]), 1).astype(F32) == keys
        out_ref[...] = dot(jnp.where(pick, 1.0, 0.0).astype(BF), done, 1, 0).astype(BF)


def grad_kernel(x_ref, u_ref, h_ref, da_ref, db_ref, g1_ref, g3_ref, g2_ref):
    x = x_ref[0]
    g1_ref[0] = dot(x, da_ref[0], 0, 0).astype(BF)
    g3_ref[0] = dot(x, db_ref[0], 0, 0).astype(BF)
    g2_ref[0] = dot(h_ref[0], u_ref[0], 0, 0).astype(BF)


def spec(shape, first):
    return pl.BlockSpec((1,) + shape, lambda i: (i + first, 0, 0))


def whole(shape):
    return pl.BlockSpec(shape, lambda i: (0,) * len(shape))


def cost(flops, nbytes):
    return pl.CostEstimate(flops=flops, bytes_accessed=nbytes, transcendentals=0)


PARAMS = pltpu.CompilerParams(dimension_semantics=("arbitrary",), vmem_limit_bytes=VMEM_LIMIT)


def expert_call(body, first, count, cap, rows_in, w1, w3, w2, keys, saved, kinds):
    rows, d, f = rows_in.shape[1], w1.shape[1], w1.shape[2]
    half = rows // 2
    outs = [((count, rows, f), t) for t in kinds] + [((cap, d), F32)] * 2
    return pl.pallas_call(
        functools.partial(body, half, cap), grid=(count,),
        in_specs=[spec((rows, d), first), spec((d, f), first), spec((d, f), first), spec((f, d), first),
                  spec((2, half), first)] + [spec((rows, f), 0)] * len(saved),
        out_specs=[spec(s[1:], 0) if len(s) == 3 else whole(s) for s, _ in outs],
        out_shape=[jax.ShapeDtypeStruct(s, t) for s, t in outs],
        compiler_params=PARAMS, cost_estimate=cost(count * 8 * rows * d * f, count * (6 * d * f + 6 * rows * d)),
    )(rows_in, w1, w3, w2, keys, *saved)


def grad_call(xs, us, h, da, db):
    count, rows, d = xs.shape
    f = h.shape[2]
    outs = [((d, f), BF), ((d, f), BF), ((f, d), BF)]
    return pl.pallas_call(
        grad_kernel, grid=(count,), name="wgrad",
        in_specs=[spec((rows, d), 0), spec((rows, d), 0)] + [spec((rows, f), 0)] * 3,
        out_specs=[spec(s, 0) for s, _ in outs],
        out_shape=[jax.ShapeDtypeStruct((count,) + s, t) for s, t in outs],
        compiler_params=PARAMS, cost_estimate=cost(count * 6 * rows * d * f, count * (6 * d * f + 4 * rows * d)),
    )(xs, us, h, da, db)


def finish_call(own, recv, keys, parts):
    rows, d = keys.shape[0] // parts, own.shape[1]
    return pl.pallas_call(
        finish_kernel, name="finish",
        out_shape=[jax.ShapeDtypeStruct((rows, d), BF)] * parts,
        compiler_params=pltpu.CompilerParams(vmem_limit_bytes=VMEM_LIMIT),
        cost_estimate=cost(2 * parts * rows * d * own.shape[0], 8 * own.shape[0] * d),
    )(own, recv, keys)


ACROSS_Y, ACROSS_XY, OWN, ACROSS_X, CORE = 0, 1, 4, 5, 6
STEPS = ((1, 0), (1, 2), (1, 1), (1, 3), (0, 0), (0, 2), (0, 1), (0, 3))


def prologue_kernel(slot_cap, num_top, cap, tok_ref, dout_ref, id_ref, val_ref, w1_hbm, w3_hbm, w2_hbm,
                    xs_hbm, us_hbm, a_hbm, b_hbm, h_hbm, yo_hbm, ym_hbm, pack_ref, aux_all_ref,
                    gathered, aux_ref, aux_all, xs, us, w1, w3, w2, a_buf, b_buf, h_buf, yo, ym, key_buf, gate_buf,
                    row_send, row_recv, aux_send, aux_recv, in_sem, out_sem, row_out):
    tp, ep = lax.axis_index("tp"), lax.axis_index("ep")
    eps = {0: ep, 2: lax.rem(ep + 2, 4), 1: ep + 1 - 2 * lax.rem(ep, 2), 3: 3 - ep}
    peers = [{"tp": 1 - tp if a else tp, "ep": eps[b]} for a, b in STEPS]
    others = [k for k in range(8) if k != OWN]
    local, width = key_buf.shape[1], key_buf.shape[2]
    half = 4 * slot_cap

    aux_ref[...] = jnp.concatenate([id_ref[...].astype(F32), val_ref[...]], axis=1).T
    barrier = pltpu.get_barrier_semaphore()
    for k in others:
        pl.semaphore_signal(barrier, inc=1, device_id=peers[k], device_id_type=MESH)
    pl.semaphore_wait(barrier, len(others))

    def aux_copy(k):
        return pltpu.make_async_remote_copy(aux_ref, aux_all.at[k], aux_send.at[k], aux_recv.at[k],
                                            device_id=peers[k], device_id_type=MESH)

    def copy(i, slot, part):
        if slot in (ACROSS_Y, ACROSS_X, CORE):
            source, peer = (tok_ref, dout_ref)[i].at[part], slot
        elif slot == ACROSS_XY:
            source, peer = (gathered.at[i, ACROSS_Y, 0], ACROSS_X) if part == 0 else (gathered.at[i, ACROSS_X, 1], ACROSS_Y)
        else:
            source, peer = gathered.at[i, slot - 2, part], CORE
        return pltpu.make_async_remote_copy(source, gathered.at[i, slot, part], row_send.at[i, slot, part],
                                            row_recv.at[i, slot, part], device_id=peers[peer], device_id_type=MESH)

    def send_own(i):
        for slot, part in ((ACROSS_Y, 0), (ACROSS_X, 1), (ACROSS_Y, 1), (ACROSS_X, 0), (CORE, 0), (CORE, 1)):
            copy(i, slot, part).start()

    def relay(i, slot, part):
        copy(i, slot, part).wait_recv()
        if (slot, part) in ((ACROSS_Y, 0), (ACROSS_X, 1)):
            copy(i, ACROSS_XY, part).start()
        copy(i, slot + 2, part).start()

    def arrive(i, *slots):
        for slot in slots:
            for part in (0, 1):
                copy(i, slot, part).wait_recv()

    for k in others:
        aux_copy(k).start()
    send_own(0)
    lead = w1.shape[0]
    loads = [pltpu.make_async_copy(w.at[pl.ds(0, lead)], buf, in_sem.at[n])
             for n, (w, buf) in enumerate(((w1_hbm, w1), (w3_hbm, w3), (w2_hbm, w2)))]
    for c in loads:
        c.start()
    gathered[0, OWN] = tok_ref[...]
    gathered[1, OWN] = dout_ref[...]
    aux_all[OWN] = aux_ref[...]

    for k in others:
        aux_copy(k).wait_recv()
    aux_all_ref[...] = aux_all[...]
    expert = (lax.broadcasted_iota(jnp.int32, (local, width), 0) + ep * local).astype(F32)
    hits = []
    for k in range(8):
        a = aux_all[k]
        hit, gate = jnp.zeros((local, width), F32), jnp.zeros((local, width), F32)
        for j in range(num_top):
            eq = a[j:j + 1, :] == expert
            hit = jnp.where(eq, 1.0, hit)
            gate = jnp.where(eq, a[num_top + j:num_top + j + 1, :], gate)
        hits.append(hit)
        gate_buf[k] = gate
    hit = jnp.concatenate(hits, axis=0)
    upper = lax.broadcasted_iota(jnp.int32, (width, width), 0) < lax.broadcasted_iota(jnp.int32, (width, width), 1)
    pos = dot(hit.astype(BF), jnp.where(upper, 1.0, 0.0).astype(BF), 1, 0)
    kept = jnp.where(pos < slot_cap, hit, 0.0)
    key = jnp.where(kept > 0.0, pos, -1.0)
    number = jnp.broadcast_to(jnp.sum(kept, axis=1, keepdims=True), key.shape)
    total = 8 * local
    row = lax.broadcasted_iota(jnp.int32, (total, total), 0)
    col = lax.broadcasted_iota(jnp.int32, (total, total), 1)
    rb, re, cb, ce = row // local, lax.rem(row, local), col // local, lax.rem(col, local)
    before = jnp.logical_and(rb // 4 == cb // 4, (re < LEAD) == (ce < LEAD))
    before = jnp.logical_and(before, jnp.logical_or(ce < re, jnp.logical_and(ce == re, cb < rb)))
    base = dot(jnp.where(before, 1.0, 0.0).astype(BF), number.astype(BF), 1, 0)
    lane = lax.broadcasted_iota(jnp.int32, (local, half), 1)
    slot, block = lax.rem(lane, slot_cap).astype(F32), lane // slot_cap
    for k in range(8):
        key_buf[k] = key[k * local:(k + 1) * local]
    for part in range(2):
        count, start = jnp.zeros((local, half), F32), jnp.zeros((local, half), F32)
        for n in range(4):
            k = (4 * part + n) * local
            count = jnp.where(block == n, number[k:k + local, :half], count)
            start = jnp.where(block == n, base[k:k + local, :half], start)
        packed = jnp.where(slot < count, start + slot, -1.0)
        for e in range(local):
            pack_ref[e, part:part + 1, :] = packed[e:e + 1]

    def dispatch(i, out, ready):
        @pl.loop(0, 4)
        def _(n):
            for at, step in enumerate(ready):
                pl.when(n == at)(step)
            first = lax.rem(OWN + 4 * n, 8) + 2 * (n // 2)
            one, two = key_buf[first], key_buf[first + 1]
            pair = jnp.concatenate([one, jnp.where(two >= 0.0, two + slot_cap, -1.0)], axis=1)
            gates = jnp.concatenate([gate_buf[first], gate_buf[first + 1]], axis=1)
            index = lax.broadcasted_iota(jnp.int32, (2 * slot_cap, 2 * width), 0).astype(F32)
            picks = [index == pair[e:e + 1, :] for e in range(local)]
            pick = jnp.concatenate([jnp.where(p, 1.0, 0.0) for p in picks], axis=0).astype(BF)
            rows = dot(pick, gathered[i, pl.ds(first, 2)].reshape(2 * width, tok_ref.shape[2]), 1, 0)
            if i == 1:
                scale = jnp.concatenate([jnp.where(p, gates[e:e + 1, :], 0.0) for e, p in enumerate(picks)], axis=0)
                rows = rows * jnp.sum(scale, axis=1, keepdims=True)
            rows = rows.astype(BF)
            at = pl.ds(pl.multiple_of(first * slot_cap, 2 * slot_cap), 2 * slot_cap)
            for e in range(local):
                out[e, at, :] = rows[e * 2 * slot_cap:(e + 1) * 2 * slot_cap]
            pltpu.make_async_copy(out.at[:, at], (xs_hbm, us_hbm)[i].at[:, at], row_out.at[i, n]).start()

    relay(0, ACROSS_Y, 0)
    relay(0, ACROSS_X, 1)
    send_own(1)

    def second(i):
        relay(i, ACROSS_Y, 1)
        relay(i, ACROSS_X, 0)

    def third(i):
        relay(i, ACROSS_XY, 0)
        relay(i, ACROSS_XY, 1)

    def core(i, *slots):
        return lambda: arrive(i, *slots)

    dispatch(0, xs, [lambda: second(0), lambda: third(0), core(0, CORE, CORE + 1), core(0, 2, 3)])
    relay(1, ACROSS_Y, 0)
    relay(1, ACROSS_X, 1)
    for c in loads:
        c.wait()

    @pl.loop(0, lead)
    def _(e):
        x = xs[e]
        a = dot(x, w1[e], 1, 0)
        b = dot(x, w3[e], 1, 0)
        h = (a * jax.nn.sigmoid(a) * b).astype(BF)
        a_buf[e] = a
        b_buf[e] = b
        h_buf[e] = h
        put_packed(e, half, cap, pack_ref[e], [(h, w2[e], 0)], (yo, ym))

        @pl.when(e == 0)
        def _():
            second(1)

        @pl.when(e == 1)
        def _():
            third(1)

    stores = [pltpu.make_async_copy(buf, out, out_sem.at[n]) for n, (buf, out) in enumerate(
        ((yo, yo_hbm), (ym, ym_hbm), (a_buf, a_hbm), (b_buf, b_hbm), (h_buf, h_hbm)))]
    for c in stores:
        c.start()
    dispatch(1, us, [lambda: None, lambda: None, core(1, CORE, CORE + 1), core(1, 2, 3)])
    for i, (out, out_hbm) in enumerate(((xs, xs_hbm), (us, us_hbm))):
        for n in range(4):
            at = pl.ds(2 * slot_cap * n, 2 * slot_cap)
            stores.append(pltpu.make_async_copy(out.at[:, at], out_hbm.at[:, at], row_out.at[i, n]))
    for k in others:
        aux_copy(k).wait_send()
        for i in (0, 1):
            for part in (0, 1):
                copy(i, k, part).wait_send()
    for c in stores:
        c.wait()


def prologue_call(tokens, d_out, ids, gates, w1, w3, w2, slot_cap):
    tok_dev, width = tokens.shape
    num_top = ids.shape[1]
    aux = (2 * num_top, tok_dev)
    local, f = w1.shape[0], w1.shape[2]
    rows, cap = 8 * slot_cap, CAPS[0]
    blocked = (2, tok_dev // 2, width)
    table = ((8, local, tok_dev), F32)
    acts = [((LEAD, rows, f), F32), ((LEAD, rows, f), F32), ((LEAD, rows, f), BF)]
    outs = [((local, rows, width), BF)] * 2 + acts + [((cap, width), F32)] * 2
    small = [((local, 2, rows // 2), F32), ((8,) + aux, F32)]
    vmem = pl.BlockSpec(memory_space=pltpu.VMEM)
    anywhere = pl.BlockSpec(memory_space=pl.ANY)
    scratch = [((2, 8) + blocked, BF), (aux, F32), ((8,) + aux, F32)] + outs[:2]
    scratch += [((LEAD, width, f), BF)] * 2 + [((LEAD, f, width), BF)] + outs[2:] + [table] * 2
    dma = pltpu.SemaphoreType.DMA
    return pl.pallas_call(
        functools.partial(prologue_kernel, slot_cap, num_top, cap), name="prologue",
        in_specs=[vmem] * 4 + [anywhere] * 3,
        out_specs=[anywhere] * len(outs) + [vmem] * len(small),
        out_shape=[jax.ShapeDtypeStruct(s, t) for s, t in outs + small],
        scratch_shapes=[pltpu.VMEM(s, t) for s, t in scratch]
        + [dma((2, 8, 2)), dma((2, 8, 2)), dma((8,)), dma((8,)), dma((3,)), dma((5,)), dma((2, 4))],
        compiler_params=pltpu.CompilerParams(collective_id=0, has_side_effects=True, vmem_limit_bytes=VMEM_LIMIT),
        cost_estimate=cost(15 * 10**9, 3 * 10**7),
    )(tokens.reshape(blocked), d_out.reshape(blocked), ids, gates, w1, w3, w2)


def solution(mesh):
    tp_size, ep_size = mesh.shape["tp"], mesh.shape["ep"]
    row_spec = P(("dp", "ep", "tp"), None)
    col_spec = P("ep", None, "tp")
    down_spec = P("ep", "tp", None)
    grad_col = P(("dp", "ep"), None, "tp")
    grad_down = P(("dp", "ep"), "tp", None)

    def swap(z, tp_bit, ep_bits):
        pairs = [(t * ep_size + e, (t ^ tp_bit) * ep_size + (e ^ ep_bits)) for t in range(tp_size) for e in range(ep_size)]
        return lax.ppermute(z, ("tp", "ep"), pairs)

    def local_step(tokens, expert_ids, gate_vals, w_one, w_three, w_two, d_out):
        tok_dev, width = tokens.shape
        num_top = expert_ids.shape[1]
        local = w_one.shape[0]
        experts = local * ep_size
        slot_cap = slot_count(num_top, tok_dev, experts)
        half = tp_size * ep_size * slot_cap // 2
        ep_here = lax.axis_index("ep")

        xs, us, *f0, pack, aux_all = prologue_call(tokens, d_out, expert_ids, gate_vals, w_one, w_three, w_two, slot_cap)

        def fwd(first, count, cap):
            return expert_call(fwd_kernel, first, count, cap, xs, w_one, w_three, w_two, pack, [], [F32, F32, BF])

        rest = local - LEAD
        y0 = swap(f0[3], 1, 0)
        f1 = fwd(LEAD, rest, CAPS[1])
        y1 = swap(f1[3], 1, 0)

        def bwd(first, count, cap, saved):
            return expert_call(bwd_kernel, first, count, cap, us, w_one, w_three, w_two, pack, saved, [BF, BF])

        b1 = bwd(LEAD, rest, CAPS[1], f1[:2])
        v1 = swap(b1[2], 1, 0)
        b0 = bwd(0, LEAD, CAPS[0], f0[:2])
        v0 = swap(b0[2], 1, 0)

        hid = jnp.concatenate([f0[2], f1[2]])
        d_one = jnp.concatenate([b0[0], b1[0]])
        d_three = jnp.concatenate([b0[1], b1[1]])
        grads = grad_call(xs, us, hid, d_one, d_three)

        sources = jnp.stack([ep_here, ep_here ^ 2, ep_here ^ 1, ep_here ^ 3])
        all_ids = (sources[:, None] * local + jnp.arange(local)).reshape(-1)
        eq = expert_ids[:, :, None] == all_ids
        hit = jnp.any(eq, axis=1)
        lower = (jnp.arange(tok_dev)[:, None] > jnp.arange(tok_dev)[None, :]).astype(BF)
        pos = jnp.dot(lower, hit.astype(BF), preferred_element_type=F32)
        own_gate = jnp.sum(jnp.where(eq, gate_vals[:, :, None], 0.0), axis=1)
        own_pick = hit[:, :, None] & (pos[:, :, None] == jnp.arange(slot_cap, dtype=F32))
        own_mul = jnp.where(own_pick, own_gate[:, :, None], 0.0).reshape(tok_dev, ep_size, local, slot_cap)
        own_pick = own_pick.astype(BF).reshape(tok_dev, ep_size, local, slot_cap)

        def send_back(parts):
            return [parts[0], swap(parts[1], 0, 2), swap(parts[2], 0, 1), swap(parts[3], 0, 3)]

        def mix(weights, back, first, count):
            flat = jnp.concatenate(back)
            weights = weights[:, :, first:first + count].reshape(tok_dev, -1)
            if weights.dtype == BF:
                return jnp.dot(weights, flat, preferred_element_type=F32)
            return jnp.dot(weights, flat.astype(F32), precision=lax.Precision.HIGHEST)

        def finish(first, count, own, recv, weights):
            keys = pack[first:first + count, 1].reshape(count, ep_size, slot_cap).transpose(1, 0, 2).reshape(-1, 1)
            back = send_back(finish_call(own, recv, keys, ep_size))
            return back[0], mix(weights, back, first, count)

        out_sum = finish(0, LEAD, f0[4], y0, own_mul)[1] + finish(LEAD, rest, f1[4], y1, own_mul)[1]
        ahead, dx_sum = finish(LEAD, rest, b1[3], v1, own_pick)
        own_last = lax.optimization_barrier((b0[3], ahead, out_sum))[0]
        dx_sum = finish(0, LEAD, own_last, v0, own_pick)[1] + dx_sum

        every = jnp.arange(experts, dtype=F32)[None, :, None]
        count_all = sum(jnp.sum(aux_all[:, j:j + 1, :] == every, axis=2, dtype=jnp.int32) for j in range(num_top))
        kept = jnp.minimum(count_all, slot_cap).reshape(2, ep_size, ep_size, local).sum(axis=1)
        full = jnp.any(kept[:, :, :LEAD].sum(axis=2) > CAPS[0]) | jnp.any(kept[:, :, LEAD:].sum(axis=2) > CAPS[1])

        def exchange_all(args):
            hid, d_one, d_three, own_mul, own_pick = args

            def back(part):
                recv = swap(part[:, :half], 1, 0)
                done = (part[:, half:] + recv).astype(BF).reshape(local, ep_size, slot_cap, width)
                return send_back([done[:, s].reshape(-1, width) for s in range(ep_size)])

            part_out = jnp.einsum("enf,efd->end", hid, w_two, preferred_element_type=F32)
            part_dx = jnp.einsum("enf,edf->end", d_one, w_one, preferred_element_type=F32)
            part_dx += jnp.einsum("enf,edf->end", d_three, w_three, preferred_element_type=F32)
            return mix(own_mul, back(part_out), 0, local), mix(own_pick, back(part_dx), 0, local)

        def exchange_none(args):
            zero = jnp.zeros((tok_dev, width), F32)
            return zero, zero

        out_full, dx_full = lax.cond(full, exchange_all, exchange_none, (hid, d_one, d_three, own_mul, own_pick))
        out_rows = jnp.where(full, out_full, out_sum).astype(BF)
        dx_rows = jnp.where(full, dx_full, dx_sum).astype(BF)
        return out_rows, dx_rows, *grads

    return jax.shard_map(local_step, mesh=mesh,
                         in_specs=(row_spec, row_spec, row_spec, col_spec, col_spec, down_spec, row_spec),
                         out_specs=(row_spec, row_spec, grad_col, grad_col, grad_down), check_vma=False)
```

```python
import functools

import jax
import jax.numpy as jnp
from jax import lax
from jax.experimental import pallas as pl
from jax.experimental.pallas import tpu as pltpu
from jax.sharding import PartitionSpec as P


BF = jnp.bfloat16
F32 = jnp.float32
MESH = pl.DeviceIdType.MESH

LEAD = 3
CAPS = (240, 376)
VMEM_LIMIT = 62 * 2**20


def slot_count(num_top, tok_dev, experts):
    return 8 * ((5 * num_top * tok_dev + 32 * experts - 1) // (32 * experts))


def dot(a, b, ca, cb):
    return lax.dot_general(a, b, (((ca,), (cb,)), ((), ())), preferred_element_type=F32)


def place(rows, keys, cap):
    pick = lax.broadcasted_iota(jnp.int32, (cap, keys.shape[1]), 0).astype(F32) == keys
    return dot(jnp.where(pick, 1.0, 0.0).astype(BF), rows, 1, 0).astype(BF)


def packed_product(part, keys, cap, terms):
    half = keys.shape[1]
    rows = slice(part * half, (part + 1) * half)
    return sum(dot(place(left[rows], keys[part:part + 1, :], cap), right, 1, dim) for left, right, dim in terms)


def put_packed(step, first, keys, terms, refs):
    for part, ref in refs:
        packed = packed_product(part, keys, ref.shape[0], terms)

        @pl.when(step == first)
        def _():
            ref[...] = packed

        @pl.when(step > first)
        def _():
            ref[...] += packed


def fwd_kernel(x_ref, w1_ref, w3_ref, w2_ref, key_ref, a_ref, b_ref, h_ref, mine0_ref, other1_ref, mine1_ref):
    step = pl.program_id(0)
    x = x_ref[0]
    a = dot(x, w1_ref[0], 1, 0)
    b = dot(x, w3_ref[0], 1, 0)
    a_ref[0] = a
    b_ref[0] = b
    h_ref[0] = (a * jax.nn.sigmoid(a) * b).astype(BF)

    @pl.when(step < LEAD)
    def _():
        put_packed(step, 0, key_ref[0], [(h_ref[0], w2_ref[0], 0)], [(1, mine0_ref)])

    @pl.when(step >= LEAD)
    def _():
        put_packed(step, LEAD, key_ref[0], [(h_ref[0], w2_ref[0], 0)], [(0, other1_ref), (1, mine1_ref)])


def bwd_kernel(u_ref, w1_ref, w3_ref, w2_ref, key_ref, a_ref, b_ref, da_ref, db_ref, vo_ref, vm_ref):
    dh = dot(u_ref[0], w2_ref[0], 1, 1)
    a = a_ref[0]
    s = jax.nn.sigmoid(a)
    da = (dh * b_ref[0] * s * (1.0 + a * (1.0 - s))).astype(BF)
    db = (dh * (a * s)).astype(BF)
    da_ref[0] = da
    db_ref[0] = db
    put_packed(pl.program_id(0), 0, key_ref[0], [(da, w1_ref[0], 1), (db, w3_ref[0], 1)], [(0, vo_ref), (1, vm_ref)])


def finish_kernel(own_ref, recv_ref, key_ref, *out_refs):
    done = (own_ref[...] + recv_ref[...]).astype(BF)
    rows = key_ref.shape[0] // len(out_refs)
    for i, out_ref in enumerate(out_refs):
        keys = key_ref[i * rows:(i + 1) * rows, :]
        pick = lax.broadcasted_iota(jnp.int32, (rows, done.shape[0]), 1).astype(F32) == keys
        out_ref[...] = dot(jnp.where(pick, 1.0, 0.0).astype(BF), done, 1, 0).astype(BF)


def grad_kernel(x_ref, u_ref, h_ref, da_ref, db_ref, g1_ref, g3_ref, g2_ref):
    x = x_ref[0]
    g1_ref[0] = dot(x, da_ref[0], 0, 0).astype(BF)
    g3_ref[0] = dot(x, db_ref[0], 0, 0).astype(BF)
    g2_ref[0] = dot(h_ref[0], u_ref[0], 0, 0).astype(BF)


def spec(shape, first):
    return pl.BlockSpec((1,) + shape, lambda i: (i + first, 0, 0))


def whole(shape):
    return pl.BlockSpec(shape, lambda i: (0,) * len(shape))


def cost(flops, nbytes):
    return pl.CostEstimate(flops=flops, bytes_accessed=nbytes, transcendentals=0)


PARAMS = pltpu.CompilerParams(dimension_semantics=("arbitrary",), vmem_limit_bytes=VMEM_LIMIT)


def expert_call(body, first, count, rows_in, w1, w3, w2, keys, saved, kinds, caps):
    rows, d, f = rows_in.shape[1], w1.shape[1], w1.shape[2]
    half = rows // 2
    outs = [((count, rows, f), t) for t in kinds] + [((cap, d), F32) for cap in caps]
    return pl.pallas_call(
        body, grid=(count,),
        in_specs=[spec((rows, d), first), spec((d, f), first), spec((d, f), first), spec((f, d), first),
                  spec((2, half), first)] + [spec((rows, f), first)] * len(saved),
        out_specs=[spec(s[1:], 0) if len(s) == 3 else whole(s) for s, _ in outs],
        out_shape=[jax.ShapeDtypeStruct(s, t) for s, t in outs],
        compiler_params=PARAMS, cost_estimate=cost(count * 8 * rows * d * f, count * (6 * d * f + 6 * rows * d)),
    )(rows_in, w1, w3, w2, keys, *saved)


def grad_call(xs, us, h, da, db):
    count, rows, d = xs.shape
    f = h.shape[2]
    outs = [((d, f), BF), ((d, f), BF), ((f, d), BF)]
    return pl.pallas_call(
        grad_kernel, grid=(count,), name="wgrad",
        in_specs=[spec((rows, d), 0), spec((rows, d), 0)] + [spec((rows, f), 0)] * 3,
        out_specs=[spec(s, 0) for s, _ in outs],
        out_shape=[jax.ShapeDtypeStruct((count,) + s, t) for s, t in outs],
        compiler_params=PARAMS, cost_estimate=cost(count * 6 * rows * d * f, count * (6 * d * f + 4 * rows * d)),
    )(xs, us, h, da, db)


def finish_call(own, recv, keys, parts):
    rows, d = keys.shape[0] // parts, own.shape[1]
    return pl.pallas_call(
        finish_kernel, name="finish",
        out_shape=[jax.ShapeDtypeStruct((rows, d), BF)] * parts,
        compiler_params=pltpu.CompilerParams(vmem_limit_bytes=VMEM_LIMIT),
        cost_estimate=cost(2 * parts * rows * d * own.shape[0], 8 * own.shape[0] * d),
    )(own, recv, keys)


ACROSS_Y, ACROSS_XY, OWN, ACROSS_X, CORE = 0, 1, 4, 5, 6
STEPS = ((1, 0), (1, 2), (1, 1), (1, 3), (0, 0), (0, 2), (0, 1), (0, 3))


def find_peers():
    tp, ep = lax.axis_index("tp"), lax.axis_index("ep")
    eps = {0: ep, 2: lax.rem(ep + 2, 4), 1: ep + 1 - 2 * lax.rem(ep, 2), 3: 3 - ep}
    return ep, [{"tp": 1 - tp if a else tp, "ep": eps[b]} for a, b in STEPS]


def meet(peers):
    barrier = pltpu.get_barrier_semaphore()
    for peer in peers:
        pl.semaphore_signal(barrier, inc=1, device_id=peer, device_id_type=MESH)
    pl.semaphore_wait(barrier, len(peers))


def dispatch(slot_cap, blocks, key_ref, gate_ref, out, out_hbm, sem, ready):
    local, width = key_ref.shape[1], key_ref.shape[2]

    @pl.loop(0, 4)
    def _(n):
        for at, step in enumerate(ready):
            pl.when(n == at)(step)
        first = lax.rem(OWN + 4 * n, 8) + 2 * (n // 2)
        one, two = key_ref[first], key_ref[first + 1]
        pair = jnp.concatenate([one, jnp.where(two >= 0.0, two + slot_cap, -1.0)], axis=1)
        index = lax.broadcasted_iota(jnp.int32, (2 * slot_cap, 2 * width), 0).astype(F32)
        picks = [index == pair[e:e + 1, :] for e in range(local)]
        pick = jnp.concatenate([jnp.where(p, 1.0, 0.0) for p in picks], axis=0).astype(BF)
        rows = dot(pick, blocks[pl.ds(first, 2)].reshape(2 * width, out.shape[2]), 1, 0)
        if gate_ref is not None:
            gates = jnp.concatenate([gate_ref[first], gate_ref[first + 1]], axis=1)
            scale = jnp.concatenate([jnp.where(p, gates[e:e + 1, :], 0.0) for e, p in enumerate(picks)], axis=0)
            rows = rows * jnp.sum(scale, axis=1, keepdims=True)
        rows = rows.astype(BF)
        at = pl.ds(pl.multiple_of(first * slot_cap, 2 * slot_cap), 2 * slot_cap)
        for e in range(local):
            out[e, at, :] = rows[e * 2 * slot_cap:(e + 1) * 2 * slot_cap]
        pltpu.make_async_copy(out.at[:, at], out_hbm.at[:, at], sem.at[n]).start()


def dispatch_done(slot_cap, out, out_hbm, sem):
    for n in range(4):
        at = pl.ds(2 * slot_cap * n, 2 * slot_cap)
        pltpu.make_async_copy(out.at[:, at], out_hbm.at[:, at], sem.at[n]).wait()


def prologue_kernel(slot_cap, tok_ref, dout_ref, id_ref, val_ref, w1_hbm, w3_hbm, w2_hbm,
                    xs_hbm, yo_hbm, key_ref, gate_ref, pack_ref, aux_all_ref, across_ref,
                    gathered, aux_ref, aux_all, xs, w1, w3, w2, yo,
                    row_send, row_recv, aux_send, aux_recv, side_send, side_recv, in_sem, out_sem, row_out):
    ep, peers = find_peers()
    others = [k for k in range(8) if k != OWN]
    local, width = key_ref.shape[1], key_ref.shape[2]
    num_top, half = id_ref.shape[0], 4 * slot_cap

    aux_ref[...] = jnp.concatenate([id_ref[...].astype(F32), val_ref[...]], axis=0)
    lead = w1.shape[0]
    loads = [pltpu.make_async_copy(w.at[pl.ds(0, lead)], buf, in_sem.at[n])
             for n, (w, buf) in enumerate(((w1_hbm, w1), (w3_hbm, w3), (w2_hbm, w2)))]
    for c in loads:
        c.start()
    meet([peers[k] for k in others])

    def aux_copy(k):
        return pltpu.make_async_remote_copy(aux_ref, aux_all.at[k], aux_send.at[k], aux_recv.at[k],
                                            device_id=peers[k], device_id_type=MESH)

    def copy(slot, part):
        if slot in (ACROSS_Y, ACROSS_X, CORE):
            source, peer = tok_ref.at[part], slot
        elif slot == ACROSS_XY:
            source, peer = (gathered.at[ACROSS_Y, 0], ACROSS_X) if part == 0 else (gathered.at[ACROSS_X, 1], ACROSS_Y)
        else:
            source, peer = gathered.at[slot - 2, part], CORE
        return pltpu.make_async_remote_copy(source, gathered.at[slot, part], row_send.at[slot, part],
                                            row_recv.at[slot, part], device_id=peers[peer], device_id_type=MESH)

    def side_copy():
        return pltpu.make_async_remote_copy(dout_ref, across_ref, side_send, side_recv,
                                            device_id=peers[ACROSS_Y], device_id_type=MESH)

    def relay(slot, part):
        copy(slot, part).wait_recv()
        if (slot, part) in ((ACROSS_Y, 0), (ACROSS_X, 1)):
            copy(ACROSS_XY, part).start()
        copy(slot + 2, part).start()

    def arrive(*slots):
        for slot in slots:
            for part in (0, 1):
                copy(slot, part).wait_recv()

    for k in others:
        aux_copy(k).start()
    for slot, part in ((ACROSS_Y, 0), (ACROSS_X, 1), (ACROSS_Y, 1), (ACROSS_X, 0), (CORE, 0), (CORE, 1)):
        copy(slot, part).start()
    gathered[OWN] = tok_ref[...]
    aux_all[OWN] = aux_ref[...]

    for k in others:
        aux_copy(k).wait_recv()
    aux_all_ref[...] = aux_all[...]
    expert = (lax.broadcasted_iota(jnp.int32, (local, width), 0) + ep * local).astype(F32)
    hits = []
    for k in range(8):
        a = aux_all[k]
        hit, gate = jnp.zeros((local, width), F32), jnp.zeros((local, width), F32)
        for j in range(num_top):
            eq = a[j:j + 1, :] == expert
            hit = jnp.where(eq, 1.0, hit)
            gate = jnp.where(eq, a[num_top + j:num_top + j + 1, :], gate)
        hits.append(hit)
        gate_ref[k] = gate
    hit = jnp.concatenate(hits, axis=0)
    upper = lax.broadcasted_iota(jnp.int32, (width, width), 0) < lax.broadcasted_iota(jnp.int32, (width, width), 1)
    pos = dot(hit.astype(BF), jnp.where(upper, 1.0, 0.0).astype(BF), 1, 0)
    kept = jnp.where(pos < slot_cap, hit, 0.0)
    key = jnp.where(kept > 0.0, pos, -1.0)
    number = jnp.broadcast_to(jnp.sum(kept, axis=1, keepdims=True), key.shape)
    total = 8 * local
    row = lax.broadcasted_iota(jnp.int32, (total, total), 0)
    col = lax.broadcasted_iota(jnp.int32, (total, total), 1)
    rb, re, cb, ce = row // local, lax.rem(row, local), col // local, lax.rem(col, local)
    before = jnp.logical_and(rb // 4 == cb // 4, (re < LEAD) == (ce < LEAD))
    before = jnp.logical_and(before, jnp.logical_or(ce < re, jnp.logical_and(ce == re, cb < rb)))
    base = dot(jnp.where(before, 1.0, 0.0).astype(BF), number.astype(BF), 1, 0)
    lane = lax.broadcasted_iota(jnp.int32, (local, half), 1)
    slot, block = lax.rem(lane, slot_cap).astype(F32), lane // slot_cap
    for k in range(8):
        key_ref[k] = key[k * local:(k + 1) * local]
    for part in range(2):
        count, start = jnp.zeros((local, half), F32), jnp.zeros((local, half), F32)
        for n in range(4):
            k = (4 * part + n) * local
            count = jnp.where(block == n, number[k:k + local, :half], count)
            start = jnp.where(block == n, base[k:k + local, :half], start)
        packed = jnp.where(slot < count, start + slot, -1.0)
        for e in range(local):
            pack_ref[e, part:part + 1, :] = packed[e:e + 1]

    relay(ACROSS_Y, 0)
    relay(ACROSS_X, 1)
    side_copy().start()

    def second():
        relay(ACROSS_Y, 1)
        relay(ACROSS_X, 0)

    def third():
        relay(ACROSS_XY, 0)
        relay(ACROSS_XY, 1)

    dispatch(slot_cap, gathered, key_ref, None, xs, xs_hbm, row_out,
             [second, third, lambda: arrive(CORE, CORE + 1), lambda: arrive(2, 3)])
    for c in loads:
        c.wait()

    @pl.loop(0, lead)
    def _(e):
        x = xs[e, :half]
        a = dot(x, w1[e], 1, 0)
        b = dot(x, w3[e], 1, 0)
        h = (a * jax.nn.sigmoid(a) * b).astype(BF)
        put_packed(e, 0, pack_ref[e], [(h, w2[e], 0)], [(0, yo)])

    store = pltpu.make_async_copy(yo, yo_hbm, out_sem)
    store.start()
    for k in others:
        aux_copy(k).wait_send()
        for part in (0, 1):
            copy(k, part).wait_send()
    side_copy().wait()
    dispatch_done(slot_cap, xs, xs_hbm, row_out)
    store.wait()


def spread_kernel(slot_cap, dout_ref, across_ref, key_ref, gate_ref, us_hbm, gathered, us, row_send, row_recv, row_out):
    _, peers = find_peers()
    meet([peers[ACROSS_X], peers[CORE]])

    def copy(slot, part):
        if slot in (ACROSS_X, CORE):
            source, peer = dout_ref.at[part], slot
        elif slot in (ACROSS_XY, 2):
            source, peer = across_ref.at[part], ACROSS_X if slot == ACROSS_XY else CORE
        else:
            source, peer = gathered.at[slot - 2, part], CORE
        return pltpu.make_async_remote_copy(source, gathered.at[slot, part], row_send.at[slot, part],
                                            row_recv.at[slot, part], device_id=peers[peer], device_id_type=MESH)

    sent = [ACROSS_X, ACROSS_XY, CORE, 2, CORE + 1, 3]
    for slot in sent[:4]:
        for part in (0, 1):
            copy(slot, part).start()
    gathered[OWN] = dout_ref[...]
    gathered[ACROSS_Y] = across_ref[...]

    def relay(slot):
        for part in (0, 1):
            copy(slot, part).wait_recv()
            copy(slot + 2, part).start()

    def arrive(*slots):
        for slot in slots:
            for part in (0, 1):
                copy(slot, part).wait_recv()

    dispatch(slot_cap, gathered, key_ref, gate_ref, us, us_hbm, row_out,
             [lambda: relay(ACROSS_X), lambda: relay(ACROSS_XY), lambda: arrive(CORE, CORE + 1), lambda: arrive(2, 3)])
    for slot in sent:
        for part in (0, 1):
            copy(slot, part).wait_send()
    dispatch_done(slot_cap, us, us_hbm, row_out)


VMEM = pl.BlockSpec(memory_space=pltpu.VMEM)
ANY = pl.BlockSpec(memory_space=pl.ANY)
DMA = pltpu.SemaphoreType.DMA


def prologue_call(tokens, d_out, ids, gates, w1, w3, w2, slot_cap):
    num_top, tok_dev = ids.shape
    width, local, f = tokens.shape[2], w1.shape[0], w1.shape[2]
    rows, aux = 8 * slot_cap, (2 * num_top, tok_dev)
    large = [((local, rows, width), BF), ((CAPS[0], width), F32)]
    small = [((8, local, tok_dev), F32)] * 2 + [((local, 2, rows // 2), F32), ((8,) + aux, F32), (tokens.shape, BF)]
    scratch = [((8,) + tokens.shape, BF), (aux, F32), ((8,) + aux, F32), large[0]]
    scratch += [((LEAD, width, f), BF)] * 2 + [((LEAD, f, width), BF), large[1]]
    return pl.pallas_call(
        functools.partial(prologue_kernel, slot_cap), name="prologue",
        in_specs=[VMEM] * 4 + [ANY] * 3,
        out_specs=[ANY] * len(large) + [VMEM] * len(small),
        out_shape=[jax.ShapeDtypeStruct(s, t) for s, t in large + small],
        scratch_shapes=[pltpu.VMEM(s, t) for s, t in scratch]
        + [DMA((8, 2)), DMA((8, 2)), DMA((8,)), DMA((8,)), DMA, DMA, DMA((3,)), DMA, DMA((4,))],
        compiler_params=pltpu.CompilerParams(collective_id=0, has_side_effects=True, vmem_limit_bytes=VMEM_LIMIT),
        cost_estimate=cost(10**10, 3 * 10**7),
    )(tokens, d_out, ids, gates, w1, w3, w2)


def spread_call(d_out, across, key, gate, slot_cap):
    local = key.shape[1]
    out = (local, 8 * slot_cap, d_out.shape[2])
    return pl.pallas_call(
        functools.partial(spread_kernel, slot_cap), name="spread",
        in_specs=[VMEM] * 4, out_specs=ANY, out_shape=jax.ShapeDtypeStruct(out, BF),
        scratch_shapes=[pltpu.VMEM((8,) + d_out.shape, BF), pltpu.VMEM(out, BF), DMA((8, 2)), DMA((8, 2)), DMA((4,))],
        compiler_params=pltpu.CompilerParams(collective_id=1, has_side_effects=True, vmem_limit_bytes=VMEM_LIMIT),
        cost_estimate=cost(10**10, 3 * 10**7),
    )(d_out, across, key, gate)


def solution(mesh):
    tp_size, ep_size = mesh.shape["tp"], mesh.shape["ep"]
    row_spec = P(("dp", "ep", "tp"), None)
    col_spec = P("ep", None, "tp")
    down_spec = P("ep", "tp", None)
    grad_col = P(("dp", "ep"), None, "tp")
    grad_down = P(("dp", "ep"), "tp", None)

    def swap(z, tp_bit, ep_bits):
        pairs = [(t * ep_size + e, (t ^ tp_bit) * ep_size + (e ^ ep_bits)) for t in range(tp_size) for e in range(ep_size)]
        return lax.ppermute(z, ("tp", "ep"), pairs)

    def local_step(tokens, expert_ids, gate_vals, w_one, w_three, w_two, d_out):
        tok_dev, width = tokens.shape
        num_top = expert_ids.shape[1]
        local = w_one.shape[0]
        experts = local * ep_size
        slot_cap = slot_count(num_top, tok_dev, experts)
        half = tp_size * ep_size * slot_cap // 2
        ep_here = lax.axis_index("ep")

        blocked = (2, tok_dev // 2, width)
        d_blocked = d_out.reshape(blocked)
        xs, y_other0, key, gate, pack, aux_all, across = prologue_call(
            tokens.reshape(blocked), d_blocked, expert_ids.T, gate_vals.T, w_one, w_three, w_two, slot_cap)
        y0 = swap(y_other0, 1, 0)
        act_one, act_three, hid, y_mine0, y_other1, y_mine1 = expert_call(
            fwd_kernel, 0, local, xs, w_one, w_three, w_two, pack, [], [F32, F32, BF], (CAPS[0], CAPS[1], CAPS[1]))
        y1 = swap(y_other1, 1, 0)
        rest = local - LEAD
        across = lax.optimization_barrier((across, hid))[0]
        us = spread_call(d_blocked, across, key, gate, slot_cap)

        def bwd(first, count, cap):
            return expert_call(bwd_kernel, first, count, us, w_one, w_three, w_two, pack,
                               [act_one, act_three], [BF, BF], (cap, cap))

        b1 = bwd(LEAD, rest, CAPS[1])
        v1 = swap(b1[2], 1, 0)
        b0 = bwd(0, LEAD, CAPS[0])
        v0 = swap(b0[2], 1, 0)

        d_one = jnp.concatenate([b0[0], b1[0]])
        d_three = jnp.concatenate([b0[1], b1[1]])
        grads = grad_call(xs, us, hid, d_one, d_three)

        sources = jnp.stack([ep_here, ep_here ^ 2, ep_here ^ 1, ep_here ^ 3])
        all_ids = (sources[:, None] * local + jnp.arange(local)).reshape(-1)
        eq = expert_ids[:, :, None] == all_ids
        hit = jnp.any(eq, axis=1)
        lower = (jnp.arange(tok_dev)[:, None] > jnp.arange(tok_dev)[None, :]).astype(BF)
        pos = jnp.dot(lower, hit.astype(BF), preferred_element_type=F32)
        own_gate = jnp.sum(jnp.where(eq, gate_vals[:, :, None], 0.0), axis=1)
        own_pick = hit[:, :, None] & (pos[:, :, None] == jnp.arange(slot_cap, dtype=F32))
        own_mul = jnp.where(own_pick, own_gate[:, :, None], 0.0).reshape(tok_dev, ep_size, local, slot_cap)
        own_pick = own_pick.astype(BF).reshape(tok_dev, ep_size, local, slot_cap)

        def send_back(parts):
            return [parts[0], swap(parts[1], 0, 2), swap(parts[2], 0, 1), swap(parts[3], 0, 3)]

        def mix(weights, back, first, count):
            flat = jnp.concatenate(back)
            weights = weights[:, :, first:first + count].reshape(tok_dev, -1)
            if weights.dtype == BF:
                return jnp.dot(weights, flat, preferred_element_type=F32)
            return jnp.dot(weights, flat.astype(F32), precision=lax.Precision.HIGHEST)

        def finish(first, count, own, recv, weights):
            keys = pack[first:first + count, 1].reshape(count, ep_size, slot_cap).transpose(1, 0, 2).reshape(-1, 1)
            back = send_back(finish_call(own, recv, keys, ep_size))
            return back[0], mix(weights, back, first, count)

        out_sum = finish(0, LEAD, y_mine0, y0, own_mul)[1] + finish(LEAD, rest, y_mine1, y1, own_mul)[1]
        ahead, dx_sum = finish(LEAD, rest, b1[3], v1, own_pick)
        own_last = lax.optimization_barrier((b0[3], ahead, out_sum))[0]
        dx_sum = finish(0, LEAD, own_last, v0, own_pick)[1] + dx_sum

        every = jnp.arange(experts, dtype=F32)[None, :, None]
        count_all = sum(jnp.sum(aux_all[:, j:j + 1, :] == every, axis=2, dtype=jnp.int32) for j in range(num_top))
        kept = jnp.minimum(count_all, slot_cap).reshape(2, ep_size, ep_size, local).sum(axis=1)
        full = jnp.any(kept[:, :, :LEAD].sum(axis=2) > CAPS[0]) | jnp.any(kept[:, :, LEAD:].sum(axis=2) > CAPS[1])

        def exchange_all(args):
            hid, d_one, d_three, own_mul, own_pick = args

            def back(part):
                recv = swap(part[:, :half], 1, 0)
                done = (part[:, half:] + recv).astype(BF).reshape(local, ep_size, slot_cap, width)
                return send_back([done[:, s].reshape(-1, width) for s in range(ep_size)])

            part_out = jnp.einsum("enf,efd->end", hid, w_two, preferred_element_type=F32)
            part_dx = jnp.einsum("enf,edf->end", d_one, w_one, preferred_element_type=F32)
            part_dx += jnp.einsum("enf,edf->end", d_three, w_three, preferred_element_type=F32)
            return mix(own_mul, back(part_out), 0, local), mix(own_pick, back(part_dx), 0, local)

        def exchange_none(args):
            zero = jnp.zeros((tok_dev, width), F32)
            return zero, zero

        out_full, dx_full = lax.cond(full, exchange_all, exchange_none, (hid, d_one, d_three, own_mul, own_pick))
        out_rows = jnp.where(full, out_full, out_sum).astype(BF)
        dx_rows = jnp.where(full, dx_full, dx_sum).astype(BF)
        return out_rows, dx_rows, *grads

    return jax.shard_map(local_step, mesh=mesh,
                         in_specs=(row_spec, row_spec, row_spec, col_spec, col_spec, down_spec, row_spec),
                         out_specs=(row_spec, row_spec, grad_col, grad_col, grad_down), check_vma=False)
```

```python
import functools

import jax
import jax.numpy as jnp
from jax import lax
from jax.experimental import pallas as pl
from jax.experimental.pallas import tpu as pltpu
from jax.sharding import PartitionSpec as P


BF = jnp.bfloat16
F32 = jnp.float32
MESH = pl.DeviceIdType.MESH

LEAD = 3
TOTAL = 584
Y_FIRST, Y_MOST = 168, 240
V_FIRST, V_MOST = 280, 376
V_CUTS = (280, 384, 512, 584)
WINDOW = 104
VMEM_LIMIT = 62 * 2**20


def slot_count(num_top, tok_dev, experts):
    return 8 * ((5 * num_top * tok_dev + 32 * experts - 1) // (32 * experts))


def dot(a, b, ca, cb):
    return lax.dot_general(a, b, (((ca,), (cb,)), ((), ())), preferred_element_type=F32)


def place(rows, keys, cap):
    pick = lax.broadcasted_iota(jnp.int32, (cap, keys.shape[1]), 0).astype(F32) == keys
    return dot(jnp.where(pick, 1.0, 0.0).astype(BF), rows, 1, 0).astype(BF)


def add_window(ref, part, keys, shift, base, terms):
    half = keys.shape[1]
    rows = slice(part * half, (part + 1) * half)
    start = jnp.clip((base - shift) // 8 * 8, 0, ref.shape[0] - WINDOW)
    at = keys[part:part + 1, :] - (start + shift).astype(F32)
    product = sum(dot(place(left[rows], at, WINDOW), right, 1, dim) for left, right, dim in terms)
    ref[pl.ds(pl.multiple_of(start, 8), WINDOW), :] += product


def fwd_kernel(base_ref, x_ref, w1_ref, w3_ref, w2_ref, key_ref, spill_ref, a_ref, b_ref, h_ref, other_ref, mine_ref):
    step = pl.program_id(0)

    @pl.when(step == 0)
    def _():
        mine_ref[...] = jnp.zeros_like(mine_ref)
        other_ref[...] = jnp.zeros_like(other_ref)
        other_ref[:spill_ref.shape[0], :] = spill_ref[...]

    x = x_ref[0]
    a = dot(x, w1_ref[0], 1, 0)
    b = dot(x, w3_ref[0], 1, 0)
    h = (a * jax.nn.sigmoid(a) * b).astype(BF)
    a_ref[0] = a
    b_ref[0] = b
    h_ref[0] = h
    add_window(mine_ref, 1, key_ref[0], 0, base_ref[1, step], [(h, w2_ref[0], 0)])

    @pl.when(step >= LEAD)
    def _():
        add_window(other_ref, 0, key_ref[0], Y_FIRST, base_ref[0, step], [(h_ref[0], w2_ref[0], 0)])


def bwd_step(expert, shift, base_ref, u_ref, w1_ref, w3_ref, w2_ref, key_ref, a_ref, b_ref, da_ref, db_ref, parts):
    dh = dot(u_ref[0], w2_ref[0], 1, 1)
    a = a_ref[0]
    s = jax.nn.sigmoid(a)
    da = (dh * b_ref[0] * s * (1.0 + a * (1.0 - s))).astype(BF)
    db = (dh * (a * s)).astype(BF)
    da_ref[0] = da
    db_ref[0] = db
    for part, ref in enumerate(parts):
        add_window(ref, part, key_ref[0], shift, base_ref[part, expert], [(da, w1_ref[0], 1), (db, w3_ref[0], 1)])


def bwd_rest_kernel(base_ref, u_ref, w1_ref, w3_ref, w2_ref, key_ref, a_ref, b_ref, da_ref, db_ref,
                    other_ref, spill_other_ref, mine_ref, spill_mine_ref, other, mine):
    step = pl.program_id(0)

    @pl.when(step == 0)
    def _():
        other[...] = jnp.zeros_like(other)
        mine[...] = jnp.zeros_like(mine)

    bwd_step(step + LEAD, 0, base_ref, u_ref, w1_ref, w3_ref, w2_ref, key_ref, a_ref, b_ref, da_ref, db_ref, (other, mine))

    @pl.when(step == pl.num_programs(0) - 1)
    def _():
        other_ref[...] = other[:V_FIRST]
        spill_other_ref[...] = other[V_FIRST:]
        mine_ref[...] = mine[:V_FIRST]
        spill_mine_ref[...] = mine[V_FIRST:]


def bwd_lead_kernel(base_ref, u_ref, w1_ref, w3_ref, w2_ref, key_ref, a_ref, b_ref, spill_other_ref, spill_mine_ref,
                    da_ref, db_ref, other1_ref, other2_ref, other3_ref, mine_ref, other):
    step = pl.program_id(0)

    @pl.when(step == 0)
    def _():
        for ref, spill_ref in ((other, spill_other_ref), (mine_ref, spill_mine_ref)):
            ref[...] = jnp.zeros_like(ref)
            ref[:spill_ref.shape[0], :] = spill_ref[...]

    bwd_step(step, V_FIRST, base_ref, u_ref, w1_ref, w3_ref, w2_ref, key_ref, a_ref, b_ref, da_ref, db_ref,
             (other, mine_ref))

    @pl.when(step == pl.num_programs(0) - 1)
    def _():
        for n, ref in enumerate((other1_ref, other2_ref, other3_ref)):
            ref[...] = other[V_CUTS[n] - V_FIRST:V_CUTS[n + 1] - V_FIRST]


def finish_kernel(pieces, owns, *refs):
    own_refs, recv_refs, key_ref = refs[:owns], refs[owns:owns + len(pieces)], refs[owns + len(pieces)]
    out_refs = refs[owns + len(pieces) + 1:]
    done = [(own_refs[i][row:row + count, :] + recv_ref[...]).astype(BF)
            for (i, row, _, count), recv_ref in zip(pieces, recv_refs)]
    rows = key_ref.shape[0] // len(out_refs)
    for i, out_ref in enumerate(out_refs):
        keys = key_ref[i * rows:(i + 1) * rows, :]
        total = None
        for (_, _, position, count), values in zip(pieces, done):
            pick = lax.broadcasted_iota(jnp.int32, (rows, count), 1).astype(F32) == keys - float(position)
            term = dot(jnp.where(pick, 1.0, 0.0).astype(BF), values, 1, 0)
            total = term if total is None else total + term
        out_ref[...] = total.astype(BF)


def grad_kernel(x_ref, u_ref, h_ref, da_ref, db_ref, g1_ref, g3_ref, g2_ref):
    x = x_ref[0]
    g1_ref[0] = dot(x, da_ref[0], 0, 0).astype(BF)
    g3_ref[0] = dot(x, db_ref[0], 0, 0).astype(BF)
    g2_ref[0] = dot(h_ref[0], u_ref[0], 0, 0).astype(BF)


def spec(shape, first):
    return pl.BlockSpec((1,) + shape, lambda i, *_: (i + first, 0, 0))


def whole(shape):
    return pl.BlockSpec(shape, lambda i, *_: (0,) * len(shape))


def cost(flops, nbytes):
    return pl.CostEstimate(flops=flops, bytes_accessed=nbytes, transcendentals=0)


PARAMS = pltpu.CompilerParams(dimension_semantics=("arbitrary",), vmem_limit_bytes=VMEM_LIMIT)


def expert_call(body, first, count, base, rows_in, w1, w3, w2, keys, saved, extra, kinds, outs, scratch):
    rows, d, f = rows_in.shape[1], w1.shape[1], w1.shape[2]
    half = rows // 2
    shapes = [((count, rows, f), t) for t in kinds] + [((n, d), F32) for n in outs]
    return pl.pallas_call(
        body,
        grid_spec=pltpu.PrefetchScalarGridSpec(
            num_scalar_prefetch=1, grid=(count,),
            in_specs=[spec((rows, d), first), spec((d, f), first), spec((d, f), first), spec((f, d), first),
                      spec((2, half), first)] + [spec((rows, f), first)] * len(saved) + [whole(e.shape) for e in extra],
            out_specs=[spec(s[1:], 0) if len(s) == 3 else whole(s) for s, _ in shapes],
            scratch_shapes=[pltpu.VMEM((n, d), F32) for n in scratch]),
        out_shape=[jax.ShapeDtypeStruct(s, t) for s, t in shapes],
        compiler_params=PARAMS, cost_estimate=cost(count * 8 * rows * d * f, count * (6 * d * f + 6 * rows * d)),
    )(base, rows_in, w1, w3, w2, keys, *saved, *extra)


def grad_call(xs, us, h, da, db):
    count, rows, d = xs.shape
    f = h.shape[2]
    outs = [((d, f), BF), ((d, f), BF), ((f, d), BF)]
    return pl.pallas_call(
        grad_kernel, grid=(count,), name="wgrad",
        in_specs=[spec((rows, d), 0), spec((rows, d), 0)] + [spec((rows, f), 0)] * 3,
        out_specs=[spec(s, 0) for s, _ in outs],
        out_shape=[jax.ShapeDtypeStruct((count,) + s, t) for s, t in outs],
        compiler_params=PARAMS, cost_estimate=cost(count * 6 * rows * d * f, count * (6 * d * f + 4 * rows * d)),
    )(xs, us, h, da, db)


def finish_call(owns, pieces, recvs, keys, parts):
    rows, d = keys.shape[0] // parts, owns[0].shape[1]
    total = sum(r.shape[0] for r in recvs)
    return pl.pallas_call(
        functools.partial(finish_kernel, pieces, len(owns)), name="finish",
        out_shape=[jax.ShapeDtypeStruct((rows, d), BF)] * parts,
        compiler_params=pltpu.CompilerParams(vmem_limit_bytes=VMEM_LIMIT),
        cost_estimate=cost(2 * parts * rows * d * total, 8 * total * d),
    )(*owns, *recvs, keys)


ACROSS_Y, ACROSS_XY, OWN, ACROSS_X, CORE = 0, 1, 4, 5, 6
STEPS = ((1, 0), (1, 2), (1, 1), (1, 3), (0, 0), (0, 2), (0, 1), (0, 3))


def find_peers():
    tp, ep = lax.axis_index("tp"), lax.axis_index("ep")
    eps = {0: ep, 2: lax.rem(ep + 2, 4), 1: ep + 1 - 2 * lax.rem(ep, 2), 3: 3 - ep}
    return ep, [{"tp": 1 - tp if a else tp, "ep": eps[b]} for a, b in STEPS]


def meet(peers):
    barrier = pltpu.get_barrier_semaphore()
    for peer in peers:
        pl.semaphore_signal(barrier, inc=1, device_id=peer, device_id_type=MESH)
    pl.semaphore_wait(barrier, len(peers))


def dispatch(slot_cap, blocks, key_ref, gate_ref, out, out_hbm, sem, ready):
    local, width = key_ref.shape[1], key_ref.shape[2]

    @pl.loop(0, 4)
    def _(n):
        for at, step in enumerate(ready):
            pl.when(n == at)(step)
        first = lax.rem(OWN + 4 * n, 8) + 2 * (n // 2)
        one, two = key_ref[first], key_ref[first + 1]
        pair = jnp.concatenate([one, jnp.where(two >= 0.0, two + slot_cap, -1.0)], axis=1)
        index = lax.broadcasted_iota(jnp.int32, (2 * slot_cap, 2 * width), 0).astype(F32)
        picks = [index == pair[e:e + 1, :] for e in range(local)]
        pick = jnp.concatenate([jnp.where(p, 1.0, 0.0) for p in picks], axis=0).astype(BF)
        rows = dot(pick, blocks[pl.ds(first, 2)].reshape(2 * width, out.shape[2]), 1, 0)
        if gate_ref is not None:
            gates = jnp.concatenate([gate_ref[first], gate_ref[first + 1]], axis=1)
            scale = jnp.concatenate([jnp.where(p, gates[e:e + 1, :], 0.0) for e, p in enumerate(picks)], axis=0)
            rows = rows * jnp.sum(scale, axis=1, keepdims=True)
        rows = rows.astype(BF)
        at = pl.ds(pl.multiple_of(first * slot_cap, 2 * slot_cap), 2 * slot_cap)
        for e in range(local):
            out[e, at, :] = rows[e * 2 * slot_cap:(e + 1) * 2 * slot_cap]
        pltpu.make_async_copy(out.at[:, at], out_hbm.at[:, at], sem.at[n]).start()


def dispatch_done(slot_cap, out, out_hbm, sem):
    for n in range(4):
        at = pl.ds(2 * slot_cap * n, 2 * slot_cap)
        pltpu.make_async_copy(out.at[:, at], out_hbm.at[:, at], sem.at[n]).wait()


def prologue_kernel(slot_cap, tok_ref, dout_ref, id_ref, val_ref, w1_hbm, w3_hbm, w2_hbm,
                    xs_hbm, yo_hbm, spill_hbm, key_ref, gate_ref, pack_y_ref, pack_v_ref, base_ref, aux_all_ref, across_ref,
                    gathered, aux_ref, aux_all, xs, w1, w3, w2, yo,
                    row_send, row_recv, aux_send, aux_recv, side_send, side_recv, in_sem, out_sem, row_out):
    ep, peers = find_peers()
    others = [k for k in range(8) if k != OWN]
    local, width = key_ref.shape[1], key_ref.shape[2]
    num_top, half = id_ref.shape[0], 4 * slot_cap

    aux_ref[...] = jnp.concatenate([id_ref[...].astype(F32), val_ref[...]], axis=0)
    lead = w1.shape[0]
    loads = [pltpu.make_async_copy(w.at[pl.ds(0, lead)], buf, in_sem.at[n])
             for n, (w, buf) in enumerate(((w1_hbm, w1), (w3_hbm, w3), (w2_hbm, w2)))]
    for c in loads:
        c.start()
    meet([peers[k] for k in others])

    def aux_copy(k):
        return pltpu.make_async_remote_copy(aux_ref, aux_all.at[k], aux_send.at[k], aux_recv.at[k],
                                            device_id=peers[k], device_id_type=MESH)

    def copy(slot, part):
        if slot in (ACROSS_Y, ACROSS_X, CORE):
            source, peer = tok_ref.at[part], slot
        elif slot == ACROSS_XY:
            source, peer = (gathered.at[ACROSS_Y, 0], ACROSS_X) if part == 0 else (gathered.at[ACROSS_X, 1], ACROSS_Y)
        else:
            source, peer = gathered.at[slot - 2, part], CORE
        return pltpu.make_async_remote_copy(source, gathered.at[slot, part], row_send.at[slot, part],
                                            row_recv.at[slot, part], device_id=peers[peer], device_id_type=MESH)

    def side_copy():
        return pltpu.make_async_remote_copy(dout_ref, across_ref, side_send, side_recv,
                                            device_id=peers[ACROSS_Y], device_id_type=MESH)

    def relay(slot, part):
        copy(slot, part).wait_recv()
        if (slot, part) in ((ACROSS_Y, 0), (ACROSS_X, 1)):
            copy(ACROSS_XY, part).start()
        copy(slot + 2, part).start()

    def arrive(*slots):
        for slot in slots:
            for part in (0, 1):
                copy(slot, part).wait_recv()

    for k in others:
        aux_copy(k).start()
    for slot, part in ((ACROSS_Y, 0), (ACROSS_X, 1), (ACROSS_Y, 1), (ACROSS_X, 0), (CORE, 0), (CORE, 1)):
        copy(slot, part).start()
    gathered[OWN] = tok_ref[...]
    aux_all[OWN] = aux_ref[...]

    for k in others:
        aux_copy(k).wait_recv()
    aux_all_ref[...] = aux_all[...]
    expert = (lax.broadcasted_iota(jnp.int32, (local, width), 0) + ep * local).astype(F32)
    hits = []
    for k in range(8):
        a = aux_all[k]
        hit, gate = jnp.zeros((local, width), F32), jnp.zeros((local, width), F32)
        for j in range(num_top):
            eq = a[j:j + 1, :] == expert
            hit = jnp.where(eq, 1.0, hit)
            gate = jnp.where(eq, a[num_top + j:num_top + j + 1, :], gate)
        hits.append(hit)
        gate_ref[k] = gate
    hit = jnp.concatenate(hits, axis=0)
    upper = lax.broadcasted_iota(jnp.int32, (width, width), 0) < lax.broadcasted_iota(jnp.int32, (width, width), 1)
    pos = dot(hit.astype(BF), jnp.where(upper, 1.0, 0.0).astype(BF), 1, 0)
    kept = jnp.where(pos < slot_cap, hit, 0.0)
    key = jnp.where(kept > 0.0, pos, -1.0)
    number = jnp.broadcast_to(jnp.sum(kept, axis=1, keepdims=True), key.shape)
    total = 8 * local
    row = lax.broadcasted_iota(jnp.int32, (total, total), 0)
    col = lax.broadcasted_iota(jnp.int32, (total, total), 1)
    rb, re, cb, ce = row // local, lax.rem(row, local), col // local, lax.rem(col, local)
    rank_row = jnp.where(re < LEAD, lax.rem(re + LEAD - 1, LEAD), re)
    rank_col = jnp.where(ce < LEAD, lax.rem(ce + LEAD - 1, LEAD), ce)
    before = jnp.logical_and(rb // 4 == cb // 4, (re < LEAD) == (ce < LEAD))
    before = jnp.logical_and(before, jnp.logical_or(rank_col < rank_row, jnp.logical_and(ce == re, cb < rb)))
    base = dot(jnp.where(before, 1.0, 0.0).astype(BF), number.astype(BF), 1, 0)
    source = lax.broadcasted_iota(jnp.int32, key.shape, 0)
    leading = lax.rem(source, local) < LEAD
    is_lead = lax.broadcasted_iota(jnp.int32, (local, width), 0) < LEAD
    lane = lax.broadcasted_iota(jnp.int32, (local, half), 1)
    slot, block = lax.rem(lane, slot_cap).astype(F32), lane // slot_cap
    for k in range(8):
        key_ref[k] = key[k * local:(k + 1) * local]
    for part in range(2):
        here = source // (4 * local) == part
        lead_rows = jnp.sum(jnp.where(jnp.logical_and(here, leading), number, 0.0), axis=0, keepdims=True)
        rest_rows = jnp.sum(jnp.where(jnp.logical_and(here, jnp.logical_not(leading)), number, 0.0), axis=0, keepdims=True)
        shift_y = jnp.where(is_lead, 0.0, jnp.maximum(lead_rows, float(Y_FIRST)))
        shift_v = jnp.where(is_lead, jnp.maximum(rest_rows, float(V_FIRST)), 0.0)
        count, start = jnp.zeros((local, half), F32), jnp.zeros((local, half), F32)
        for n in range(4):
            k = (4 * part + n) * local
            count = jnp.where(block == n, number[k:k + local, :half], count)
            start = jnp.where(block == n, base[k:k + local, :half], start)
        first = base[4 * part * local:(4 * part + 1) * local]
        for n, (shift, pack_ref) in enumerate(((shift_y, pack_y_ref), (shift_v, pack_v_ref))):
            base_ref[2 * n + part] = (first + shift).astype(jnp.int32)
            packed = jnp.where(slot < count, start + slot + shift[:, :half], -1.0)
            for e in range(local):
                pack_ref[e, part:part + 1, :] = packed[e:e + 1]

    relay(ACROSS_Y, 0)
    relay(ACROSS_X, 1)
    side_copy().start()

    def second():
        relay(ACROSS_Y, 1)
        relay(ACROSS_X, 0)

    def third():
        relay(ACROSS_XY, 0)
        relay(ACROSS_XY, 1)

    dispatch(slot_cap, gathered, key_ref, None, xs, xs_hbm, row_out,
             [second, third, lambda: arrive(CORE, CORE + 1), lambda: arrive(2, 3)])
    for c in loads:
        c.wait()

    @pl.loop(0, lead)
    def _(e):
        x = xs[e, :half]
        a = dot(x, w1[e], 1, 0)
        b = dot(x, w3[e], 1, 0)
        h = (a * jax.nn.sigmoid(a) * b).astype(BF)
        packed = dot(place(h, pack_y_ref[e, 0:1, :], Y_MOST), w2[e], 1, 0)

        @pl.when(e == 0)
        def _():
            yo[...] = packed

        @pl.when(e > 0)
        def _():
            yo[...] += packed

    stores = [pltpu.make_async_copy(yo.at[pl.ds(0, Y_FIRST)], yo_hbm, out_sem.at[0]),
              pltpu.make_async_copy(yo.at[pl.ds(Y_FIRST, Y_MOST - Y_FIRST)], spill_hbm, out_sem.at[1])]
    for c in stores:
        c.start()
    for k in others:
        aux_copy(k).wait_send()
        for part in (0, 1):
            copy(k, part).wait_send()
    side_copy().wait()
    dispatch_done(slot_cap, xs, xs_hbm, row_out)
    for c in stores:
        c.wait()


def spread_kernel(slot_cap, dout_ref, across_ref, key_ref, gate_ref, us_hbm, gathered, us, row_send, row_recv, row_out):
    _, peers = find_peers()
    meet([peers[ACROSS_X], peers[CORE]])

    def copy(slot, part):
        if slot in (ACROSS_X, CORE):
            source, peer = dout_ref.at[part], slot
        elif slot in (ACROSS_XY, 2):
            source, peer = across_ref.at[part], ACROSS_X if slot == ACROSS_XY else CORE
        else:
            source, peer = gathered.at[slot - 2, part], CORE
        return pltpu.make_async_remote_copy(source, gathered.at[slot, part], row_send.at[slot, part],
                                            row_recv.at[slot, part], device_id=peers[peer], device_id_type=MESH)

    sent = [ACROSS_X, ACROSS_XY, CORE, 2, CORE + 1, 3]
    for slot in sent[:4]:
        for part in (0, 1):
            copy(slot, part).start()
    gathered[OWN] = dout_ref[...]
    gathered[ACROSS_Y] = across_ref[...]

    def relay(slot):
        for part in (0, 1):
            copy(slot, part).wait_recv()
            copy(slot + 2, part).start()

    def arrive(*slots):
        for slot in slots:
            for part in (0, 1):
                copy(slot, part).wait_recv()

    dispatch(slot_cap, gathered, key_ref, gate_ref, us, us_hbm, row_out,
             [lambda: relay(ACROSS_X), lambda: relay(ACROSS_XY), lambda: arrive(CORE, CORE + 1), lambda: arrive(2, 3)])
    for slot in sent:
        for part in (0, 1):
            copy(slot, part).wait_send()
    dispatch_done(slot_cap, us, us_hbm, row_out)


VMEM = pl.BlockSpec(memory_space=pltpu.VMEM)
ANY = pl.BlockSpec(memory_space=pl.ANY)
DMA = pltpu.SemaphoreType.DMA


def prologue_call(tokens, d_out, ids, gates, w1, w3, w2, slot_cap):
    num_top, tok_dev = ids.shape
    width, local, f = tokens.shape[2], w1.shape[0], w1.shape[2]
    rows, aux = 8 * slot_cap, (2 * num_top, tok_dev)
    large = [((local, rows, width), BF), ((Y_FIRST, width), F32), ((Y_MOST - Y_FIRST, width), F32)]
    small = [((8, local, tok_dev), F32)] * 2 + [((local, 2, rows // 2), F32)] * 2
    small += [((4, local, tok_dev), jnp.int32), ((8,) + aux, F32), (tokens.shape, BF)]
    scratch = [((8,) + tokens.shape, BF), (aux, F32), ((8,) + aux, F32), large[0]]
    scratch += [((LEAD, width, f), BF)] * 2 + [((LEAD, f, width), BF), ((Y_MOST, width), F32)]
    return pl.pallas_call(
        functools.partial(prologue_kernel, slot_cap), name="prologue",
        in_specs=[VMEM] * 4 + [ANY] * 3,
        out_specs=[ANY] * len(large) + [VMEM] * len(small),
        out_shape=[jax.ShapeDtypeStruct(s, t) for s, t in large + small],
        scratch_shapes=[pltpu.VMEM(s, t) for s, t in scratch]
        + [DMA((8, 2)), DMA((8, 2)), DMA((8,)), DMA((8,)), DMA, DMA, DMA((3,)), DMA((2,)), DMA((4,))],
        compiler_params=pltpu.CompilerParams(collective_id=0, has_side_effects=True, vmem_limit_bytes=VMEM_LIMIT),
        cost_estimate=cost(10**10, 3 * 10**7),
    )(tokens, d_out, ids, gates, w1, w3, w2)


def spread_call(d_out, across, key, gate, slot_cap):
    local = key.shape[1]
    out = (local, 8 * slot_cap, d_out.shape[2])
    return pl.pallas_call(
        functools.partial(spread_kernel, slot_cap), name="spread",
        in_specs=[VMEM] * 4, out_specs=ANY, out_shape=jax.ShapeDtypeStruct(out, BF),
        scratch_shapes=[pltpu.VMEM((8,) + d_out.shape, BF), pltpu.VMEM(out, BF), DMA((8, 2)), DMA((8, 2)), DMA((4,))],
        compiler_params=pltpu.CompilerParams(collective_id=1, has_side_effects=True, vmem_limit_bytes=VMEM_LIMIT),
        cost_estimate=cost(10**10, 3 * 10**7),
    )(d_out, across, key, gate)


def solution(mesh):
    tp_size, ep_size = mesh.shape["tp"], mesh.shape["ep"]
    row_spec = P(("dp", "ep", "tp"), None)
    col_spec = P("ep", None, "tp")
    down_spec = P("ep", "tp", None)
    grad_col = P(("dp", "ep"), None, "tp")
    grad_down = P(("dp", "ep"), "tp", None)

    def swap(z, tp_bit, ep_bits):
        pairs = [(t * ep_size + e, (t ^ tp_bit) * ep_size + (e ^ ep_bits)) for t in range(tp_size) for e in range(ep_size)]
        return lax.ppermute(z, ("tp", "ep"), pairs)

    def local_step(tokens, expert_ids, gate_vals, w_one, w_three, w_two, d_out):
        tok_dev, width = tokens.shape
        num_top = expert_ids.shape[1]
        local = w_one.shape[0]
        experts = local * ep_size
        slot_cap = slot_count(num_top, tok_dev, experts)
        half = tp_size * ep_size * slot_cap // 2
        ep_here = lax.axis_index("ep")

        blocked = (2, tok_dev // 2, width)
        d_blocked = d_out.reshape(blocked)
        xs, y_other0, y_spill, key, gate, pack_y, pack_v, base, aux_all, across = prologue_call(
            tokens.reshape(blocked), d_blocked, expert_ids.T, gate_vals.T, w_one, w_three, w_two, slot_cap)
        y0 = swap(y_other0, 1, 0)
        base = base[:, :, 0]
        rest = local - LEAD
        act_one, act_three, hid, y_other1, y_mine = expert_call(
            fwd_kernel, 0, local, base[:2], xs, w_one, w_three, w_two, pack_y, [], [y_spill],
            [F32, F32, BF], (TOTAL - Y_FIRST, TOTAL), ())
        y1 = swap(y_other1, 1, 0)
        across = lax.optimization_barrier((across, hid))[0]
        us = spread_call(d_blocked, across, key, gate, slot_cap)

        saved = [act_one, act_three]
        spill = V_MOST - V_FIRST
        tail = TOTAL - V_FIRST
        one1, three1, v_other0, spill_other, v_mine0, spill_mine = expert_call(
            bwd_rest_kernel, LEAD, rest, base[2:], us, w_one, w_three, w_two, pack_v, saved, [],
            [BF, BF], (V_FIRST, spill, V_FIRST, spill), (V_MOST, V_MOST))
        v0 = swap(v_other0, 1, 0)
        one0, three0, v_other1, v_other2, v_other3, v_mine1 = expert_call(
            bwd_lead_kernel, 0, LEAD, base[2:], us, w_one, w_three, w_two, pack_v, saved,
            [spill_other, spill_mine], [BF, BF],
            tuple(V_CUTS[n + 1] - V_CUTS[n] for n in range(3)) + (tail,), (tail,))
        v1 = swap(v_other1, 1, 0)
        v2 = swap(v_other2, 1, 0)
        v3 = swap(v_other3, 1, 0)

        d_one = jnp.concatenate([one0, one1])
        d_three = jnp.concatenate([three0, three1])
        grads = grad_call(xs, us, hid, d_one, d_three)

        sources = jnp.stack([ep_here, ep_here ^ 2, ep_here ^ 1, ep_here ^ 3])
        all_ids = (sources[:, None] * local + jnp.arange(local)).reshape(-1)
        eq = expert_ids[:, :, None] == all_ids
        hit = jnp.any(eq, axis=1)
        lower = (jnp.arange(tok_dev)[:, None] > jnp.arange(tok_dev)[None, :]).astype(BF)
        pos = jnp.dot(lower, hit.astype(BF), preferred_element_type=F32)
        own_gate = jnp.sum(jnp.where(eq, gate_vals[:, :, None], 0.0), axis=1)
        own_pick = hit[:, :, None] & (pos[:, :, None] == jnp.arange(slot_cap, dtype=F32))
        own_mul = jnp.where(own_pick, own_gate[:, :, None], 0.0).reshape(tok_dev, ep_size, local, slot_cap)
        own_pick = own_pick.astype(BF).reshape(tok_dev, ep_size, local, slot_cap)

        def send_back(parts):
            back = [parts[0]]
            for n, bits in ((1, 2), (2, 1), (3, 3)):
                back.append(swap(parts[n], 0, bits))
            return back

        def mix(weights, back, first, count):
            flat = jnp.concatenate(back)
            weights = weights[:, :, first:first + count].reshape(tok_dev, -1)
            if weights.dtype == BF:
                return jnp.dot(weights, flat, preferred_element_type=F32)
            return jnp.dot(weights, flat.astype(F32), precision=lax.Precision.HIGHEST)

        def finish(first, count, pack, owns, pieces, recvs, weights):
            keys = pack[first:first + count, 1].reshape(count, ep_size, slot_cap).transpose(1, 0, 2).reshape(-1, 1)
            back = send_back(finish_call(owns, pieces, recvs, keys, ep_size))
            return back[0], mix(weights, back, first, count)

        def after(value, *others):
            return lax.optimization_barrier((value,) + others)[0]

        out_sum = finish(0, local, pack_y, [y_mine], [(0, 0, 0, Y_FIRST), (0, Y_FIRST, Y_FIRST, TOTAL - Y_FIRST)],
                         [y0, y1], own_mul)[1]
        piece = [(0, 0, 0, V_FIRST)] + [(1, V_CUTS[n] - V_FIRST, V_CUTS[n], V_CUTS[n + 1] - V_CUTS[n]) for n in range(3)]
        late = [(0,) + p[1:] for p in piece[1:]]
        step0, dx0 = finish(LEAD, 3, pack_v, [v_mine0], piece[:1], [v0], own_pick)
        step1, dx1 = finish(LEAD + 3, rest - 3, pack_v, [after(v_mine0, step0), v_mine1], piece[:2], [v0, v1], own_pick)
        step2, dx2 = finish(1, LEAD - 1, pack_v, [after(v_mine1, step1)], late[:2], [v1, v2], own_pick)
        dx_early = dx0 + dx1
        dx3 = finish(0, 1, pack_v, [after(v_mine1, step2, out_sum, dx_early)], late, [v1, v2, v3], own_pick)[1]
        dx_sum = dx_early + dx2 + dx3

        every = jnp.arange(experts, dtype=F32)[None, :, None]
        count_all = sum(jnp.sum(aux_all[:, j:j + 1, :] == every, axis=2, dtype=jnp.int32) for j in range(num_top))
        kept = jnp.minimum(count_all, slot_cap).reshape(2, ep_size, ep_size, local).sum(axis=1)
        lead_rows, rest_rows = kept[:, :, :LEAD].sum(axis=2), kept[:, :, LEAD:].sum(axis=2)
        y_rows = jnp.maximum(lead_rows, Y_FIRST) + rest_rows
        v_rest = jnp.maximum(rest_rows, V_FIRST)
        full = jnp.any((lead_rows > Y_MOST) | (rest_rows > V_MOST) | (y_rows > TOTAL) | (v_rest + lead_rows > TOTAL)
                       | (v_rest + lead_rows - kept[:, :, 0] > V_CUTS[2])
                       | (kept[:, :, LEAD:LEAD + 3].sum(axis=2) > V_FIRST))

        def exchange_all(args):
            hid, d_one, d_three, own_mul, own_pick = args

            def back(part):
                recv = swap(part[:, :half], 1, 0)
                done = (part[:, half:] + recv).astype(BF).reshape(local, ep_size, slot_cap, width)
                return send_back([done[:, s].reshape(-1, width) for s in range(ep_size)])

            part_out = jnp.einsum("enf,efd->end", hid, w_two, preferred_element_type=F32)
            part_dx = jnp.einsum("enf,edf->end", d_one, w_one, preferred_element_type=F32)
            part_dx += jnp.einsum("enf,edf->end", d_three, w_three, preferred_element_type=F32)
            return mix(own_mul, back(part_out), 0, local), mix(own_pick, back(part_dx), 0, local)

        def exchange_none(args):
            zero = jnp.zeros((tok_dev, width), F32)
            return zero, zero

        out_full, dx_full = lax.cond(full, exchange_all, exchange_none, (hid, d_one, d_three, own_mul, own_pick))
        out_rows = jnp.where(full, out_full, out_sum).astype(BF)
        dx_rows = jnp.where(full, dx_full, dx_sum).astype(BF)
        return out_rows, dx_rows, *grads

    return jax.shard_map(local_step, mesh=mesh,
                         in_specs=(row_spec, row_spec, row_spec, col_spec, col_spec, down_spec, row_spec),
                         out_specs=(row_spec, row_spec, grad_col, grad_col, grad_down), check_vma=False)
```

```python
import functools

import jax
import jax.numpy as jnp
from jax import lax
from jax.experimental import pallas as pl
from jax.experimental.pallas import tpu as pltpu
from jax.sharding import PartitionSpec as P


BF = jnp.bfloat16
F32 = jnp.float32
MESH = pl.DeviceIdType.MESH

LEAD = 3
TOTAL = 584
Y_FIRST, Y_MOST = 184, 240
V_FIRST, V_MOST = 280, 376
V_CUTS = (280, 384, 512, 584)
WINDOW = 104
VMEM_LIMIT = 62 * 2**20


def slot_count(num_top, tok_dev, experts):
    return 8 * ((5 * num_top * tok_dev + 32 * experts - 1) // (32 * experts))


def dot(a, b, ca, cb):
    return lax.dot_general(a, b, (((ca,), (cb,)), ((), ())), preferred_element_type=F32)


def place(rows, keys, cap):
    pick = lax.broadcasted_iota(jnp.int32, (cap, keys.shape[1]), 0).astype(F32) == keys
    return dot(jnp.where(pick, 1.0, 0.0).astype(BF), rows, 1, 0).astype(BF)


def add_window(ref, part, keys, shift, terms):
    half = keys.shape[1]
    rows = slice(part * half, (part + 1) * half)
    keys = keys[part:part + 1, :]
    first = jnp.min(jnp.where(keys >= 0.0, keys, float(TOTAL))).astype(jnp.int32)
    start = jnp.clip((first - shift) // 8 * 8, 0, ref.shape[0] - WINDOW)
    at = keys - (start + shift).astype(F32)
    product = sum(dot(place(left[rows], at, WINDOW), right, 1, dim) for left, right, dim in terms)
    ref[pl.ds(pl.multiple_of(start, 8), WINDOW), :] += product


def fwd_kernel(x_ref, w1_ref, w3_ref, w2_ref, key_ref, spill_ref, a_ref, b_ref, h_ref, other_ref, mine_ref):
    step = pl.program_id(0)

    @pl.when(step == 0)
    def _():
        mine_ref[...] = jnp.zeros_like(mine_ref)
        other_ref[...] = jnp.zeros_like(other_ref)
        other_ref[:spill_ref.shape[0], :] = spill_ref[...]

    x = x_ref[0]
    a = dot(x, w1_ref[0], 1, 0)
    b = dot(x, w3_ref[0], 1, 0)
    h = (a * jax.nn.sigmoid(a) * b).astype(BF)
    a_ref[0] = a
    b_ref[0] = b
    h_ref[0] = h
    add_window(mine_ref, 1, key_ref[0], 0, [(h, w2_ref[0], 0)])

    @pl.when(step >= LEAD)
    def _():
        add_window(other_ref, 0, key_ref[0], Y_FIRST, [(h_ref[0], w2_ref[0], 0)])


def bwd_step(shift, u_ref, w1_ref, w3_ref, w2_ref, key_ref, a_ref, b_ref, da_ref, db_ref, parts):
    dh = dot(u_ref[0], w2_ref[0], 1, 1)
    a = a_ref[0]
    s = jax.nn.sigmoid(a)
    da = (dh * b_ref[0] * s * (1.0 + a * (1.0 - s))).astype(BF)
    db = (dh * (a * s)).astype(BF)
    da_ref[0] = da
    db_ref[0] = db
    for part, ref in enumerate(parts):
        add_window(ref, part, key_ref[0], shift, [(da, w1_ref[0], 1), (db, w3_ref[0], 1)])


def cut(source, refs):
    row = 0
    for ref in refs:
        ref[...] = source[row:row + ref.shape[0]]
        row += ref.shape[0]


def bwd_rest_kernel(u_ref, w1_ref, w3_ref, w2_ref, key_ref, a_ref, b_ref, da_ref, db_ref,
                    other_ref, spill_other_ref, mine_ref, spill_mine_ref, other, mine):
    step = pl.program_id(0)

    @pl.when(step == 0)
    def _():
        other[...] = jnp.zeros_like(other)
        mine[...] = jnp.zeros_like(mine)

    bwd_step(0, u_ref, w1_ref, w3_ref, w2_ref, key_ref, a_ref, b_ref, da_ref, db_ref, (other, mine))

    @pl.when(step == pl.num_programs(0) - 1)
    def _():
        cut(other, (other_ref, spill_other_ref))
        cut(mine, (mine_ref, spill_mine_ref))


def bwd_lead_kernel(u_ref, w1_ref, w3_ref, w2_ref, key_ref, a_ref, b_ref, spill_other_ref, spill_mine_ref,
                    da_ref, db_ref, other1_ref, other2_ref, other3_ref, mine_ref, mine3_ref, other, mine):
    step = pl.program_id(0)

    @pl.when(step == 0)
    def _():
        for ref, spill_ref in ((other, spill_other_ref), (mine, spill_mine_ref)):
            ref[...] = jnp.zeros_like(ref)
            ref[:spill_ref.shape[0], :] = spill_ref[...]

    bwd_step(V_FIRST, u_ref, w1_ref, w3_ref, w2_ref, key_ref, a_ref, b_ref, da_ref, db_ref, (other, mine))

    @pl.when(step == pl.num_programs(0) - 1)
    def _():
        cut(other, (other1_ref, other2_ref, other3_ref))
        cut(mine, (mine_ref, mine3_ref))


def finish_kernel(pieces, owns, known, *refs):
    own_refs, recv_refs, key_ref = refs[:owns], refs[owns:owns + len(pieces)], refs[owns + len(pieces)]
    known_refs = refs[owns + len(pieces) + 1:][:known]
    out_refs = refs[owns + len(pieces) + 1 + known:]
    done = [(own_refs[i][row:row + count, :] + recv_ref[...]).astype(BF)
            for (i, row, _, count), recv_ref in zip(pieces, recv_refs)]
    first = 0
    for i, out_ref in enumerate(out_refs):
        rows = out_ref.shape[0]
        keys = key_ref[first:first + rows, :]
        first += rows
        total = known_refs[i][...].astype(F32) if known else None
        for (_, _, position, count), values in zip(pieces, done):
            pick = lax.broadcasted_iota(jnp.int32, (rows, count), 1).astype(F32) == keys - float(position)
            term = dot(jnp.where(pick, 1.0, 0.0).astype(BF), values, 1, 0)
            total = term if total is None else total + term
        out_ref[...] = total.astype(BF)


def grad_kernel(x_ref, u_ref, h_ref, da_ref, db_ref, g1_ref, g3_ref, g2_ref):
    x = x_ref[0]
    g1_ref[0] = dot(x, da_ref[0], 0, 0).astype(BF)
    g3_ref[0] = dot(x, db_ref[0], 0, 0).astype(BF)
    g2_ref[0] = dot(h_ref[0], u_ref[0], 0, 0).astype(BF)


def spec(shape, first):
    return pl.BlockSpec((1,) + shape, lambda i: (i + first, 0, 0))


def whole(shape):
    return pl.BlockSpec(shape, lambda i: (0,) * len(shape))


def cost(flops, nbytes):
    return pl.CostEstimate(flops=flops, bytes_accessed=nbytes, transcendentals=0)


PARAMS = pltpu.CompilerParams(dimension_semantics=("arbitrary",), vmem_limit_bytes=VMEM_LIMIT)


def expert_call(body, first, count, rows_in, w1, w3, w2, keys, saved, extra, kinds, outs, scratch):
    rows, d, f = rows_in.shape[1], w1.shape[1], w1.shape[2]
    half = rows // 2
    shapes = [((count, rows, f), t) for t in kinds] + [((n, d), F32) for n in outs]
    return pl.pallas_call(
        body, grid=(count,),
        in_specs=[spec((rows, d), first), spec((d, f), first), spec((d, f), first), spec((f, d), first),
                  spec((2, half), first)] + [spec((rows, f), first)] * len(saved) + [whole(e.shape) for e in extra],
        out_specs=[spec(s[1:], 0) if len(s) == 3 else whole(s) for s, _ in shapes],
        out_shape=[jax.ShapeDtypeStruct(s, t) for s, t in shapes],
        scratch_shapes=[pltpu.VMEM((n, d), F32) for n in scratch],
        compiler_params=PARAMS, cost_estimate=cost(count * 8 * rows * d * f, count * (6 * d * f + 6 * rows * d)),
    )(rows_in, w1, w3, w2, keys, *saved, *extra)


def grad_call(xs, us, h, da, db):
    count, rows, d = xs.shape
    f = h.shape[2]
    outs = [((d, f), BF), ((d, f), BF), ((f, d), BF)]
    return pl.pallas_call(
        grad_kernel, grid=(count,), name="wgrad",
        in_specs=[spec((rows, d), 0), spec((rows, d), 0)] + [spec((rows, f), 0)] * 3,
        out_specs=[spec(s, 0) for s, _ in outs],
        out_shape=[jax.ShapeDtypeStruct((count,) + s, t) for s, t in outs],
        compiler_params=PARAMS, cost_estimate=cost(count * 6 * rows * d * f, count * (6 * d * f + 4 * rows * d)),
    )(xs, us, h, da, db)


def finish_call(owns, pieces, recvs, keys, known, sizes):
    d = owns[0].shape[1]
    total = sum(r.shape[0] for r in recvs)
    return pl.pallas_call(
        functools.partial(finish_kernel, pieces, len(owns), len(known)), name="finish",
        out_shape=[jax.ShapeDtypeStruct((rows, d), BF) for rows in sizes],
        compiler_params=pltpu.CompilerParams(vmem_limit_bytes=VMEM_LIMIT),
        cost_estimate=cost(2 * keys.shape[0] * d * total, 8 * total * d),
    )(*owns, *recvs, keys, *known)


ACROSS_Y, ACROSS_XY, OWN, ACROSS_X, CORE = 0, 1, 4, 5, 6
STEPS = ((1, 0), (1, 2), (1, 1), (1, 3), (0, 0), (0, 2), (0, 1), (0, 3))


def find_peers():
    tp, ep = lax.axis_index("tp"), lax.axis_index("ep")
    eps = {0: ep, 2: lax.rem(ep + 2, 4), 1: ep + 1 - 2 * lax.rem(ep, 2), 3: 3 - ep}
    return ep, [{"tp": 1 - tp if a else tp, "ep": eps[b]} for a, b in STEPS]


def meet(peers):
    barrier = pltpu.get_barrier_semaphore()
    for peer in peers:
        pl.semaphore_signal(barrier, inc=1, device_id=peer, device_id_type=MESH)
    pl.semaphore_wait(barrier, len(peers))


def dispatch(slot_cap, blocks, key_ref, gate_ref, out, out_hbm, sem, ready):
    local, width = key_ref.shape[1], key_ref.shape[2]

    @pl.loop(0, 4)
    def _(n):
        for at, step in enumerate(ready):
            pl.when(n == at)(step)
        first = lax.rem(OWN + 4 * n, 8) + 2 * (n // 2)
        one, two = key_ref[first], key_ref[first + 1]
        pair = jnp.concatenate([one, jnp.where(two >= 0.0, two + slot_cap, -1.0)], axis=1)
        index = lax.broadcasted_iota(jnp.int32, (2 * slot_cap, 2 * width), 0).astype(F32)
        picks = [index == pair[e:e + 1, :] for e in range(local)]
        pick = jnp.concatenate([jnp.where(p, 1.0, 0.0) for p in picks], axis=0).astype(BF)
        rows = dot(pick, blocks[pl.ds(first, 2)].reshape(2 * width, out.shape[2]), 1, 0)
        if gate_ref is not None:
            gates = jnp.concatenate([gate_ref[first], gate_ref[first + 1]], axis=1)
            scale = jnp.concatenate([jnp.where(p, gates[e:e + 1, :], 0.0) for e, p in enumerate(picks)], axis=0)
            rows = rows * jnp.sum(scale, axis=1, keepdims=True)
        rows = rows.astype(BF)
        at = pl.ds(pl.multiple_of(first * slot_cap, 2 * slot_cap), 2 * slot_cap)
        for e in range(local):
            out[e, at, :] = rows[e * 2 * slot_cap:(e + 1) * 2 * slot_cap]
        pltpu.make_async_copy(out.at[:, at], out_hbm.at[:, at], sem.at[n]).start()


def dispatch_done(slot_cap, out, out_hbm, sem):
    for n in range(4):
        at = pl.ds(2 * slot_cap * n, 2 * slot_cap)
        pltpu.make_async_copy(out.at[:, at], out_hbm.at[:, at], sem.at[n]).wait()


def prologue_kernel(slot_cap, tok_ref, dout_ref, id_ref, val_ref, w1_hbm, w3_hbm, w2_hbm,
                    xs_hbm, yo_hbm, spill_hbm, key_ref, gate_ref, pack_y_ref, pack_v_ref, aux_all_ref, across_ref,
                    gathered, aux_ref, aux_all, xs, w1, w3, w2, yo,
                    row_send, row_recv, aux_send, aux_recv, side_send, side_recv, in_sem, out_sem, row_out):
    ep, peers = find_peers()
    others = [k for k in range(8) if k != OWN]
    local, width = key_ref.shape[1], key_ref.shape[2]
    num_top, half = id_ref.shape[0], 4 * slot_cap

    aux_ref[...] = jnp.concatenate([id_ref[...].astype(F32), val_ref[...]], axis=0)
    lead = w1.shape[0]
    loads = [pltpu.make_async_copy(w.at[pl.ds(0, lead)], buf, in_sem.at[n])
             for n, (w, buf) in enumerate(((w1_hbm, w1), (w3_hbm, w3), (w2_hbm, w2)))]
    for c in loads:
        c.start()
    meet([peers[k] for k in others])

    def aux_copy(k):
        return pltpu.make_async_remote_copy(aux_ref, aux_all.at[k], aux_send.at[k], aux_recv.at[k],
                                            device_id=peers[k], device_id_type=MESH)

    def copy(slot, part):
        if slot in (ACROSS_Y, ACROSS_X, CORE):
            source, peer = tok_ref.at[part], slot
        elif slot == ACROSS_XY:
            source, peer = (gathered.at[ACROSS_Y, 0], ACROSS_X) if part == 0 else (gathered.at[ACROSS_X, 1], ACROSS_Y)
        else:
            source, peer = gathered.at[slot - 2, part], CORE
        return pltpu.make_async_remote_copy(source, gathered.at[slot, part], row_send.at[slot, part],
                                            row_recv.at[slot, part], device_id=peers[peer], device_id_type=MESH)

    def side_copy():
        return pltpu.make_async_remote_copy(dout_ref, across_ref, side_send, side_recv,
                                            device_id=peers[ACROSS_Y], device_id_type=MESH)

    def relay(slot, part):
        copy(slot, part).wait_recv()
        if (slot, part) in ((ACROSS_Y, 0), (ACROSS_X, 1)):
            copy(ACROSS_XY, part).start()
        copy(slot + 2, part).start()

    def arrive(*slots):
        for slot in slots:
            for part in (0, 1):
                copy(slot, part).wait_recv()

    for k in others:
        aux_copy(k).start()
    for slot, part in ((ACROSS_Y, 0), (ACROSS_X, 1), (ACROSS_Y, 1), (ACROSS_X, 0), (CORE, 0), (CORE, 1)):
        copy(slot, part).start()
    gathered[OWN] = tok_ref[...]
    aux_all[OWN] = aux_ref[...]

    for k in others:
        aux_copy(k).wait_recv()
    aux_all_ref[...] = aux_all[...]
    expert = (lax.broadcasted_iota(jnp.int32, (local, width), 0) + ep * local).astype(F32)
    hits = []
    for k in range(8):
        a = aux_all[k]
        hit, gate = jnp.zeros((local, width), F32), jnp.zeros((local, width), F32)
        for j in range(num_top):
            eq = a[j:j + 1, :] == expert
            hit = jnp.where(eq, 1.0, hit)
            gate = jnp.where(eq, a[num_top + j:num_top + j + 1, :], gate)
        hits.append(hit)
        gate_ref[k] = gate
    hit = jnp.concatenate(hits, axis=0)
    upper = lax.broadcasted_iota(jnp.int32, (width, width), 0) < lax.broadcasted_iota(jnp.int32, (width, width), 1)
    pos = dot(hit.astype(BF), jnp.where(upper, 1.0, 0.0).astype(BF), 1, 0)
    kept = jnp.where(pos < slot_cap, hit, 0.0)
    key = jnp.where(kept > 0.0, pos, -1.0)
    number = jnp.broadcast_to(jnp.sum(kept, axis=1, keepdims=True), key.shape)
    total = 8 * local
    row = lax.broadcasted_iota(jnp.int32, (total, total), 0)
    col = lax.broadcasted_iota(jnp.int32, (total, total), 1)
    rb, re, cb, ce = row // local, lax.rem(row, local), col // local, lax.rem(col, local)
    rank_row = jnp.where(re < LEAD, lax.rem(re + LEAD - 1, LEAD), re)
    rank_col = jnp.where(ce < LEAD, lax.rem(ce + LEAD - 1, LEAD), ce)
    before = jnp.logical_and(rb // 4 == cb // 4, (re < LEAD) == (ce < LEAD))
    before = jnp.logical_and(before, jnp.logical_or(rank_col < rank_row, jnp.logical_and(ce == re, cb < rb)))
    base = dot(jnp.where(before, 1.0, 0.0).astype(BF), number.astype(BF), 1, 0)
    source = lax.broadcasted_iota(jnp.int32, key.shape, 0)
    leading = lax.rem(source, local) < LEAD
    is_lead = lax.broadcasted_iota(jnp.int32, (local, width), 0) < LEAD
    lane = lax.broadcasted_iota(jnp.int32, (local, half), 1)
    slot, block = lax.rem(lane, slot_cap).astype(F32), lane // slot_cap
    for k in range(8):
        key_ref[k] = key[k * local:(k + 1) * local]
    for part in range(2):
        here = source // (4 * local) == part
        lead_rows = jnp.sum(jnp.where(jnp.logical_and(here, leading), number, 0.0), axis=0, keepdims=True)
        rest_rows = jnp.sum(jnp.where(jnp.logical_and(here, jnp.logical_not(leading)), number, 0.0), axis=0, keepdims=True)
        shift_y = jnp.where(is_lead, 0.0, jnp.maximum(lead_rows, float(Y_FIRST)))
        shift_v = jnp.where(is_lead, jnp.maximum(rest_rows, float(V_FIRST)), 0.0)
        count, start = jnp.zeros((local, half), F32), jnp.zeros((local, half), F32)
        for n in range(4):
            k = (4 * part + n) * local
            count = jnp.where(block == n, number[k:k + local, :half], count)
            start = jnp.where(block == n, base[k:k + local, :half], start)
        for shift, pack_ref in ((shift_y, pack_y_ref), (shift_v, pack_v_ref)):
            packed = jnp.where(slot < count, start + slot + shift[:, :half], -1.0)
            for e in range(local):
                pack_ref[e, part:part + 1, :] = packed[e:e + 1]

    relay(ACROSS_Y, 0)
    relay(ACROSS_X, 1)
    side_copy().start()

    def second():
        relay(ACROSS_Y, 1)
        relay(ACROSS_X, 0)

    def third():
        relay(ACROSS_XY, 0)
        relay(ACROSS_XY, 1)

    dispatch(slot_cap, gathered, key_ref, None, xs, xs_hbm, row_out,
             [second, third, lambda: arrive(CORE, CORE + 1), lambda: arrive(2, 3)])
    for c in loads:
        c.wait()

    @pl.loop(0, lead)
    def _(e):
        x = xs[e, :half]
        a = dot(x, w1[e], 1, 0)
        b = dot(x, w3[e], 1, 0)
        h = (a * jax.nn.sigmoid(a) * b).astype(BF)
        packed = dot(place(h, pack_y_ref[e, 0:1, :], Y_MOST), w2[e], 1, 0)

        @pl.when(e == 0)
        def _():
            yo[...] = packed

        @pl.when(e > 0)
        def _():
            yo[...] += packed

    stores = [pltpu.make_async_copy(yo.at[pl.ds(0, Y_FIRST)], yo_hbm, out_sem.at[0]),
              pltpu.make_async_copy(yo.at[pl.ds(Y_FIRST, Y_MOST - Y_FIRST)], spill_hbm, out_sem.at[1])]
    for c in stores:
        c.start()
    for k in others:
        aux_copy(k).wait_send()
        for part in (0, 1):
            copy(k, part).wait_send()
    side_copy().wait()
    dispatch_done(slot_cap, xs, xs_hbm, row_out)
    for c in stores:
        c.wait()


def spread_kernel(slot_cap, dout_ref, across_ref, key_ref, gate_ref, us_hbm, gathered, us, row_send, row_recv, row_out):
    _, peers = find_peers()
    meet([peers[ACROSS_X], peers[CORE]])

    def copy(slot, part):
        if slot in (ACROSS_X, CORE):
            source, peer = dout_ref.at[part], slot
        elif slot in (ACROSS_XY, 2):
            source, peer = across_ref.at[part], ACROSS_X if slot == ACROSS_XY else CORE
        else:
            source, peer = gathered.at[slot - 2, part], CORE
        return pltpu.make_async_remote_copy(source, gathered.at[slot, part], row_send.at[slot, part],
                                            row_recv.at[slot, part], device_id=peers[peer], device_id_type=MESH)

    sent = [ACROSS_X, ACROSS_XY, CORE, 2, CORE + 1, 3]
    for slot in sent[:4]:
        for part in (0, 1):
            copy(slot, part).start()
    gathered[OWN] = dout_ref[...]
    gathered[ACROSS_Y] = across_ref[...]

    def relay(slot):
        for part in (0, 1):
            copy(slot, part).wait_recv()
            copy(slot + 2, part).start()

    def arrive(*slots):
        for slot in slots:
            for part in (0, 1):
                copy(slot, part).wait_recv()

    dispatch(slot_cap, gathered, key_ref, gate_ref, us, us_hbm, row_out,
             [lambda: relay(ACROSS_X), lambda: relay(ACROSS_XY), lambda: arrive(CORE, CORE + 1), lambda: arrive(2, 3)])
    for slot in sent:
        for part in (0, 1):
            copy(slot, part).wait_send()
    dispatch_done(slot_cap, us, us_hbm, row_out)


VMEM = pl.BlockSpec(memory_space=pltpu.VMEM)
ANY = pl.BlockSpec(memory_space=pl.ANY)
DMA = pltpu.SemaphoreType.DMA


def prologue_call(tokens, d_out, ids, gates, w1, w3, w2, slot_cap):
    num_top, tok_dev = ids.shape
    width, local, f = tokens.shape[2], w1.shape[0], w1.shape[2]
    rows, aux = 8 * slot_cap, (2 * num_top, tok_dev)
    large = [((local, rows, width), BF), ((Y_FIRST, width), F32), ((Y_MOST - Y_FIRST, width), F32)]
    small = [((8, local, tok_dev), F32)] * 2 + [((local, 2, rows // 2), F32)] * 2
    small += [((8,) + aux, F32), (tokens.shape, BF)]
    scratch = [((8,) + tokens.shape, BF), (aux, F32), ((8,) + aux, F32), large[0]]
    scratch += [((LEAD, width, f), BF)] * 2 + [((LEAD, f, width), BF), ((Y_MOST, width), F32)]
    return pl.pallas_call(
        functools.partial(prologue_kernel, slot_cap), name="prologue",
        in_specs=[VMEM] * 4 + [ANY] * 3,
        out_specs=[ANY] * len(large) + [VMEM] * len(small),
        out_shape=[jax.ShapeDtypeStruct(s, t) for s, t in large + small],
        scratch_shapes=[pltpu.VMEM(s, t) for s, t in scratch]
        + [DMA((8, 2)), DMA((8, 2)), DMA((8,)), DMA((8,)), DMA, DMA, DMA((3,)), DMA((2,)), DMA((4,))],
        compiler_params=pltpu.CompilerParams(collective_id=0, has_side_effects=True, vmem_limit_bytes=VMEM_LIMIT),
        cost_estimate=cost(10**10, 3 * 10**7),
    )(tokens, d_out, ids, gates, w1, w3, w2)


def spread_call(d_out, across, key, gate, slot_cap):
    local = key.shape[1]
    out = (local, 8 * slot_cap, d_out.shape[2])
    return pl.pallas_call(
        functools.partial(spread_kernel, slot_cap), name="spread",
        in_specs=[VMEM] * 4, out_specs=ANY, out_shape=jax.ShapeDtypeStruct(out, BF),
        scratch_shapes=[pltpu.VMEM((8,) + d_out.shape, BF), pltpu.VMEM(out, BF), DMA((8, 2)), DMA((8, 2)), DMA((4,))],
        compiler_params=pltpu.CompilerParams(collective_id=1, has_side_effects=True, vmem_limit_bytes=VMEM_LIMIT),
        cost_estimate=cost(10**10, 3 * 10**7),
    )(d_out, across, key, gate)


def solution(mesh):
    tp_size, ep_size = mesh.shape["tp"], mesh.shape["ep"]
    row_spec = P(("dp", "ep", "tp"), None)
    col_spec = P("ep", None, "tp")
    down_spec = P("ep", "tp", None)
    grad_col = P(("dp", "ep"), None, "tp")
    grad_down = P(("dp", "ep"), "tp", None)

    def swap(z, tp_bit, ep_bits):
        pairs = [(t * ep_size + e, (t ^ tp_bit) * ep_size + (e ^ ep_bits)) for t in range(tp_size) for e in range(ep_size)]
        return lax.ppermute(z, ("tp", "ep"), pairs)

    def local_step(tokens, expert_ids, gate_vals, w_one, w_three, w_two, d_out):
        tok_dev, width = tokens.shape
        num_top = expert_ids.shape[1]
        local = w_one.shape[0]
        experts = local * ep_size
        slot_cap = slot_count(num_top, tok_dev, experts)
        half = tp_size * ep_size * slot_cap // 2
        ep_here = lax.axis_index("ep")

        blocked = (2, tok_dev // 2, width)
        d_blocked = d_out.reshape(blocked)
        xs, y_other0, y_spill, key, gate, pack_y, pack_v, aux_all, across = prologue_call(
            tokens.reshape(blocked), d_blocked, expert_ids.T, gate_vals.T, w_one, w_three, w_two, slot_cap)
        y0 = swap(y_other0, 1, 0)
        rest = local - LEAD
        act_one, act_three, hid, y_other1, y_mine = expert_call(
            fwd_kernel, 0, local, xs, w_one, w_three, w_two, pack_y, [], [y_spill],
            [F32, F32, BF], (TOTAL - Y_FIRST, TOTAL), ())
        y1 = swap(y_other1, 1, 0)
        across = lax.optimization_barrier((across, hid))[0]
        us = spread_call(d_blocked, across, key, gate, slot_cap)

        saved = [act_one, act_three]
        spill = V_MOST - V_FIRST
        tail = TOTAL - V_FIRST
        one1, three1, v_other0, spill_other, v_mine0, spill_mine = expert_call(
            bwd_rest_kernel, LEAD, rest, us, w_one, w_three, w_two, pack_v, saved, [],
            [BF, BF], (V_FIRST, spill, V_FIRST, spill), (V_MOST, V_MOST))
        v0 = swap(v_other0, 1, 0)
        one0, three0, v_other1, v_other2, v_other3, v_mine1, v_mine3 = expert_call(
            bwd_lead_kernel, 0, LEAD, us, w_one, w_three, w_two, pack_v, saved,
            [spill_other, spill_mine], [BF, BF],
            tuple(V_CUTS[n + 1] - V_CUTS[n] for n in range(3)) + (V_CUTS[2] - V_FIRST, TOTAL - V_CUTS[2]), (tail, tail))
        v1 = swap(v_other1, 1, 0)
        v2 = swap(v_other2, 1, 0)
        v3 = swap(v_other3, 1, 0)

        d_one = jnp.concatenate([one0, one1])
        d_three = jnp.concatenate([three0, three1])
        grads = grad_call(xs, us, hid, d_one, d_three)

        sources = jnp.stack([ep_here, ep_here ^ 2, ep_here ^ 1, ep_here ^ 3])
        all_ids = (sources[:, None] * local + jnp.arange(local)).reshape(-1)
        eq = expert_ids[:, :, None] == all_ids
        hit = jnp.any(eq, axis=1)
        lower = (jnp.arange(tok_dev)[:, None] > jnp.arange(tok_dev)[None, :]).astype(BF)
        pos = jnp.dot(lower, hit.astype(BF), preferred_element_type=F32)
        own_gate = jnp.sum(jnp.where(eq, gate_vals[:, :, None], 0.0), axis=1)
        own_pick = hit[:, :, None] & (pos[:, :, None] == jnp.arange(slot_cap, dtype=F32))
        own_mul = jnp.where(own_pick, own_gate[:, :, None], 0.0).reshape(tok_dev, ep_size, local, slot_cap)
        own_pick = own_pick.astype(BF).reshape(tok_dev, ep_size, local, slot_cap)

        def send_back(parts):
            back = [parts[0]]
            for n, bits in ((1, 2), (2, 1), (3, 3)):
                back.append(swap(parts[n], 0, bits))
            return back

        def mix(weights, back, first, count):
            flat = jnp.concatenate(back)
            weights = weights[:, :, first:first + count].reshape(tok_dev, -1)
            if weights.dtype == BF:
                return jnp.dot(weights, flat, preferred_element_type=F32)
            return jnp.dot(weights, flat.astype(F32), precision=lax.Precision.HIGHEST)

        def slots_of(pack, first, count):
            return pack[first:first + count, 1].reshape(count, ep_size, slot_cap).transpose(1, 0, 2).reshape(-1, 1)

        def after(value, *others):
            return lax.optimization_barrier((value,) + others)[0]

        def finish(first, count, pack, owns, pieces, recvs, known=(), early=0):
            keys = [slots_of(pack, first, count)] + [slots_of(pack, 0, early)] * (early > 0)
            sizes = [count * slot_cap] * ep_size + [early * slot_cap] * (ep_size * (early > 0))
            out = finish_call(owns, pieces, recvs, jnp.concatenate(keys), known, sizes)
            back = send_back(out[:ep_size])
            return back, out[ep_size:]

        y_back, _ = finish(0, local, pack_y, [y_mine],
                           [(0, 0, 0, Y_FIRST), (0, Y_FIRST, Y_FIRST, TOTAL - Y_FIRST)], [y0, y1])
        piece = [(0, 0, 0, V_FIRST)] + [(1, V_CUTS[n] - V_FIRST, V_CUTS[n], V_CUTS[n + 1] - V_CUTS[n]) for n in range(2)]
        late = [(0,) + p[1:] for p in piece[1:]]
        last = [(0, 0, V_CUTS[2], TOTAL - V_CUTS[2])]
        back0, _ = finish(LEAD, 3, pack_v, [v_mine0], piece[:1], [v0])
        back1, _ = finish(LEAD + 3, rest - 3, pack_v, [after(v_mine0, back0[0]), v_mine1], piece[:2], [v0, v1])
        back2, known = finish(1, LEAD - 1, pack_v, [after(v_mine1, back1[0])], late, [v1, v2], early=1)
        out_sum = mix(own_mul, y_back, 0, local)
        dx_early = mix(own_pick, back0, LEAD, 3) + mix(own_pick, back1, LEAD + 3, rest - 3)
        back3, _ = finish(0, 1, pack_v, [after(v_mine3, out_sum, dx_early)], last, [v3], known=known)
        dx_early = mix(own_pick, back2, 1, LEAD - 1) + dx_early
        dx_sum = mix(own_pick, after(tuple(back3), dx_early), 0, 1) + dx_early

        every = jnp.arange(experts, dtype=F32)[None, :, None]
        count_all = sum(jnp.sum(aux_all[:, j:j + 1, :] == every, axis=2, dtype=jnp.int32) for j in range(num_top))
        kept = jnp.minimum(count_all, slot_cap).reshape(2, ep_size, ep_size, local).sum(axis=1)
        lead_rows, rest_rows = kept[:, :, :LEAD].sum(axis=2), kept[:, :, LEAD:].sum(axis=2)
        y_rows = jnp.maximum(lead_rows, Y_FIRST) + rest_rows
        v_rest = jnp.maximum(rest_rows, V_FIRST)
        full = jnp.any((lead_rows > Y_MOST) | (rest_rows > V_MOST) | (y_rows > TOTAL) | (v_rest + lead_rows > TOTAL)
                       | (v_rest + lead_rows - kept[:, :, 0] > V_CUTS[2])
                       | (kept[:, :, LEAD:LEAD + 3].sum(axis=2) > V_FIRST))

        def exchange_all(args):
            hid, d_one, d_three, own_mul, own_pick = args

            def back(part):
                recv = swap(part[:, :half], 1, 0)
                done = (part[:, half:] + recv).astype(BF).reshape(local, ep_size, slot_cap, width)
                return send_back([done[:, s].reshape(-1, width) for s in range(ep_size)])

            part_out = jnp.einsum("enf,efd->end", hid, w_two, preferred_element_type=F32)
            part_dx = jnp.einsum("enf,edf->end", d_one, w_one, preferred_element_type=F32)
            part_dx += jnp.einsum("enf,edf->end", d_three, w_three, preferred_element_type=F32)
            return mix(own_mul, back(part_out), 0, local), mix(own_pick, back(part_dx), 0, local)

        def exchange_none(args):
            zero = jnp.zeros((tok_dev, width), F32)
            return zero, zero

        out_full, dx_full = lax.cond(full, exchange_all, exchange_none, (hid, d_one, d_three, own_mul, own_pick))
        out_rows = jnp.where(full, out_full, out_sum).astype(BF)
        dx_rows = jnp.where(full, dx_full, dx_sum).astype(BF)
        return out_rows, dx_rows, *grads

    return jax.shard_map(local_step, mesh=mesh,
                         in_specs=(row_spec, row_spec, row_spec, col_spec, col_spec, down_spec, row_spec),
                         out_specs=(row_spec, row_spec, grad_col, grad_col, grad_down), check_vma=False)
```

```python
import functools

import jax
import jax.numpy as jnp
from jax import lax
from jax.experimental import pallas as pl
from jax.experimental.pallas import tpu as pltpu
from jax.sharding import PartitionSpec as P


BF = jnp.bfloat16
F32 = jnp.float32
MESH = pl.DeviceIdType.MESH

LEAD = 3
TOTAL = 584
Y_FIRST, Y_MOST = 184, 240
V_FIRST, V_MOST = 280, 376
V_CUTS = (280, 384, 512, 584)
WINDOW = 104
VMEM_LIMIT = 62 * 2**20


def slot_count(num_top, tok_dev, experts):
    return 8 * ((5 * num_top * tok_dev + 32 * experts - 1) // (32 * experts))


def dot(a, b, ca, cb):
    return lax.dot_general(a, b, (((ca,), (cb,)), ((), ())), preferred_element_type=F32)


def place(rows, keys, cap):
    pick = lax.broadcasted_iota(jnp.int32, (cap, keys.shape[1]), 0).astype(F32) == keys
    return dot(jnp.where(pick, 1.0, 0.0).astype(BF), rows, 1, 0).astype(BF)


def add_window(ref, part, keys, shift, terms):
    half = keys.shape[1]
    rows = slice(part * half, (part + 1) * half)
    keys = keys[part:part + 1, :]
    first = jnp.min(jnp.where(keys >= 0.0, keys, float(TOTAL))).astype(jnp.int32)
    start = jnp.clip((first - shift) // 8 * 8, 0, ref.shape[0] - WINDOW)
    at = keys - (start + shift).astype(F32)
    product = sum(dot(place(left[rows], at, WINDOW), right, 1, dim) for left, right, dim in terms)
    ref[pl.ds(pl.multiple_of(start, 8), WINDOW), :] += product


def fwd_kernel(x_ref, w1_ref, w3_ref, w2_ref, key_ref, spill_ref, a_ref, b_ref, h_ref, other_ref, mine_ref):
    step = pl.program_id(0)

    @pl.when(step == 0)
    def _():
        mine_ref[...] = jnp.zeros_like(mine_ref)
        other_ref[...] = jnp.zeros_like(other_ref)
        other_ref[:spill_ref.shape[0], :] = spill_ref[...]

    x = x_ref[0]
    a = dot(x, w1_ref[0], 1, 0)
    b = dot(x, w3_ref[0], 1, 0)
    h = (a * jax.nn.sigmoid(a) * b).astype(BF)
    a_ref[0] = a
    b_ref[0] = b
    h_ref[0] = h
    add_window(mine_ref, 1, key_ref[0], 0, [(h, w2_ref[0], 0)])

    @pl.when(step >= LEAD)
    def _():
        add_window(other_ref, 0, key_ref[0], Y_FIRST, [(h_ref[0], w2_ref[0], 0)])


def bwd_step(shift, u_ref, w1_ref, w3_ref, w2_ref, key_ref, a_ref, b_ref, da_ref, db_ref, parts):
    dh = dot(u_ref[0], w2_ref[0], 1, 1)
    a = a_ref[0]
    s = jax.nn.sigmoid(a)
    da = (dh * b_ref[0] * s * (1.0 + a * (1.0 - s))).astype(BF)
    db = (dh * (a * s)).astype(BF)
    da_ref[0] = da
    db_ref[0] = db
    for part, ref in enumerate(parts):
        add_window(ref, part, key_ref[0], shift, [(da, w1_ref[0], 1), (db, w3_ref[0], 1)])


def cut(source, refs):
    row = 0
    for ref in refs:
        ref[...] = source[row:row + ref.shape[0]]
        row += ref.shape[0]


def bwd_rest_kernel(u_ref, w1_ref, w3_ref, w2_ref, key_ref, a_ref, b_ref, da_ref, db_ref,
                    other_ref, spill_other_ref, mine_ref, spill_mine_ref, other, mine):
    step = pl.program_id(0)

    @pl.when(step == 0)
    def _():
        other[...] = jnp.zeros_like(other)
        mine[...] = jnp.zeros_like(mine)

    bwd_step(0, u_ref, w1_ref, w3_ref, w2_ref, key_ref, a_ref, b_ref, da_ref, db_ref, (other, mine))

    @pl.when(step == pl.num_programs(0) - 1)
    def _():
        cut(other, (other_ref, spill_other_ref))
        cut(mine, (mine_ref, spill_mine_ref))


def bwd_lead_kernel(u_ref, w1_ref, w3_ref, w2_ref, key_ref, a_ref, b_ref, spill_other_ref, spill_mine_ref,
                    da_ref, db_ref, other1_ref, other2_ref, other3_ref, mine_ref, mine3_ref, other, mine):
    step = pl.program_id(0)

    @pl.when(step == 0)
    def _():
        for ref, spill_ref in ((other, spill_other_ref), (mine, spill_mine_ref)):
            ref[...] = jnp.zeros_like(ref)
            ref[:spill_ref.shape[0], :] = spill_ref[...]

    bwd_step(V_FIRST, u_ref, w1_ref, w3_ref, w2_ref, key_ref, a_ref, b_ref, da_ref, db_ref, (other, mine))

    @pl.when(step == pl.num_programs(0) - 1)
    def _():
        cut(other, (other1_ref, other2_ref, other3_ref))
        cut(mine, (mine_ref, mine3_ref))


def finish_kernel(pieces, owns, known, *refs):
    own_refs, recv_refs, key_ref = refs[:owns], refs[owns:owns + len(pieces)], refs[owns + len(pieces)]
    known_refs = refs[owns + len(pieces) + 1:][:known]
    out_refs = refs[owns + len(pieces) + 1 + known:]
    done = [(own_refs[i][row:row + count, :] + recv_ref[...]).astype(BF)
            for (i, row, _, count), recv_ref in zip(pieces, recv_refs)]
    first = 0
    for i, out_ref in enumerate(out_refs):
        rows = out_ref.shape[0]
        keys = key_ref[first:first + rows, :]
        first += rows
        total = known_refs[i][...].astype(F32) if known else None
        for (_, _, position, count), values in zip(pieces, done):
            pick = lax.broadcasted_iota(jnp.int32, (rows, count), 1).astype(F32) == keys - float(position)
            term = dot(jnp.where(pick, 1.0, 0.0).astype(BF), values, 1, 0)
            total = term if total is None else total + term
        out_ref[...] = total.astype(BF)


def grad_kernel(x_ref, u_ref, h_ref, da_ref, db_ref, g1_ref, g3_ref, g2_ref):
    x = x_ref[0]
    g1_ref[0] = dot(x, da_ref[0], 0, 0).astype(BF)
    g3_ref[0] = dot(x, db_ref[0], 0, 0).astype(BF)
    g2_ref[0] = dot(h_ref[0], u_ref[0], 0, 0).astype(BF)


def spec(shape, first):
    return pl.BlockSpec((1,) + shape, lambda i: (i + first, 0, 0))


def whole(shape):
    return pl.BlockSpec(shape, lambda i: (0,) * len(shape))


def cost(flops, nbytes):
    return pl.CostEstimate(flops=flops, bytes_accessed=nbytes, transcendentals=0)


PARAMS = pltpu.CompilerParams(dimension_semantics=("arbitrary",), vmem_limit_bytes=VMEM_LIMIT)


def expert_call(body, first, count, rows_in, w1, w3, w2, keys, saved, extra, kinds, outs, scratch):
    rows, d, f = rows_in.shape[1], w1.shape[1], w1.shape[2]
    half = rows // 2
    shapes = [((count, rows, f), t) for t in kinds] + [((n, d), F32) for n in outs]
    return pl.pallas_call(
        body, grid=(count,),
        in_specs=[spec((rows, d), first), spec((d, f), first), spec((d, f), first), spec((f, d), first),
                  spec((2, half), first)] + [spec((rows, f), first)] * len(saved) + [whole(e.shape) for e in extra],
        out_specs=[spec(s[1:], 0) if len(s) == 3 else whole(s) for s, _ in shapes],
        out_shape=[jax.ShapeDtypeStruct(s, t) for s, t in shapes],
        scratch_shapes=[pltpu.VMEM((n, d), F32) for n in scratch],
        compiler_params=PARAMS, cost_estimate=cost(count * 8 * rows * d * f, count * (6 * d * f + 6 * rows * d)),
    )(rows_in, w1, w3, w2, keys, *saved, *extra)


def grad_call(xs, us, h, da, db):
    count, rows, d = xs.shape
    f = h.shape[2]
    outs = [((d, f), BF), ((d, f), BF), ((f, d), BF)]
    return pl.pallas_call(
        grad_kernel, grid=(count,), name="wgrad",
        in_specs=[spec((rows, d), 0), spec((rows, d), 0)] + [spec((rows, f), 0)] * 3,
        out_specs=[spec(s, 0) for s, _ in outs],
        out_shape=[jax.ShapeDtypeStruct((count,) + s, t) for s, t in outs],
        compiler_params=PARAMS, cost_estimate=cost(count * 6 * rows * d * f, count * (6 * d * f + 4 * rows * d)),
    )(xs, us, h, da, db)


def finish_call(owns, pieces, recvs, keys, known, sizes):
    d = owns[0].shape[1]
    total = sum(r.shape[0] for r in recvs)
    return pl.pallas_call(
        functools.partial(finish_kernel, pieces, len(owns), len(known)), name="finish",
        out_shape=[jax.ShapeDtypeStruct((rows, d), BF) for rows in sizes],
        compiler_params=pltpu.CompilerParams(vmem_limit_bytes=VMEM_LIMIT),
        cost_estimate=cost(2 * keys.shape[0] * d * total, 8 * total * d),
    )(*owns, *recvs, keys, *known)


ACROSS_Y, ACROSS_XY, OWN, ACROSS_X, CORE = 0, 1, 4, 5, 6
STEPS = ((1, 0), (1, 2), (1, 1), (1, 3), (0, 0), (0, 2), (0, 1), (0, 3))


def find_peers():
    tp, ep = lax.axis_index("tp"), lax.axis_index("ep")
    eps = {0: ep, 2: lax.rem(ep + 2, 4), 1: ep + 1 - 2 * lax.rem(ep, 2), 3: 3 - ep}
    return ep, [{"tp": 1 - tp if a else tp, "ep": eps[b]} for a, b in STEPS]


def meet(peers):
    barrier = pltpu.get_barrier_semaphore()
    for peer in peers:
        pl.semaphore_signal(barrier, inc=1, device_id=peer, device_id_type=MESH)
    pl.semaphore_wait(barrier, len(peers))


def dispatch(slot_cap, blocks, key_ref, gate_ref, out, out_hbm, sem, ready):
    local, width = key_ref.shape[1], key_ref.shape[2]

    @pl.loop(0, 4)
    def _(n):
        for at, step in enumerate(ready):
            pl.when(n == at)(step)
        first = lax.rem(OWN + 4 * n, 8) + 2 * (n // 2)
        one, two = key_ref[first], key_ref[first + 1]
        pair = jnp.concatenate([one, jnp.where(two >= 0.0, two + slot_cap, -1.0)], axis=1)
        index = lax.broadcasted_iota(jnp.int32, (2 * slot_cap, 2 * width), 0).astype(F32)
        picks = [index == pair[e:e + 1, :] for e in range(local)]
        pick = jnp.concatenate([jnp.where(p, 1.0, 0.0) for p in picks], axis=0).astype(BF)
        rows = dot(pick, blocks[pl.ds(first, 2)].reshape(2 * width, out.shape[2]), 1, 0)
        if gate_ref is not None:
            gates = jnp.concatenate([gate_ref[first], gate_ref[first + 1]], axis=1)
            scale = jnp.concatenate([jnp.where(p, gates[e:e + 1, :], 0.0) for e, p in enumerate(picks)], axis=0)
            rows = rows * jnp.sum(scale, axis=1, keepdims=True)
        rows = rows.astype(BF)
        at = pl.ds(pl.multiple_of(first * slot_cap, 2 * slot_cap), 2 * slot_cap)
        for e in range(local):
            out[e, at, :] = rows[e * 2 * slot_cap:(e + 1) * 2 * slot_cap]
        pltpu.make_async_copy(out.at[:, at], out_hbm.at[:, at], sem.at[n]).start()


def dispatch_done(slot_cap, out, out_hbm, sem):
    for n in range(4):
        at = pl.ds(2 * slot_cap * n, 2 * slot_cap)
        pltpu.make_async_copy(out.at[:, at], out_hbm.at[:, at], sem.at[n]).wait()


def prologue_kernel(slot_cap, tok_ref, dout_ref, id_ref, val_ref, w1_hbm, w3_hbm, w2_hbm,
                    xs_hbm, yo_hbm, spill_hbm, key_ref, gate_ref, pack_y_ref, pack_v_ref, aux_all_ref, across_ref,
                    gathered, aux_ref, aux_all, xs, w13, w2, yo,
                    row_send, row_recv, aux_send, aux_recv, side_send, side_recv, in_sem, out_sem, row_out):
    ep, peers = find_peers()
    others = [k for k in range(8) if k != OWN]
    local, width = key_ref.shape[1], key_ref.shape[2]
    num_top, half = id_ref.shape[0], 4 * slot_cap

    aux_ref[...] = jnp.concatenate([id_ref[...].astype(F32), val_ref[...]], axis=0)
    lead, hidden = w2.shape[0], w2.shape[1]
    loads = [pltpu.make_async_copy(w.at[pl.ds(0, lead)], buf, in_sem.at[n]) for n, (w, buf) in enumerate(
        ((w1_hbm, w13.at[:, :, pl.ds(0, hidden)]), (w3_hbm, w13.at[:, :, pl.ds(hidden, hidden)]), (w2_hbm, w2)))]
    for c in loads:
        c.start()
    meet([peers[k] for k in others])

    def aux_copy(k):
        return pltpu.make_async_remote_copy(aux_ref, aux_all.at[k], aux_send.at[k], aux_recv.at[k],
                                            device_id=peers[k], device_id_type=MESH)

    def copy(slot, part):
        if slot in (ACROSS_Y, ACROSS_X, CORE):
            source, peer = tok_ref.at[part], slot
        elif slot == ACROSS_XY:
            source, peer = (gathered.at[ACROSS_Y, 0], ACROSS_X) if part == 0 else (gathered.at[ACROSS_X, 1], ACROSS_Y)
        else:
            source, peer = gathered.at[slot - 2, part], CORE
        return pltpu.make_async_remote_copy(source, gathered.at[slot, part], row_send.at[slot, part],
                                            row_recv.at[slot, part], device_id=peers[peer], device_id_type=MESH)

    def side_copy():
        return pltpu.make_async_remote_copy(dout_ref, across_ref, side_send, side_recv,
                                            device_id=peers[ACROSS_Y], device_id_type=MESH)

    def relay(slot, part):
        copy(slot, part).wait_recv()
        if (slot, part) in ((ACROSS_Y, 0), (ACROSS_X, 1)):
            copy(ACROSS_XY, part).start()
        copy(slot + 2, part).start()

    def arrive(*slots):
        for slot in slots:
            for part in (0, 1):
                copy(slot, part).wait_recv()

    for k in others:
        aux_copy(k).start()
    for slot, part in ((ACROSS_Y, 0), (ACROSS_X, 1), (ACROSS_Y, 1), (ACROSS_X, 0), (CORE, 0), (CORE, 1)):
        copy(slot, part).start()
    gathered[OWN] = tok_ref[...]
    aux_all[OWN] = aux_ref[...]

    for k in others:
        aux_copy(k).wait_recv()
    aux_all_ref[...] = aux_all[...]
    expert = (lax.broadcasted_iota(jnp.int32, (local, width), 0) + ep * local).astype(F32)
    hits = []
    for k in range(8):
        a = aux_all[k]
        hit, gate = jnp.zeros((local, width), F32), jnp.zeros((local, width), F32)
        for j in range(num_top):
            eq = a[j:j + 1, :] == expert
            hit = jnp.where(eq, 1.0, hit)
            gate = jnp.where(eq, a[num_top + j:num_top + j + 1, :], gate)
        hits.append(hit)
        gate_ref[k] = gate
    hit = jnp.concatenate(hits, axis=0)
    upper = lax.broadcasted_iota(jnp.int32, (width, width), 0) < lax.broadcasted_iota(jnp.int32, (width, width), 1)
    pos = dot(hit.astype(BF), jnp.where(upper, 1.0, 0.0).astype(BF), 1, 0)
    kept = jnp.where(pos < slot_cap, hit, 0.0)
    key = jnp.where(kept > 0.0, pos, -1.0)
    number = jnp.broadcast_to(jnp.sum(kept, axis=1, keepdims=True), key.shape)
    total = 8 * local
    row = lax.broadcasted_iota(jnp.int32, (total, total), 0)
    col = lax.broadcasted_iota(jnp.int32, (total, total), 1)
    rb, re, cb, ce = row // local, lax.rem(row, local), col // local, lax.rem(col, local)
    rank_row = jnp.where(re < LEAD, lax.rem(re + LEAD - 1, LEAD), re)
    rank_col = jnp.where(ce < LEAD, lax.rem(ce + LEAD - 1, LEAD), ce)
    before = jnp.logical_and(rb // 4 == cb // 4, (re < LEAD) == (ce < LEAD))
    before = jnp.logical_and(before, jnp.logical_or(rank_col < rank_row, jnp.logical_and(ce == re, cb < rb)))
    base = dot(jnp.where(before, 1.0, 0.0).astype(BF), number.astype(BF), 1, 0)
    source = lax.broadcasted_iota(jnp.int32, key.shape, 0)
    leading = lax.rem(source, local) < LEAD
    is_lead = lax.broadcasted_iota(jnp.int32, (local, width), 0) < LEAD
    lane = lax.broadcasted_iota(jnp.int32, (local, half), 1)
    slot, block = lax.rem(lane, slot_cap).astype(F32), lane // slot_cap
    for k in range(8):
        key_ref[k] = key[k * local:(k + 1) * local]
    for part in range(2):
        here = source // (4 * local) == part
        lead_rows = jnp.sum(jnp.where(jnp.logical_and(here, leading), number, 0.0), axis=0, keepdims=True)
        rest_rows = jnp.sum(jnp.where(jnp.logical_and(here, jnp.logical_not(leading)), number, 0.0), axis=0, keepdims=True)
        shift_y = jnp.where(is_lead, 0.0, jnp.maximum(lead_rows, float(Y_FIRST)))
        shift_v = jnp.where(is_lead, jnp.maximum(rest_rows, float(V_FIRST)), 0.0)
        count, start = jnp.zeros((local, half), F32), jnp.zeros((local, half), F32)
        for n in range(4):
            k = (4 * part + n) * local
            count = jnp.where(block == n, number[k:k + local, :half], count)
            start = jnp.where(block == n, base[k:k + local, :half], start)
        for shift, pack_ref in ((shift_y, pack_y_ref), (shift_v, pack_v_ref)):
            packed = jnp.where(slot < count, start + slot + shift[:, :half], -1.0)
            for e in range(local):
                pack_ref[e, part:part + 1, :] = packed[e:e + 1]

    relay(ACROSS_Y, 0)
    relay(ACROSS_X, 1)
    side_copy().start()

    def second():
        relay(ACROSS_Y, 1)
        relay(ACROSS_X, 0)

    def third():
        relay(ACROSS_XY, 0)
        relay(ACROSS_XY, 1)

    dispatch(slot_cap, gathered, key_ref, None, xs, xs_hbm, row_out,
             [second, third, lambda: arrive(CORE, CORE + 1), lambda: arrive(2, 3)])
    for c in loads:
        c.wait()

    @pl.loop(0, lead)
    def _(e):
        act = dot(xs[e, :half], w13[e], 1, 0)
        a, b = act[:, :hidden], act[:, hidden:]
        h = (a * jax.nn.sigmoid(a) * b).astype(BF)
        packed = dot(place(h, pack_y_ref[e, 0:1, :], Y_MOST), w2[e], 1, 0)

        @pl.when(e == 0)
        def _():
            yo[...] = packed

        @pl.when(e > 0)
        def _():
            yo[...] += packed

    stores = [pltpu.make_async_copy(yo.at[pl.ds(0, Y_FIRST)], yo_hbm, out_sem.at[0]),
              pltpu.make_async_copy(yo.at[pl.ds(Y_FIRST, Y_MOST - Y_FIRST)], spill_hbm, out_sem.at[1])]
    for c in stores:
        c.start()
    for k in others:
        aux_copy(k).wait_send()
        for part in (0, 1):
            copy(k, part).wait_send()
    side_copy().wait()
    dispatch_done(slot_cap, xs, xs_hbm, row_out)
    for c in stores:
        c.wait()


def spread_kernel(slot_cap, dout_ref, across_ref, key_ref, gate_ref, us_hbm, gathered, us, row_send, row_recv, row_out):
    _, peers = find_peers()
    meet([peers[ACROSS_X], peers[CORE]])

    def copy(slot, part):
        if slot in (ACROSS_X, CORE):
            source, peer = dout_ref.at[part], slot
        elif slot in (ACROSS_XY, 2):
            source, peer = across_ref.at[part], ACROSS_X if slot == ACROSS_XY else CORE
        else:
            source, peer = gathered.at[slot - 2, part], CORE
        return pltpu.make_async_remote_copy(source, gathered.at[slot, part], row_send.at[slot, part],
                                            row_recv.at[slot, part], device_id=peers[peer], device_id_type=MESH)

    sent = [ACROSS_X, ACROSS_XY, CORE, 2, CORE + 1, 3]
    for slot in sent[:4]:
        for part in (0, 1):
            copy(slot, part).start()
    gathered[OWN] = dout_ref[...]
    gathered[ACROSS_Y] = across_ref[...]

    def relay(slot):
        for part in (0, 1):
            copy(slot, part).wait_recv()
            copy(slot + 2, part).start()

    def arrive(*slots):
        for slot in slots:
            for part in (0, 1):
                copy(slot, part).wait_recv()

    dispatch(slot_cap, gathered, key_ref, gate_ref, us, us_hbm, row_out,
             [lambda: relay(ACROSS_X), lambda: relay(ACROSS_XY), lambda: arrive(CORE, CORE + 1), lambda: arrive(2, 3)])
    for slot in sent:
        for part in (0, 1):
            copy(slot, part).wait_send()
    dispatch_done(slot_cap, us, us_hbm, row_out)


VMEM = pl.BlockSpec(memory_space=pltpu.VMEM)
ANY = pl.BlockSpec(memory_space=pl.ANY)
DMA = pltpu.SemaphoreType.DMA


def prologue_call(tokens, d_out, ids, gates, w1, w3, w2, slot_cap):
    num_top, tok_dev = ids.shape
    width, local, f = tokens.shape[2], w1.shape[0], w1.shape[2]
    rows, aux = 8 * slot_cap, (2 * num_top, tok_dev)
    large = [((local, rows, width), BF), ((Y_FIRST, width), F32), ((Y_MOST - Y_FIRST, width), F32)]
    small = [((8, local, tok_dev), F32)] * 2 + [((local, 2, rows // 2), F32)] * 2
    small += [((8,) + aux, F32), (tokens.shape, BF)]
    scratch = [((8,) + tokens.shape, BF), (aux, F32), ((8,) + aux, F32), large[0]]
    scratch += [((LEAD, width, 2 * f), BF), ((LEAD, f, width), BF), ((Y_MOST, width), F32)]
    return pl.pallas_call(
        functools.partial(prologue_kernel, slot_cap), name="prologue",
        in_specs=[VMEM] * 4 + [ANY] * 3,
        out_specs=[ANY] * len(large) + [VMEM] * len(small),
        out_shape=[jax.ShapeDtypeStruct(s, t) for s, t in large + small],
        scratch_shapes=[pltpu.VMEM(s, t) for s, t in scratch]
        + [DMA((8, 2)), DMA((8, 2)), DMA((8,)), DMA((8,)), DMA, DMA, DMA((3,)), DMA((2,)), DMA((4,))],
        compiler_params=pltpu.CompilerParams(collective_id=0, has_side_effects=True, vmem_limit_bytes=VMEM_LIMIT),
        cost_estimate=cost(10**10, 3 * 10**7),
    )(tokens, d_out, ids, gates, w1, w3, w2)


def spread_call(d_out, across, key, gate, slot_cap):
    local = key.shape[1]
    out = (local, 8 * slot_cap, d_out.shape[2])
    return pl.pallas_call(
        functools.partial(spread_kernel, slot_cap), name="spread",
        in_specs=[VMEM] * 4, out_specs=ANY, out_shape=jax.ShapeDtypeStruct(out, BF),
        scratch_shapes=[pltpu.VMEM((8,) + d_out.shape, BF), pltpu.VMEM(out, BF), DMA((8, 2)), DMA((8, 2)), DMA((4,))],
        compiler_params=pltpu.CompilerParams(collective_id=1, has_side_effects=True, vmem_limit_bytes=VMEM_LIMIT),
        cost_estimate=cost(10**10, 3 * 10**7),
    )(d_out, across, key, gate)


def solution(mesh):
    tp_size, ep_size = mesh.shape["tp"], mesh.shape["ep"]
    row_spec = P(("dp", "ep", "tp"), None)
    col_spec = P("ep", None, "tp")
    down_spec = P("ep", "tp", None)
    grad_col = P(("dp", "ep"), None, "tp")
    grad_down = P(("dp", "ep"), "tp", None)

    def swap(z, tp_bit, ep_bits):
        pairs = [(t * ep_size + e, (t ^ tp_bit) * ep_size + (e ^ ep_bits)) for t in range(tp_size) for e in range(ep_size)]
        return lax.ppermute(z, ("tp", "ep"), pairs)

    def local_step(tokens, expert_ids, gate_vals, w_one, w_three, w_two, d_out):
        tok_dev, width = tokens.shape
        num_top = expert_ids.shape[1]
        local = w_one.shape[0]
        experts = local * ep_size
        slot_cap = slot_count(num_top, tok_dev, experts)
        half = tp_size * ep_size * slot_cap // 2
        ep_here = lax.axis_index("ep")

        blocked = (2, tok_dev // 2, width)
        d_blocked = d_out.reshape(blocked)
        xs, y_other0, y_spill, key, gate, pack_y, pack_v, aux_all, across = prologue_call(
            tokens.reshape(blocked), d_blocked, expert_ids.T, gate_vals.T, w_one, w_three, w_two, slot_cap)
        y0 = swap(y_other0, 1, 0)
        rest = local - LEAD
        act_one, act_three, hid, y_other1, y_mine = expert_call(
            fwd_kernel, 0, local, xs, w_one, w_three, w_two, pack_y, [], [y_spill],
            [F32, F32, BF], (TOTAL - Y_FIRST, TOTAL), ())
        y1 = swap(y_other1, 1, 0)
        across = lax.optimization_barrier((across, hid))[0]
        us = spread_call(d_blocked, across, key, gate, slot_cap)

        saved = [act_one, act_three]
        spill = V_MOST - V_FIRST
        tail = TOTAL - V_FIRST
        one1, three1, v_other0, spill_other, v_mine0, spill_mine = expert_call(
            bwd_rest_kernel, LEAD, rest, us, w_one, w_three, w_two, pack_v, saved, [],
            [BF, BF], (V_FIRST, spill, V_FIRST, spill), (V_MOST, V_MOST))
        v0 = swap(v_other0, 1, 0)
        one0, three0, v_other1, v_other2, v_other3, v_mine1, v_mine3 = expert_call(
            bwd_lead_kernel, 0, LEAD, us, w_one, w_three, w_two, pack_v, saved,
            [spill_other, spill_mine], [BF, BF],
            tuple(V_CUTS[n + 1] - V_CUTS[n] for n in range(3)) + (V_CUTS[2] - V_FIRST, TOTAL - V_CUTS[2]), (tail, tail))
        v1 = swap(v_other1, 1, 0)
        v2 = swap(v_other2, 1, 0)
        v3 = swap(v_other3, 1, 0)

        d_one = jnp.concatenate([one0, one1])
        d_three = jnp.concatenate([three0, three1])
        grads = grad_call(xs, us, hid, d_one, d_three)

        sources = jnp.stack([ep_here, ep_here ^ 2, ep_here ^ 1, ep_here ^ 3])
        all_ids = (sources[:, None] * local + jnp.arange(local)).reshape(-1)
        eq = expert_ids[:, :, None] == all_ids
        hit = jnp.any(eq, axis=1)
        lower = (jnp.arange(tok_dev)[:, None] > jnp.arange(tok_dev)[None, :]).astype(BF)
        pos = jnp.dot(lower, hit.astype(BF), preferred_element_type=F32)
        own_gate = jnp.sum(jnp.where(eq, gate_vals[:, :, None], 0.0), axis=1)
        own_pick = hit[:, :, None] & (pos[:, :, None] == jnp.arange(slot_cap, dtype=F32))
        own_mul = jnp.where(own_pick, own_gate[:, :, None], 0.0).reshape(tok_dev, ep_size, local, slot_cap)
        own_pick = own_pick.astype(BF).reshape(tok_dev, ep_size, local, slot_cap)

        def send_back(parts):
            back = [parts[0]]
            for n, bits in ((1, 2), (2, 1), (3, 3)):
                back.append(swap(parts[n], 0, bits))
            return back

        def mix(weights, back, first, count):
            flat = jnp.concatenate(back)
            weights = weights[:, :, first:first + count].reshape(tok_dev, -1)
            if weights.dtype == BF:
                return jnp.dot(weights, flat, preferred_element_type=F32)
            return jnp.dot(weights, flat.astype(F32), precision=lax.Precision.HIGHEST)

        def slots_of(pack, first, count):
            return pack[first:first + count, 1].reshape(count, ep_size, slot_cap).transpose(1, 0, 2).reshape(-1, 1)

        def after(value, *others):
            return lax.optimization_barrier((value,) + others)[0]

        def finish(first, count, pack, owns, pieces, recvs, known=(), early=0):
            keys = [slots_of(pack, first, count)] + [slots_of(pack, 0, early)] * (early > 0)
            sizes = [count * slot_cap] * ep_size + [early * slot_cap] * (ep_size * (early > 0))
            out = finish_call(owns, pieces, recvs, jnp.concatenate(keys), known, sizes)
            back = send_back(out[:ep_size])
            return back, out[ep_size:]

        y_back, _ = finish(0, local, pack_y, [y_mine],
                           [(0, 0, 0, Y_FIRST), (0, Y_FIRST, Y_FIRST, TOTAL - Y_FIRST)], [y0, y1])
        piece = [(0, 0, 0, V_FIRST)] + [(1, V_CUTS[n] - V_FIRST, V_CUTS[n], V_CUTS[n + 1] - V_CUTS[n]) for n in range(2)]
        late = [(0,) + p[1:] for p in piece[1:]]
        last = [(0, 0, V_CUTS[2], TOTAL - V_CUTS[2])]
        back0, _ = finish(LEAD, 3, pack_v, [v_mine0], piece[:1], [v0])
        back1, _ = finish(LEAD + 3, rest - 3, pack_v, [after(v_mine0, back0[0]), v_mine1], piece[:2], [v0, v1])
        out_sum = mix(own_mul, y_back, 0, local)
        dx_early = mix(own_pick, back0, LEAD, 3)
        back2, known = finish(1, LEAD - 1, pack_v, [after(v_mine1, back1[0], out_sum, dx_early)], late, [v1, v2], early=1)
        dx_early = dx_early + mix(own_pick, back1, LEAD + 3, rest - 3)
        back3, _ = finish(0, 1, pack_v, [after(v_mine3, dx_early)], last, [v3], known=known)
        dx_early = mix(own_pick, back2, 1, LEAD - 1) + dx_early
        dx_sum = mix(own_pick, after(tuple(back3), dx_early), 0, 1) + dx_early

        every = jnp.arange(experts, dtype=F32)[None, :, None]
        count_all = sum(jnp.sum(aux_all[:, j:j + 1, :] == every, axis=2, dtype=jnp.int32) for j in range(num_top))
        kept = jnp.minimum(count_all, slot_cap).reshape(2, ep_size, ep_size, local).sum(axis=1)
        lead_rows, rest_rows = kept[:, :, :LEAD].sum(axis=2), kept[:, :, LEAD:].sum(axis=2)
        y_rows = jnp.maximum(lead_rows, Y_FIRST) + rest_rows
        v_rest = jnp.maximum(rest_rows, V_FIRST)
        full = jnp.any((lead_rows > Y_MOST) | (rest_rows > V_MOST) | (y_rows > TOTAL) | (v_rest + lead_rows > TOTAL)
                       | (v_rest + lead_rows - kept[:, :, 0] > V_CUTS[2])
                       | (kept[:, :, LEAD:LEAD + 3].sum(axis=2) > V_FIRST))

        def exchange_all(args):
            hid, d_one, d_three, own_mul, own_pick = args

            def back(part):
                recv = swap(part[:, :half], 1, 0)
                done = (part[:, half:] + recv).astype(BF).reshape(local, ep_size, slot_cap, width)
                return send_back([done[:, s].reshape(-1, width) for s in range(ep_size)])

            part_out = jnp.einsum("enf,efd->end", hid, w_two, preferred_element_type=F32)
            part_dx = jnp.einsum("enf,edf->end", d_one, w_one, preferred_element_type=F32)
            part_dx += jnp.einsum("enf,edf->end", d_three, w_three, preferred_element_type=F32)
            return mix(own_mul, back(part_out), 0, local), mix(own_pick, back(part_dx), 0, local)

        def exchange_none(args):
            zero = jnp.zeros((tok_dev, width), F32)
            return zero, zero

        out_full, dx_full = lax.cond(full, exchange_all, exchange_none, (hid, d_one, d_three, own_mul, own_pick))
        out_rows = jnp.where(full, out_full, out_sum).astype(BF)
        dx_rows = jnp.where(full, dx_full, dx_sum).astype(BF)
        return out_rows, dx_rows, *grads

    return jax.shard_map(local_step, mesh=mesh,
                         in_specs=(row_spec, row_spec, row_spec, col_spec, col_spec, down_spec, row_spec),
                         out_specs=(row_spec, row_spec, grad_col, grad_col, grad_down), check_vma=False)
```

```python
import functools

import jax
import jax.numpy as jnp
from jax import lax
from jax.experimental import pallas as pl
from jax.experimental.pallas import tpu as pltpu
from jax.sharding import PartitionSpec as P


BF = jnp.bfloat16
F32 = jnp.float32
MESH = pl.DeviceIdType.MESH

LEAD = 3
USUAL, TOTAL = 552, 616
Y_FIRST, Y_MOST = 184, 240
V_FIRST, V_MOST = 280, 376
V_CUTS = (280, 384, 512, 552, 616)
WINDOW = 104
VMEM_LIMIT = 62 * 2**20


def slot_count(num_top, tok_dev, experts):
    return 8 * ((5 * num_top * tok_dev + 32 * experts - 1) // (32 * experts))


def dot(a, b, ca, cb):
    return lax.dot_general(a, b, (((ca,), (cb,)), ((), ())), preferred_element_type=F32)


def place(rows, keys, cap):
    pick = lax.broadcasted_iota(jnp.int32, (cap, keys.shape[1]), 0).astype(F32) == keys
    return dot(jnp.where(pick, 1.0, 0.0).astype(BF), rows, 1, 0).astype(BF)


def add_window(ref, part, keys, shift, terms):
    half = keys.shape[1]
    rows = slice(part * half, (part + 1) * half)
    keys = keys[part:part + 1, :]
    first = jnp.min(jnp.where(keys >= 0.0, keys, float(TOTAL))).astype(jnp.int32)
    start = jnp.clip((first - shift) // 8 * 8, 0, ref.shape[0] - WINDOW)
    at = keys - (start + shift).astype(F32)
    product = sum(dot(place(left[rows], at, WINDOW), right, 1, dim) for left, right, dim in terms)
    ref[pl.ds(pl.multiple_of(start, 8), WINDOW), :] += product


def cut(source, refs):
    row = 0
    for ref in refs:
        ref[...] = source[row:row + ref.shape[0]]
        row += ref.shape[0]


def fwd_kernel(x_ref, w1_ref, w3_ref, w2_ref, key_ref, spill_ref, a_ref, b_ref, h_ref, other_ref, extra_ref, mine_ref, other):
    step = pl.program_id(0)

    @pl.when(step == 0)
    def _():
        mine_ref[...] = jnp.zeros_like(mine_ref)
        other[...] = jnp.zeros_like(other)
        other[:spill_ref.shape[0], :] = spill_ref[...]

    x = x_ref[0]
    a = dot(x, w1_ref[0], 1, 0)
    b = dot(x, w3_ref[0], 1, 0)
    h = (a * jax.nn.sigmoid(a) * b).astype(BF)
    a_ref[0] = a
    b_ref[0] = b
    h_ref[0] = h
    add_window(mine_ref, 1, key_ref[0], 0, [(h, w2_ref[0], 0)])

    @pl.when(step >= LEAD)
    def _():
        add_window(other, 0, key_ref[0], Y_FIRST, [(h_ref[0], w2_ref[0], 0)])

    @pl.when(step == pl.num_programs(0) - 1)
    def _():
        cut(other, (other_ref, extra_ref))


def bwd_step(shift, u_ref, w1_ref, w3_ref, w2_ref, key_ref, a_ref, b_ref, da_ref, db_ref, parts):
    dh = dot(u_ref[0], w2_ref[0], 1, 1)
    a = a_ref[0]
    s = jax.nn.sigmoid(a)
    da = (dh * b_ref[0] * s * (1.0 + a * (1.0 - s))).astype(BF)
    db = (dh * (a * s)).astype(BF)
    da_ref[0] = da
    db_ref[0] = db
    for part, ref in enumerate(parts):
        add_window(ref, part, key_ref[0], shift, [(da, w1_ref[0], 1), (db, w3_ref[0], 1)])


def bwd_rest_kernel(u_ref, w1_ref, w3_ref, w2_ref, key_ref, a_ref, b_ref, da_ref, db_ref,
                    other_ref, spill_other_ref, mine_ref, spill_mine_ref, other, mine):
    step = pl.program_id(0)

    @pl.when(step == 0)
    def _():
        other[...] = jnp.zeros_like(other)
        mine[...] = jnp.zeros_like(mine)

    bwd_step(0, u_ref, w1_ref, w3_ref, w2_ref, key_ref, a_ref, b_ref, da_ref, db_ref, (other, mine))

    @pl.when(step == pl.num_programs(0) - 1)
    def _():
        cut(other, (other_ref, spill_other_ref))
        cut(mine, (mine_ref, spill_mine_ref))


def bwd_lead_kernel(u_ref, w1_ref, w3_ref, w2_ref, key_ref, a_ref, b_ref, spill_other_ref, spill_mine_ref,
                    da_ref, db_ref, other1_ref, other2_ref, other3_ref, extra_ref, mine_ref, mine3_ref, other, mine):
    step = pl.program_id(0)

    @pl.when(step == 0)
    def _():
        for ref, spill_ref in ((other, spill_other_ref), (mine, spill_mine_ref)):
            ref[...] = jnp.zeros_like(ref)
            ref[:spill_ref.shape[0], :] = spill_ref[...]

    bwd_step(V_FIRST, u_ref, w1_ref, w3_ref, w2_ref, key_ref, a_ref, b_ref, da_ref, db_ref, (other, mine))

    @pl.when(step == pl.num_programs(0) - 1)
    def _():
        cut(other, (other1_ref, other2_ref, other3_ref, extra_ref))
        cut(mine, (mine_ref, mine3_ref))


def finish_kernel(pieces, owns, known, *refs):
    own_refs, recv_refs, key_ref = refs[:owns], refs[owns:owns + len(pieces)], refs[owns + len(pieces)]
    known_refs = refs[owns + len(pieces) + 1:][:known]
    out_refs = refs[owns + len(pieces) + 1 + known:]
    done = [(own_refs[i][row:row + count, :] + recv_ref[...]).astype(BF)
            for (i, row, _, count), recv_ref in zip(pieces, recv_refs)]
    total = None
    for (_, _, position, count), values in zip(pieces, done):
        pick = lax.broadcasted_iota(jnp.int32, (key_ref.shape[0], count), 1).astype(F32) == key_ref[...] - float(position)
        term = dot(jnp.where(pick, 1.0, 0.0).astype(BF), values, 1, 0)
        total = term if total is None else total + term
    first = 0
    for i, out_ref in enumerate(out_refs):
        rows = total[first:first + out_ref.shape[0]]
        first += out_ref.shape[0]
        if known:
            rows = rows + known_refs[i][...].astype(F32)
        out_ref[...] = rows.astype(BF)


def grad_kernel(x_ref, u_ref, h_ref, da_ref, db_ref, g1_ref, g3_ref, g2_ref):
    x = x_ref[0]
    g1_ref[0] = dot(x, da_ref[0], 0, 0).astype(BF)
    g3_ref[0] = dot(x, db_ref[0], 0, 0).astype(BF)
    g2_ref[0] = dot(h_ref[0], u_ref[0], 0, 0).astype(BF)


def spec(shape, first):
    return pl.BlockSpec((1,) + shape, lambda i: (i + first, 0, 0))


def whole(shape):
    return pl.BlockSpec(shape, lambda i: (0,) * len(shape))


def cost(flops, nbytes):
    return pl.CostEstimate(flops=flops, bytes_accessed=nbytes, transcendentals=0)


PARAMS = pltpu.CompilerParams(dimension_semantics=("arbitrary",), vmem_limit_bytes=VMEM_LIMIT)


def expert_call(body, first, count, rows_in, w1, w3, w2, keys, saved, extra, kinds, outs, scratch):
    rows, d, f = rows_in.shape[1], w1.shape[1], w1.shape[2]
    half = rows // 2
    shapes = [((count, rows, f), t) for t in kinds] + [((n, d), F32) for n in outs]
    return pl.pallas_call(
        body, grid=(count,),
        in_specs=[spec((rows, d), first), spec((d, f), first), spec((d, f), first), spec((f, d), first),
                  spec((2, half), first)] + [spec((rows, f), first)] * len(saved) + [whole(e.shape) for e in extra],
        out_specs=[spec(s[1:], 0) if len(s) == 3 else whole(s) for s, _ in shapes],
        out_shape=[jax.ShapeDtypeStruct(s, t) for s, t in shapes],
        scratch_shapes=[pltpu.VMEM((n, d), F32) for n in scratch],
        compiler_params=PARAMS, cost_estimate=cost(count * 8 * rows * d * f, count * (6 * d * f + 6 * rows * d)),
    )(rows_in, w1, w3, w2, keys, *saved, *extra)


def grad_call(xs, us, h, da, db):
    count, rows, d = xs.shape
    f = h.shape[2]
    outs = [((d, f), BF), ((d, f), BF), ((f, d), BF)]
    return pl.pallas_call(
        grad_kernel, grid=(count,), name="wgrad",
        in_specs=[spec((rows, d), 0), spec((rows, d), 0)] + [spec((rows, f), 0)] * 3,
        out_specs=[spec(s, 0) for s, _ in outs],
        out_shape=[jax.ShapeDtypeStruct((count,) + s, t) for s, t in outs],
        compiler_params=PARAMS, cost_estimate=cost(count * 6 * rows * d * f, count * (6 * d * f + 4 * rows * d)),
    )(xs, us, h, da, db)


def finish_call(owns, pieces, recvs, keys, known, sizes):
    d = owns[0].shape[1]
    total = sum(r.shape[0] for r in recvs)
    return pl.pallas_call(
        functools.partial(finish_kernel, pieces, len(owns), len(known)), name="finish",
        out_shape=[jax.ShapeDtypeStruct((rows, d), BF) for rows in sizes],
        compiler_params=pltpu.CompilerParams(vmem_limit_bytes=VMEM_LIMIT),
        cost_estimate=cost(2 * keys.shape[0] * d * total, 8 * total * d),
    )(*owns, *recvs, keys, *known)


ACROSS_Y, ACROSS_XY, OWN, ACROSS_X, CORE = 0, 1, 4, 5, 6
STEPS = ((1, 0), (1, 2), (1, 1), (1, 3), (0, 0), (0, 2), (0, 1), (0, 3))


def find_peers():
    tp, ep = lax.axis_index("tp"), lax.axis_index("ep")
    eps = {0: ep, 2: lax.rem(ep + 2, 4), 1: ep + 1 - 2 * lax.rem(ep, 2), 3: 3 - ep}
    return ep, [{"tp": 1 - tp if a else tp, "ep": eps[b]} for a, b in STEPS]


def meet(peers):
    barrier = pltpu.get_barrier_semaphore()
    for peer in peers:
        pl.semaphore_signal(barrier, inc=1, device_id=peer, device_id_type=MESH)
    pl.semaphore_wait(barrier, len(peers))


def dispatch(slot_cap, blocks, key_ref, gate_ref, out, out_hbm, sem, ready):
    local, width = key_ref.shape[1], key_ref.shape[2]

    @pl.loop(0, 4)
    def _(n):
        for at, step in enumerate(ready):
            pl.when(n == at)(step)
        first = lax.rem(OWN + 4 * n, 8) + 2 * (n // 2)
        one, two = key_ref[first], key_ref[first + 1]
        pair = jnp.concatenate([one, jnp.where(two >= 0.0, two + slot_cap, -1.0)], axis=1)
        index = lax.broadcasted_iota(jnp.int32, (2 * slot_cap, 2 * width), 0).astype(F32)
        picks = [index == pair[e:e + 1, :] for e in range(local)]
        pick = jnp.concatenate([jnp.where(p, 1.0, 0.0) for p in picks], axis=0).astype(BF)
        rows = dot(pick, blocks[pl.ds(first, 2)].reshape(2 * width, out.shape[2]), 1, 0)
        if gate_ref is not None:
            gates = jnp.concatenate([gate_ref[first], gate_ref[first + 1]], axis=1)
            scale = jnp.concatenate([jnp.where(p, gates[e:e + 1, :], 0.0) for e, p in enumerate(picks)], axis=0)
            rows = rows * jnp.sum(scale, axis=1, keepdims=True)
        rows = rows.astype(BF)
        at = pl.ds(pl.multiple_of(first * slot_cap, 2 * slot_cap), 2 * slot_cap)
        for e in range(local):
            out[e, at, :] = rows[e * 2 * slot_cap:(e + 1) * 2 * slot_cap]
        pltpu.make_async_copy(out.at[:, at], out_hbm.at[:, at], sem.at[n]).start()


def dispatch_done(slot_cap, out, out_hbm, sem):
    for n in range(4):
        at = pl.ds(2 * slot_cap * n, 2 * slot_cap)
        pltpu.make_async_copy(out.at[:, at], out_hbm.at[:, at], sem.at[n]).wait()


def prologue_kernel(slot_cap, tok_ref, dout_ref, id_ref, val_ref, w1_hbm, w3_hbm, w2_hbm,
                    xs_hbm, yo_hbm, spill_hbm, key_ref, gate_ref, pack_y_ref, pack_v_ref, aux_all_ref, across_ref,
                    gathered, aux_ref, aux_all, xs, w13, w2, yo,
                    row_send, row_recv, aux_send, aux_recv, side_send, side_recv, in_sem, out_sem, row_out):
    ep, peers = find_peers()
    others = [k for k in range(8) if k != OWN]
    local, width = key_ref.shape[1], key_ref.shape[2]
    num_top, half = id_ref.shape[0], 4 * slot_cap

    aux_ref[...] = jnp.concatenate([id_ref[...].astype(F32), val_ref[...]], axis=0)
    lead, hidden = w2.shape[0], w2.shape[1]
    loads = [pltpu.make_async_copy(w.at[pl.ds(0, lead)], buf, in_sem.at[n]) for n, (w, buf) in enumerate(
        ((w1_hbm, w13.at[:, :, pl.ds(0, hidden)]), (w3_hbm, w13.at[:, :, pl.ds(hidden, hidden)]), (w2_hbm, w2)))]
    for c in loads:
        c.start()
    meet([peers[k] for k in others])

    def aux_copy(k):
        return pltpu.make_async_remote_copy(aux_ref, aux_all.at[k], aux_send.at[k], aux_recv.at[k],
                                            device_id=peers[k], device_id_type=MESH)

    def copy(slot, part):
        if slot in (ACROSS_Y, ACROSS_X, CORE):
            source, peer = tok_ref.at[part], slot
        elif slot == ACROSS_XY:
            source, peer = (gathered.at[ACROSS_Y, 0], ACROSS_X) if part == 0 else (gathered.at[ACROSS_X, 1], ACROSS_Y)
        else:
            source, peer = gathered.at[slot - 2, part], CORE
        return pltpu.make_async_remote_copy(source, gathered.at[slot, part], row_send.at[slot, part],
                                            row_recv.at[slot, part], device_id=peers[peer], device_id_type=MESH)

    def side_copy():
        return pltpu.make_async_remote_copy(dout_ref, across_ref, side_send, side_recv,
                                            device_id=peers[ACROSS_Y], device_id_type=MESH)

    def relay(slot, part):
        copy(slot, part).wait_recv()
        if (slot, part) in ((ACROSS_Y, 0), (ACROSS_X, 1)):
            copy(ACROSS_XY, part).start()
        copy(slot + 2, part).start()

    def arrive(*slots):
        for slot in slots:
            for part in (0, 1):
                copy(slot, part).wait_recv()

    for k in others:
        aux_copy(k).start()
    for slot, part in ((ACROSS_Y, 0), (ACROSS_X, 1), (ACROSS_Y, 1), (ACROSS_X, 0), (CORE, 0), (CORE, 1)):
        copy(slot, part).start()
    gathered[OWN] = tok_ref[...]
    aux_all[OWN] = aux_ref[...]

    for k in others:
        aux_copy(k).wait_recv()
    aux_all_ref[...] = aux_all[...]
    expert = (lax.broadcasted_iota(jnp.int32, (local, width), 0) + ep * local).astype(F32)
    hits = []
    for k in range(8):
        a = aux_all[k]
        hit, gate = jnp.zeros((local, width), F32), jnp.zeros((local, width), F32)
        for j in range(num_top):
            eq = a[j:j + 1, :] == expert
            hit = jnp.where(eq, 1.0, hit)
            gate = jnp.where(eq, a[num_top + j:num_top + j + 1, :], gate)
        hits.append(hit)
        gate_ref[k] = gate
    hit = jnp.concatenate(hits, axis=0)
    upper = lax.broadcasted_iota(jnp.int32, (width, width), 0) < lax.broadcasted_iota(jnp.int32, (width, width), 1)
    pos = dot(hit.astype(BF), jnp.where(upper, 1.0, 0.0).astype(BF), 1, 0)
    kept = jnp.where(pos < slot_cap, hit, 0.0)
    key = jnp.where(kept > 0.0, pos, -1.0)
    number = jnp.broadcast_to(jnp.sum(kept, axis=1, keepdims=True), key.shape)
    total = 8 * local
    row = lax.broadcasted_iota(jnp.int32, (total, total), 0)
    col = lax.broadcasted_iota(jnp.int32, (total, total), 1)
    rb, re, cb, ce = row // local, lax.rem(row, local), col // local, lax.rem(col, local)
    rank_row = jnp.where(re < LEAD, lax.rem(re + LEAD - 1, LEAD), re)
    rank_col = jnp.where(ce < LEAD, lax.rem(ce + LEAD - 1, LEAD), ce)
    before = jnp.logical_and(rb // 4 == cb // 4, (re < LEAD) == (ce < LEAD))
    before = jnp.logical_and(before, jnp.logical_or(rank_col < rank_row, jnp.logical_and(ce == re, cb < rb)))
    base = dot(jnp.where(before, 1.0, 0.0).astype(BF), number.astype(BF), 1, 0)
    source = lax.broadcasted_iota(jnp.int32, key.shape, 0)
    leading = lax.rem(source, local) < LEAD
    is_lead = lax.broadcasted_iota(jnp.int32, (local, width), 0) < LEAD
    lane = lax.broadcasted_iota(jnp.int32, (local, half), 1)
    slot, block = lax.rem(lane, slot_cap).astype(F32), lane // slot_cap
    for k in range(8):
        key_ref[k] = key[k * local:(k + 1) * local]
    for part in range(2):
        here = source // (4 * local) == part
        lead_rows = jnp.sum(jnp.where(jnp.logical_and(here, leading), number, 0.0), axis=0, keepdims=True)
        rest_rows = jnp.sum(jnp.where(jnp.logical_and(here, jnp.logical_not(leading)), number, 0.0), axis=0, keepdims=True)
        shift_y = jnp.where(is_lead, 0.0, jnp.maximum(lead_rows, float(Y_FIRST)))
        shift_v = jnp.where(is_lead, jnp.maximum(rest_rows, float(V_FIRST)), 0.0)
        count, start = jnp.zeros((local, half), F32), jnp.zeros((local, half), F32)
        for n in range(4):
            k = (4 * part + n) * local
            count = jnp.where(block == n, number[k:k + local, :half], count)
            start = jnp.where(block == n, base[k:k + local, :half], start)
        for shift, pack_ref in ((shift_y, pack_y_ref), (shift_v, pack_v_ref)):
            packed = jnp.where(slot < count, start + slot + shift[:, :half], -1.0)
            for e in range(local):
                pack_ref[e, part:part + 1, :] = packed[e:e + 1]

    relay(ACROSS_Y, 0)
    relay(ACROSS_X, 1)
    side_copy().start()

    def second():
        relay(ACROSS_Y, 1)
        relay(ACROSS_X, 0)

    def third():
        relay(ACROSS_XY, 0)
        relay(ACROSS_XY, 1)

    dispatch(slot_cap, gathered, key_ref, None, xs, xs_hbm, row_out,
             [second, third, lambda: arrive(CORE, CORE + 1), lambda: arrive(2, 3)])
    for c in loads:
        c.wait()

    @pl.loop(0, lead)
    def _(e):
        act = dot(xs[e, :half], w13[e], 1, 0)
        a, b = act[:, :hidden], act[:, hidden:]
        h = (a * jax.nn.sigmoid(a) * b).astype(BF)
        packed = dot(place(h, pack_y_ref[e, 0:1, :], Y_MOST), w2[e], 1, 0)

        @pl.when(e == 0)
        def _():
            yo[...] = packed

        @pl.when(e > 0)
        def _():
            yo[...] += packed

    stores = [pltpu.make_async_copy(yo.at[pl.ds(0, Y_FIRST)], yo_hbm, out_sem.at[0]),
              pltpu.make_async_copy(yo.at[pl.ds(Y_FIRST, Y_MOST - Y_FIRST)], spill_hbm, out_sem.at[1])]
    for c in stores:
        c.start()
    for k in others:
        aux_copy(k).wait_send()
        for part in (0, 1):
            copy(k, part).wait_send()
    side_copy().wait()
    dispatch_done(slot_cap, xs, xs_hbm, row_out)
    for c in stores:
        c.wait()


def spread_kernel(slot_cap, dout_ref, across_ref, key_ref, gate_ref, us_hbm, gathered, us, row_send, row_recv, row_out):
    _, peers = find_peers()
    meet([peers[ACROSS_X], peers[CORE]])

    def copy(slot, part):
        if slot in (ACROSS_X, CORE):
            source, peer = dout_ref.at[part], slot
        elif slot in (ACROSS_XY, 2):
            source, peer = across_ref.at[part], ACROSS_X if slot == ACROSS_XY else CORE
        else:
            source, peer = gathered.at[slot - 2, part], CORE
        return pltpu.make_async_remote_copy(source, gathered.at[slot, part], row_send.at[slot, part],
                                            row_recv.at[slot, part], device_id=peers[peer], device_id_type=MESH)

    sent = [ACROSS_X, ACROSS_XY, CORE, 2, CORE + 1, 3]
    for slot in sent[:4]:
        for part in (0, 1):
            copy(slot, part).start()
    gathered[OWN] = dout_ref[...]
    gathered[ACROSS_Y] = across_ref[...]

    def relay(slot):
        for part in (0, 1):
            copy(slot, part).wait_recv()
            copy(slot + 2, part).start()

    def arrive(*slots):
        for slot in slots:
            for part in (0, 1):
                copy(slot, part).wait_recv()

    dispatch(slot_cap, gathered, key_ref, gate_ref, us, us_hbm, row_out,
             [lambda: relay(ACROSS_X), lambda: relay(ACROSS_XY), lambda: arrive(CORE, CORE + 1), lambda: arrive(2, 3)])
    for slot in sent:
        for part in (0, 1):
            copy(slot, part).wait_send()
    dispatch_done(slot_cap, us, us_hbm, row_out)


VMEM = pl.BlockSpec(memory_space=pltpu.VMEM)
ANY = pl.BlockSpec(memory_space=pl.ANY)
DMA = pltpu.SemaphoreType.DMA


def prologue_call(tokens, d_out, ids, gates, w1, w3, w2, slot_cap):
    num_top, tok_dev = ids.shape
    width, local, f = tokens.shape[2], w1.shape[0], w1.shape[2]
    rows, aux = 8 * slot_cap, (2 * num_top, tok_dev)
    large = [((local, rows, width), BF), ((Y_FIRST, width), F32), ((Y_MOST - Y_FIRST, width), F32)]
    small = [((8, local, tok_dev), F32)] * 2 + [((local, 2, rows // 2), F32)] * 2
    small += [((8,) + aux, F32), (tokens.shape, BF)]
    scratch = [((8,) + tokens.shape, BF), (aux, F32), ((8,) + aux, F32), large[0]]
    scratch += [((LEAD, width, 2 * f), BF), ((LEAD, f, width), BF), ((Y_MOST, width), F32)]
    return pl.pallas_call(
        functools.partial(prologue_kernel, slot_cap), name="prologue",
        in_specs=[VMEM] * 4 + [ANY] * 3,
        out_specs=[ANY] * len(large) + [VMEM] * len(small),
        out_shape=[jax.ShapeDtypeStruct(s, t) for s, t in large + small],
        scratch_shapes=[pltpu.VMEM(s, t) for s, t in scratch]
        + [DMA((8, 2)), DMA((8, 2)), DMA((8,)), DMA((8,)), DMA, DMA, DMA((3,)), DMA((2,)), DMA((4,))],
        compiler_params=pltpu.CompilerParams(collective_id=0, has_side_effects=True, vmem_limit_bytes=VMEM_LIMIT),
        cost_estimate=cost(10**10, 3 * 10**7),
    )(tokens, d_out, ids, gates, w1, w3, w2)


def spread_call(d_out, across, key, gate, slot_cap):
    local = key.shape[1]
    out = (local, 8 * slot_cap, d_out.shape[2])
    return pl.pallas_call(
        functools.partial(spread_kernel, slot_cap), name="spread",
        in_specs=[VMEM] * 4, out_specs=ANY, out_shape=jax.ShapeDtypeStruct(out, BF),
        scratch_shapes=[pltpu.VMEM((8,) + d_out.shape, BF), pltpu.VMEM(out, BF), DMA((8, 2)), DMA((8, 2)), DMA((4,))],
        compiler_params=pltpu.CompilerParams(collective_id=1, has_side_effects=True, vmem_limit_bytes=VMEM_LIMIT),
        cost_estimate=cost(10**10, 3 * 10**7),
    )(d_out, across, key, gate)


def solution(mesh):
    tp_size, ep_size = mesh.shape["tp"], mesh.shape["ep"]
    row_spec = P(("dp", "ep", "tp"), None)
    col_spec = P("ep", None, "tp")
    down_spec = P("ep", "tp", None)
    grad_col = P(("dp", "ep"), None, "tp")
    grad_down = P(("dp", "ep"), "tp", None)

    def swap(z, tp_bit, ep_bits):
        pairs = [(t * ep_size + e, (t ^ tp_bit) * ep_size + (e ^ ep_bits)) for t in range(tp_size) for e in range(ep_size)]
        return lax.ppermute(z, ("tp", "ep"), pairs)

    def local_step(tokens, expert_ids, gate_vals, w_one, w_three, w_two, d_out):
        tok_dev, width = tokens.shape
        num_top = expert_ids.shape[1]
        local = w_one.shape[0]
        experts = local * ep_size
        slot_cap = slot_count(num_top, tok_dev, experts)
        half = tp_size * ep_size * slot_cap // 2
        ep_here = lax.axis_index("ep")

        blocked = (2, tok_dev // 2, width)
        d_blocked = d_out.reshape(blocked)
        xs, y_other0, y_spill, key, gate, pack_y, pack_v, aux_all, across = prologue_call(
            tokens.reshape(blocked), d_blocked, expert_ids.T, gate_vals.T, w_one, w_three, w_two, slot_cap)
        y0 = swap(y_other0, 1, 0)
        rest = local - LEAD
        act_one, act_three, hid, y_other1, y_extra, y_mine = expert_call(
            fwd_kernel, 0, local, xs, w_one, w_three, w_two, pack_y, [], [y_spill],
            [F32, F32, BF], (USUAL - Y_FIRST, TOTAL - USUAL, TOTAL), (TOTAL - Y_FIRST,))
        y1 = swap(y_other1, 1, 0)
        across = lax.optimization_barrier((across, hid))[0]
        us = spread_call(d_blocked, across, key, gate, slot_cap)

        every = jnp.arange(experts, dtype=F32)[None, :, None]
        count_all = sum(jnp.sum(aux_all[:, j:j + 1, :] == every, axis=2, dtype=jnp.int32) for j in range(num_top))
        kept = jnp.minimum(count_all, slot_cap).reshape(2, ep_size, ep_size, local).sum(axis=1)
        lead_rows, rest_rows = kept[:, :, :LEAD].sum(axis=2), kept[:, :, LEAD:].sum(axis=2)
        v_rest = jnp.maximum(rest_rows, V_FIRST)
        most = jnp.maximum(jnp.maximum(lead_rows, Y_FIRST) + rest_rows, v_rest + lead_rows)
        more = jnp.any(most > USUAL)
        full = jnp.any((lead_rows > Y_MOST) | (rest_rows > V_MOST) | (most > TOTAL)
                       | (v_rest + lead_rows - kept[:, :, 0] > V_CUTS[2])
                       | (kept[:, :, LEAD:LEAD + 3].sum(axis=2) > V_FIRST))

        def after(value, *others):
            return lax.optimization_barrier((value,) + others)[0]

        def extra(rows):
            return lax.cond(more, lambda z: swap(z, 1, 0), lambda z: z, rows)

        saved = [act_one, act_three]
        spill = V_MOST - V_FIRST
        tail = TOTAL - V_FIRST
        one1, three1, v_other0, spill_other, v_mine0, spill_mine = expert_call(
            bwd_rest_kernel, LEAD, rest, us, w_one, w_three, w_two, pack_v, saved, [],
            [BF, BF], (V_FIRST, spill, V_FIRST, spill), (V_MOST, V_MOST))
        y2 = extra(after(y_extra, v_mine0))
        v0 = swap(after(v_other0, y2), 1, 0)
        one0, three0, v_other1, v_other2, v_other3, v_extra, v_mine1, v_mine3 = expert_call(
            bwd_lead_kernel, 0, LEAD, us, w_one, w_three, w_two, pack_v, saved,
            [spill_other, spill_mine], [BF, BF],
            tuple(V_CUTS[n + 1] - V_CUTS[n] for n in range(4)) + (V_CUTS[2] - V_FIRST, TOTAL - V_CUTS[2]), (tail, tail))
        v1 = swap(v_other1, 1, 0)
        v2 = swap(v_other2, 1, 0)
        v3 = swap(v_other3, 1, 0)

        d_one = jnp.concatenate([one0, one1])
        d_three = jnp.concatenate([three0, three1])
        grads = grad_call(xs, us, hid, d_one, d_three)

        sources = jnp.stack([ep_here, ep_here ^ 2, ep_here ^ 1, ep_here ^ 3])
        all_ids = (sources[:, None] * local + jnp.arange(local)).reshape(-1)
        eq = expert_ids[:, :, None] == all_ids
        hit = jnp.any(eq, axis=1)
        lower = (jnp.arange(tok_dev)[:, None] > jnp.arange(tok_dev)[None, :]).astype(BF)
        pos = jnp.dot(lower, hit.astype(BF), preferred_element_type=F32)
        own_gate = jnp.sum(jnp.where(eq, gate_vals[:, :, None], 0.0), axis=1)
        own_pick = hit[:, :, None] & (pos[:, :, None] == jnp.arange(slot_cap, dtype=F32))
        own_mul = jnp.where(own_pick, own_gate[:, :, None], 0.0).reshape(tok_dev, ep_size, local, slot_cap)
        own_pick = own_pick.astype(BF).reshape(tok_dev, ep_size, local, slot_cap)

        def send_back(parts):
            back = [parts[0]]
            for n, bits in ((1, 2), (2, 1), (3, 3)):
                back.append(swap(parts[n], 0, bits))
            return back

        def mix(weights, back, first, count):
            flat = jnp.concatenate(back)
            weights = weights[:, :, first:first + count].reshape(tok_dev, -1)
            if weights.dtype == BF:
                return jnp.dot(weights, flat, preferred_element_type=F32)
            return jnp.dot(weights, flat.astype(F32), precision=lax.Precision.HIGHEST)

        def slots_of(pack, first, count):
            return pack[first:first + count, 1].reshape(count, ep_size, slot_cap).transpose(1, 0, 2).reshape(-1, 1)

        def finish(first, count, pack, owns, pieces, recvs, known=(), early=0):
            keys = [slots_of(pack, first, count)] + [slots_of(pack, 0, early)] * (early > 0)
            sizes = [count * slot_cap] * ep_size + [early * slot_cap] * (ep_size * (early > 0))
            out = finish_call(owns, pieces, recvs, jnp.concatenate(keys), known, sizes)
            back = send_back(out[:ep_size])
            return back, out[ep_size:]

        y_back, _ = finish(0, local, pack_y, [y_mine],
                           [(0, 0, 0, Y_FIRST), (0, Y_FIRST, Y_FIRST, USUAL - Y_FIRST), (0, USUAL, USUAL, TOTAL - USUAL)],
                           [y0, y1, y2])
        piece = [(0, 0, 0, V_FIRST)] + [(1, V_CUTS[n] - V_FIRST, V_CUTS[n], V_CUTS[n + 1] - V_CUTS[n]) for n in range(2)]
        late = [(0,) + p[1:] for p in piece[1:]]
        last = [(0, V_CUTS[n] - V_CUTS[2], V_CUTS[n], V_CUTS[n + 1] - V_CUTS[n]) for n in (2, 3)]
        back0, _ = finish(LEAD, 3, pack_v, [v_mine0], piece[:1], [v0])
        back1, _ = finish(LEAD + 3, rest - 3, pack_v, [after(v_mine0, back0[0]), v_mine1], piece[:2], [v0, v1])
        out_sum = mix(own_mul, y_back, 0, local)
        dx_early = mix(own_pick, back0, LEAD, 3)
        v4 = extra(after(v_extra, dx_early, out_sum))
        back2, known = finish(1, LEAD - 1, pack_v, [after(v_mine1, back1[0], v4)], late, [v1, v2], early=1)
        back3, _ = finish(0, 1, pack_v, [after(v_mine3, back2[0])], last, [v3, v4], known=known)
        dx_early = dx_early + mix(own_pick, back1, LEAD + 3, rest - 3)
        dx_early = mix(own_pick, back2, 1, LEAD - 1) + dx_early
        dx_sum = mix(own_pick, after(tuple(back3), dx_early), 0, 1) + dx_early

        def exchange_all(args):
            hid, d_one, d_three, own_mul, own_pick = args

            def back(part):
                recv = swap(part[:, :half], 1, 0)
                done = (part[:, half:] + recv).astype(BF).reshape(local, ep_size, slot_cap, width)
                return send_back([done[:, s].reshape(-1, width) for s in range(ep_size)])

            part_out = jnp.einsum("enf,efd->end", hid, w_two, preferred_element_type=F32)
            part_dx = jnp.einsum("enf,edf->end", d_one, w_one, preferred_element_type=F32)
            part_dx += jnp.einsum("enf,edf->end", d_three, w_three, preferred_element_type=F32)
            return mix(own_mul, back(part_out), 0, local), mix(own_pick, back(part_dx), 0, local)

        def exchange_none(args):
            zero = jnp.zeros((tok_dev, width), F32)
            return zero, zero

        out_full, dx_full = lax.cond(full, exchange_all, exchange_none, (hid, d_one, d_three, own_mul, own_pick))
        out_rows = jnp.where(full, out_full, out_sum).astype(BF)
        dx_rows = jnp.where(full, dx_full, dx_sum).astype(BF)
        return out_rows, dx_rows, *grads

    return jax.shard_map(local_step, mesh=mesh,
                         in_specs=(row_spec, row_spec, row_spec, col_spec, col_spec, down_spec, row_spec),
                         out_specs=(row_spec, row_spec, grad_col, grad_col, grad_down), check_vma=False)
```

```python
import functools

import jax
import jax.numpy as jnp
from jax import lax
from jax.experimental import pallas as pl
from jax.experimental.pallas import tpu as pltpu
from jax.sharding import PartitionSpec as P


BF = jnp.bfloat16
F32 = jnp.float32
MESH = pl.DeviceIdType.MESH

LEAD = 3
USUAL, TOTAL = 552, 616
Y_FIRST, Y_MOST = 184, 240
V_FIRST, V_MOST = 280, 376
V_CUTS = (280, 456, 512, 552, 616)
WINDOW = 104
VMEM_LIMIT = 62 * 2**20


def slot_count(num_top, tok_dev, experts):
    return 8 * ((5 * num_top * tok_dev + 32 * experts - 1) // (32 * experts))


def dot(a, b, ca, cb):
    return lax.dot_general(a, b, (((ca,), (cb,)), ((), ())), preferred_element_type=F32)


def place(rows, keys, cap):
    pick = lax.broadcasted_iota(jnp.int32, (cap, keys.shape[1]), 0).astype(F32) == keys
    return dot(jnp.where(pick, 1.0, 0.0).astype(BF), rows, 1, 0).astype(BF)


def add_window(ref, part, keys, shift, terms):
    half = keys.shape[1]
    rows = slice(part * half, (part + 1) * half)
    keys = keys[part:part + 1, :]
    first = jnp.min(jnp.where(keys >= 0.0, keys, float(TOTAL))).astype(jnp.int32)
    start = jnp.clip((first - shift) // 8 * 8, 0, ref.shape[0] - WINDOW)
    at = keys - (start + shift).astype(F32)
    product = sum(dot(place(left[rows], at, WINDOW), right, 1, dim) for left, right, dim in terms)
    ref[pl.ds(pl.multiple_of(start, 8), WINDOW), :] += product


def cut(source, refs):
    row = 0
    for ref in refs:
        ref[...] = source[row:row + ref.shape[0]]
        row += ref.shape[0]


def fwd_kernel(x_ref, w1_ref, w3_ref, w2_ref, key_ref, spill_ref, a_ref, b_ref, h_ref, other_ref, extra_ref, mine_ref, other):
    step = pl.program_id(0)

    @pl.when(step == 0)
    def _():
        mine_ref[...] = jnp.zeros_like(mine_ref)
        other[...] = jnp.zeros_like(other)
        other[:spill_ref.shape[0], :] = spill_ref[...]

    x = x_ref[0]
    a = dot(x, w1_ref[0], 1, 0)
    b = dot(x, w3_ref[0], 1, 0)
    h = (a * jax.nn.sigmoid(a) * b).astype(BF)
    a_ref[0] = a
    b_ref[0] = b
    h_ref[0] = h
    add_window(mine_ref, 1, key_ref[0], 0, [(h, w2_ref[0], 0)])

    @pl.when(step >= LEAD)
    def _():
        add_window(other, 0, key_ref[0], Y_FIRST, [(h_ref[0], w2_ref[0], 0)])

    @pl.when(step == pl.num_programs(0) - 1)
    def _():
        cut(other, (other_ref, extra_ref))


def bwd_step(shift, u_ref, w1_ref, w3_ref, w2_ref, key_ref, a_ref, b_ref, da_ref, db_ref, parts):
    dh = dot(u_ref[0], w2_ref[0], 1, 1)
    a = a_ref[0]
    s = jax.nn.sigmoid(a)
    da = (dh * b_ref[0] * s * (1.0 + a * (1.0 - s))).astype(BF)
    db = (dh * (a * s)).astype(BF)
    da_ref[0] = da
    db_ref[0] = db
    for part, ref in enumerate(parts):
        add_window(ref, part, key_ref[0], shift, [(da, w1_ref[0], 1), (db, w3_ref[0], 1)])


def bwd_rest_kernel(u_ref, w1_ref, w3_ref, w2_ref, key_ref, a_ref, b_ref, da_ref, db_ref,
                    other_ref, spill_other_ref, mine_ref, spill_mine_ref, other, mine):
    step = pl.program_id(0)

    @pl.when(step == 0)
    def _():
        other[...] = jnp.zeros_like(other)
        mine[...] = jnp.zeros_like(mine)

    bwd_step(0, u_ref, w1_ref, w3_ref, w2_ref, key_ref, a_ref, b_ref, da_ref, db_ref, (other, mine))

    @pl.when(step == pl.num_programs(0) - 1)
    def _():
        cut(other, (other_ref, spill_other_ref))
        cut(mine, (mine_ref, spill_mine_ref))


def bwd_lead_kernel(u_ref, w1_ref, w3_ref, w2_ref, key_ref, a_ref, b_ref, spill_other_ref, spill_mine_ref,
                    da_ref, db_ref, other1_ref, other2_ref, other3_ref, extra_ref, mine_ref, mine3_ref, other, mine):
    step = pl.program_id(0)

    @pl.when(step == 0)
    def _():
        for ref, spill_ref in ((other, spill_other_ref), (mine, spill_mine_ref)):
            ref[...] = jnp.zeros_like(ref)
            ref[:spill_ref.shape[0], :] = spill_ref[...]

    bwd_step(V_FIRST, u_ref, w1_ref, w3_ref, w2_ref, key_ref, a_ref, b_ref, da_ref, db_ref, (other, mine))

    @pl.when(step == pl.num_programs(0) - 1)
    def _():
        cut(other, (other1_ref, other2_ref, other3_ref, extra_ref))
        cut(mine, (mine_ref, mine3_ref))


def finish_kernel(pieces, owns, known, *refs):
    own_refs, recv_refs, key_ref = refs[:owns], refs[owns:owns + len(pieces)], refs[owns + len(pieces)]
    known_refs = refs[owns + len(pieces) + 1:][:known]
    out_refs = refs[owns + len(pieces) + 1 + known:]
    done = [(own_refs[i][row:row + count, :] + recv_ref[...]).astype(BF)
            for (i, row, _, count), recv_ref in zip(pieces, recv_refs)]
    total = None
    for (_, _, position, count), values in zip(pieces, done):
        pick = lax.broadcasted_iota(jnp.int32, (key_ref.shape[0], count), 1).astype(F32) == key_ref[...] - float(position)
        term = dot(jnp.where(pick, 1.0, 0.0).astype(BF), values, 1, 0)
        total = term if total is None else total + term
    first = 0
    for i, out_ref in enumerate(out_refs):
        rows = total[first:first + out_ref.shape[0]]
        first += out_ref.shape[0]
        if known:
            rows = rows + known_refs[i][...].astype(F32)
        out_ref[...] = rows.astype(BF)


def grad_kernel(x_ref, u_ref, h_ref, da0_ref, db0_ref, da1_ref, db1_ref, g1_ref, g3_ref, g2_ref):
    x = x_ref[0]
    lead = pl.program_id(0) < LEAD
    g1_ref[0] = dot(x, jnp.where(lead, da0_ref[0], da1_ref[0]), 0, 0).astype(BF)
    g3_ref[0] = dot(x, jnp.where(lead, db0_ref[0], db1_ref[0]), 0, 0).astype(BF)
    g2_ref[0] = dot(h_ref[0], u_ref[0], 0, 0).astype(BF)


def spec(shape, first):
    return pl.BlockSpec((1,) + shape, lambda i: (i + first, 0, 0))


def whole(shape):
    return pl.BlockSpec(shape, lambda i: (0,) * len(shape))


def cost(flops, nbytes):
    return pl.CostEstimate(flops=flops, bytes_accessed=nbytes, transcendentals=0)


PARAMS = pltpu.CompilerParams(dimension_semantics=("arbitrary",), vmem_limit_bytes=VMEM_LIMIT)


def expert_call(body, first, count, rows_in, w1, w3, w2, keys, saved, extra, kinds, outs, scratch):
    rows, d, f = rows_in.shape[1], w1.shape[1], w1.shape[2]
    half = rows // 2
    shapes = [((count, rows, f), t) for t in kinds] + [((n, d), F32) for n in outs]
    return pl.pallas_call(
        body, grid=(count,),
        in_specs=[spec((rows, d), first), spec((d, f), first), spec((d, f), first), spec((f, d), first),
                  spec((2, half), first)] + [spec((rows, f), first)] * len(saved) + [whole(e.shape) for e in extra],
        out_specs=[spec(s[1:], 0) if len(s) == 3 else whole(s) for s, _ in shapes],
        out_shape=[jax.ShapeDtypeStruct(s, t) for s, t in shapes],
        scratch_shapes=[pltpu.VMEM((n, d), F32) for n in scratch],
        compiler_params=PARAMS, cost_estimate=cost(count * 8 * rows * d * f, count * (6 * d * f + 6 * rows * d)),
    )(rows_in, w1, w3, w2, keys, *saved, *extra)


def grad_call(xs, us, h, lead, rest):
    count, rows, d = xs.shape
    f = h.shape[2]
    outs = [((d, f), BF), ((d, f), BF), ((f, d), BF)]
    return pl.pallas_call(
        grad_kernel, grid=(count,), name="wgrad",
        in_specs=[spec((rows, d), 0), spec((rows, d), 0), spec((rows, f), 0)]
        + [pl.BlockSpec((1, rows, f), lambda i: (jnp.minimum(i, LEAD - 1), 0, 0))] * 2
        + [pl.BlockSpec((1, rows, f), lambda i: (jnp.maximum(i - LEAD, 0), 0, 0))] * 2,
        out_specs=[spec(s, 0) for s, _ in outs],
        out_shape=[jax.ShapeDtypeStruct((count,) + s, t) for s, t in outs],
        compiler_params=PARAMS, cost_estimate=cost(count * 6 * rows * d * f, count * (6 * d * f + 4 * rows * d)),
    )(xs, us, h, *lead, *rest)


def finish_call(owns, pieces, recvs, keys, known, sizes, steps):
    d = owns[0].shape[1]
    total = sum(r.shape[0] for r in recvs)

    def columns(rows):
        return pl.BlockSpec((rows, d // steps), lambda i: (0, i))

    return pl.pallas_call(
        functools.partial(finish_kernel, pieces, len(owns), len(known)), name="finish", grid=(steps,),
        in_specs=[columns(r.shape[0]) for r in (*owns, *recvs)] + [whole(keys.shape)] + [columns(r.shape[0]) for r in known],
        out_specs=[columns(rows) for rows in sizes],
        out_shape=[jax.ShapeDtypeStruct((rows, d), BF) for rows in sizes],
        compiler_params=PARAMS,
        cost_estimate=cost(2 * keys.shape[0] * d * total, 8 * total * d),
    )(*owns, *recvs, keys, *known)


ACROSS_Y, ACROSS_XY, OWN, ACROSS_X, CORE = 0, 1, 4, 5, 6
STEPS = ((1, 0), (1, 2), (1, 1), (1, 3), (0, 0), (0, 2), (0, 1), (0, 3))


def find_peers():
    tp, ep = lax.axis_index("tp"), lax.axis_index("ep")
    eps = {0: ep, 2: lax.rem(ep + 2, 4), 1: ep + 1 - 2 * lax.rem(ep, 2), 3: 3 - ep}
    return ep, [{"tp": 1 - tp if a else tp, "ep": eps[b]} for a, b in STEPS]


def meet(peers):
    barrier = pltpu.get_barrier_semaphore()
    for peer in peers:
        pl.semaphore_signal(barrier, inc=1, device_id=peer, device_id_type=MESH)
    pl.semaphore_wait(barrier, len(peers))


def dispatch(slot_cap, blocks, key_ref, gate_ref, out, out_hbm, sem, ready):
    local, width = key_ref.shape[1], key_ref.shape[2]

    @pl.loop(0, 4)
    def _(n):
        for at, step in enumerate(ready):
            pl.when(n == at)(step)
        first = lax.rem(OWN + 4 * n, 8) + 2 * (n // 2)
        one, two = key_ref[first], key_ref[first + 1]
        pair = jnp.concatenate([one, jnp.where(two >= 0.0, two + slot_cap, -1.0)], axis=1)
        index = lax.broadcasted_iota(jnp.int32, (2 * slot_cap, 2 * width), 0).astype(F32)
        picks = [index == pair[e:e + 1, :] for e in range(local)]
        pick = jnp.concatenate([jnp.where(p, 1.0, 0.0) for p in picks], axis=0).astype(BF)
        rows = dot(pick, blocks[pl.ds(first, 2)].reshape(2 * width, out.shape[2]), 1, 0)
        if gate_ref is not None:
            gates = jnp.concatenate([gate_ref[first], gate_ref[first + 1]], axis=1)
            scale = jnp.concatenate([jnp.where(p, gates[e:e + 1, :], 0.0) for e, p in enumerate(picks)], axis=0)
            rows = rows * jnp.sum(scale, axis=1, keepdims=True)
        rows = rows.astype(BF)
        at = pl.ds(pl.multiple_of(first * slot_cap, 2 * slot_cap), 2 * slot_cap)
        for e in range(local):
            out[e, at, :] = rows[e * 2 * slot_cap:(e + 1) * 2 * slot_cap]
        pltpu.make_async_copy(out.at[:, at], out_hbm.at[:, at], sem.at[n]).start()


def dispatch_done(slot_cap, out, out_hbm, sem):
    for n in range(4):
        at = pl.ds(2 * slot_cap * n, 2 * slot_cap)
        pltpu.make_async_copy(out.at[:, at], out_hbm.at[:, at], sem.at[n]).wait()


def prologue_kernel(slot_cap, tok_ref, dout_ref, id_ref, val_ref, w1_hbm, w3_hbm, w2_hbm,
                    xs_hbm, yo_hbm, spill_hbm, key_ref, gate_ref, pack_y_ref, pack_v_ref, aux_all_ref, across_ref,
                    gathered, aux_ref, aux_all, xs, w13, w2, yo,
                    row_send, row_recv, aux_send, aux_recv, side_send, side_recv, in_sem, out_sem, row_out):
    ep, peers = find_peers()
    others = [k for k in range(8) if k != OWN]
    local, width = key_ref.shape[1], key_ref.shape[2]
    num_top, half = id_ref.shape[0], 4 * slot_cap

    aux_ref[...] = jnp.concatenate([id_ref[...].astype(F32), val_ref[...]], axis=0)
    lead, hidden = w2.shape[0], w2.shape[1]
    loads = [pltpu.make_async_copy(w.at[pl.ds(0, lead)], buf, in_sem.at[n]) for n, (w, buf) in enumerate(
        ((w1_hbm, w13.at[:, :, pl.ds(0, hidden)]), (w3_hbm, w13.at[:, :, pl.ds(hidden, hidden)]), (w2_hbm, w2)))]
    for c in loads:
        c.start()
    meet([peers[k] for k in others])

    def aux_copy(k):
        return pltpu.make_async_remote_copy(aux_ref, aux_all.at[k], aux_send.at[k], aux_recv.at[k],
                                            device_id=peers[k], device_id_type=MESH)

    def copy(slot, part):
        if slot in (ACROSS_Y, ACROSS_X, CORE):
            source, peer = tok_ref.at[part], slot
        elif slot == ACROSS_XY:
            source, peer = (gathered.at[ACROSS_Y, 0], ACROSS_X) if part == 0 else (gathered.at[ACROSS_X, 1], ACROSS_Y)
        else:
            source, peer = gathered.at[slot - 2, part], CORE
        return pltpu.make_async_remote_copy(source, gathered.at[slot, part], row_send.at[slot, part],
                                            row_recv.at[slot, part], device_id=peers[peer], device_id_type=MESH)

    def side_copy():
        return pltpu.make_async_remote_copy(dout_ref, across_ref, side_send, side_recv,
                                            device_id=peers[ACROSS_Y], device_id_type=MESH)

    def relay(slot, part):
        copy(slot, part).wait_recv()
        if (slot, part) in ((ACROSS_Y, 0), (ACROSS_X, 1)):
            copy(ACROSS_XY, part).start()
        copy(slot + 2, part).start()

    def arrive(*slots):
        for slot in slots:
            for part in (0, 1):
                copy(slot, part).wait_recv()

    for k in others:
        aux_copy(k).start()
    for slot, part in ((ACROSS_Y, 0), (ACROSS_X, 1), (ACROSS_Y, 1), (ACROSS_X, 0), (CORE, 0), (CORE, 1)):
        copy(slot, part).start()
    gathered[OWN] = tok_ref[...]
    aux_all[OWN] = aux_ref[...]

    for k in others:
        aux_copy(k).wait_recv()
    aux_all_ref[...] = aux_all[...]
    expert = (lax.broadcasted_iota(jnp.int32, (local, width), 0) + ep * local).astype(F32)
    hits = []
    for k in range(8):
        a = aux_all[k]
        hit, gate = jnp.zeros((local, width), F32), jnp.zeros((local, width), F32)
        for j in range(num_top):
            eq = a[j:j + 1, :] == expert
            hit = jnp.where(eq, 1.0, hit)
            gate = jnp.where(eq, a[num_top + j:num_top + j + 1, :], gate)
        hits.append(hit)
        gate_ref[k] = gate
    hit = jnp.concatenate(hits, axis=0)
    upper = lax.broadcasted_iota(jnp.int32, (width, width), 0) < lax.broadcasted_iota(jnp.int32, (width, width), 1)
    pos = dot(hit.astype(BF), jnp.where(upper, 1.0, 0.0).astype(BF), 1, 0)
    kept = jnp.where(pos < slot_cap, hit, 0.0)
    key = jnp.where(kept > 0.0, pos, -1.0)
    number = jnp.broadcast_to(jnp.sum(kept, axis=1, keepdims=True), key.shape)
    total = 8 * local
    row = lax.broadcasted_iota(jnp.int32, (total, total), 0)
    col = lax.broadcasted_iota(jnp.int32, (total, total), 1)
    rb, re, cb, ce = row // local, lax.rem(row, local), col // local, lax.rem(col, local)
    rank_row = jnp.where(re < LEAD, lax.rem(re + LEAD - 1, LEAD), re)
    rank_col = jnp.where(ce < LEAD, lax.rem(ce + LEAD - 1, LEAD), ce)
    before = jnp.logical_and(rb // 4 == cb // 4, (re < LEAD) == (ce < LEAD))
    before = jnp.logical_and(before, jnp.logical_or(rank_col < rank_row, jnp.logical_and(ce == re, cb < rb)))
    base = dot(jnp.where(before, 1.0, 0.0).astype(BF), number.astype(BF), 1, 0)
    source = lax.broadcasted_iota(jnp.int32, key.shape, 0)
    leading = lax.rem(source, local) < LEAD
    is_lead = lax.broadcasted_iota(jnp.int32, (local, width), 0) < LEAD
    lane = lax.broadcasted_iota(jnp.int32, (local, half), 1)
    slot, block = lax.rem(lane, slot_cap).astype(F32), lane // slot_cap
    for k in range(8):
        key_ref[k] = key[k * local:(k + 1) * local]
    for part in range(2):
        here = source // (4 * local) == part
        lead_rows = jnp.sum(jnp.where(jnp.logical_and(here, leading), number, 0.0), axis=0, keepdims=True)
        rest_rows = jnp.sum(jnp.where(jnp.logical_and(here, jnp.logical_not(leading)), number, 0.0), axis=0, keepdims=True)
        shift_y = jnp.where(is_lead, 0.0, jnp.maximum(lead_rows, float(Y_FIRST)))
        shift_v = jnp.where(is_lead, jnp.maximum(rest_rows, float(V_FIRST)), 0.0)
        count, start = jnp.zeros((local, half), F32), jnp.zeros((local, half), F32)
        for n in range(4):
            k = (4 * part + n) * local
            count = jnp.where(block == n, number[k:k + local, :half], count)
            start = jnp.where(block == n, base[k:k + local, :half], start)
        for shift, pack_ref in ((shift_y, pack_y_ref), (shift_v, pack_v_ref)):
            packed = jnp.where(slot < count, start + slot + shift[:, :half], -1.0)
            for e in range(local):
                pack_ref[e, part:part + 1, :] = packed[e:e + 1]

    relay(ACROSS_Y, 0)
    relay(ACROSS_X, 1)
    side_copy().start()

    def second():
        relay(ACROSS_Y, 1)
        relay(ACROSS_X, 0)

    def third():
        relay(ACROSS_XY, 0)
        relay(ACROSS_XY, 1)

    dispatch(slot_cap, gathered, key_ref, None, xs, xs_hbm, row_out,
             [second, third, lambda: arrive(CORE, CORE + 1), lambda: arrive(2, 3)])
    for c in loads:
        c.wait()

    @pl.loop(0, lead)
    def _(e):
        act = dot(xs[e, :half], w13[e], 1, 0)
        a, b = act[:, :hidden], act[:, hidden:]
        h = (a * jax.nn.sigmoid(a) * b).astype(BF)
        packed = dot(place(h, pack_y_ref[e, 0:1, :], Y_MOST), w2[e], 1, 0)

        @pl.when(e == 0)
        def _():
            yo[...] = packed

        @pl.when(e > 0)
        def _():
            yo[...] += packed

    stores = [pltpu.make_async_copy(yo.at[pl.ds(0, Y_FIRST)], yo_hbm, out_sem.at[0]),
              pltpu.make_async_copy(yo.at[pl.ds(Y_FIRST, Y_MOST - Y_FIRST)], spill_hbm, out_sem.at[1])]
    for c in stores:
        c.start()
    for k in others:
        aux_copy(k).wait_send()
        for part in (0, 1):
            copy(k, part).wait_send()
    side_copy().wait()
    dispatch_done(slot_cap, xs, xs_hbm, row_out)
    for c in stores:
        c.wait()


def spread_kernel(slot_cap, dout_ref, across_ref, key_ref, gate_ref, us_hbm, gathered, us, row_send, row_recv, row_out):
    _, peers = find_peers()
    meet([peers[ACROSS_X], peers[CORE]])

    def copy(slot, part):
        if slot in (ACROSS_X, CORE):
            source, peer = dout_ref.at[part], slot
        elif slot in (ACROSS_XY, 2):
            source, peer = across_ref.at[part], ACROSS_X if slot == ACROSS_XY else CORE
        else:
            source, peer = gathered.at[slot - 2, part], CORE
        return pltpu.make_async_remote_copy(source, gathered.at[slot, part], row_send.at[slot, part],
                                            row_recv.at[slot, part], device_id=peers[peer], device_id_type=MESH)

    sent = [ACROSS_X, ACROSS_XY, CORE, 2, CORE + 1, 3]
    for slot in sent[:4]:
        for part in (0, 1):
            copy(slot, part).start()
    gathered[OWN] = dout_ref[...]
    gathered[ACROSS_Y] = across_ref[...]

    def relay(slot):
        for part in (0, 1):
            copy(slot, part).wait_recv()
            copy(slot + 2, part).start()

    def arrive(*slots):
        for slot in slots:
            for part in (0, 1):
                copy(slot, part).wait_recv()

    dispatch(slot_cap, gathered, key_ref, gate_ref, us, us_hbm, row_out,
             [lambda: relay(ACROSS_X), lambda: relay(ACROSS_XY), lambda: arrive(CORE, CORE + 1), lambda: arrive(2, 3)])
    for slot in sent:
        for part in (0, 1):
            copy(slot, part).wait_send()
    dispatch_done(slot_cap, us, us_hbm, row_out)


VMEM = pl.BlockSpec(memory_space=pltpu.VMEM)
ANY = pl.BlockSpec(memory_space=pl.ANY)
DMA = pltpu.SemaphoreType.DMA


def prologue_call(tokens, d_out, ids, gates, w1, w3, w2, slot_cap):
    num_top, tok_dev = ids.shape
    width, local, f = tokens.shape[2], w1.shape[0], w1.shape[2]
    rows, aux = 8 * slot_cap, (2 * num_top, tok_dev)
    large = [((local, rows, width), BF), ((Y_FIRST, width), F32), ((Y_MOST - Y_FIRST, width), F32)]
    small = [((8, local, tok_dev), F32)] * 2 + [((local, 2, rows // 2), F32)] * 2
    small += [((8,) + aux, F32), (tokens.shape, BF)]
    scratch = [((8,) + tokens.shape, BF), (aux, F32), ((8,) + aux, F32), large[0]]
    scratch += [((LEAD, width, 2 * f), BF), ((LEAD, f, width), BF), ((Y_MOST, width), F32)]
    return pl.pallas_call(
        functools.partial(prologue_kernel, slot_cap), name="prologue",
        in_specs=[VMEM] * 4 + [ANY] * 3,
        out_specs=[ANY] * len(large) + [VMEM] * len(small),
        out_shape=[jax.ShapeDtypeStruct(s, t) for s, t in large + small],
        scratch_shapes=[pltpu.VMEM(s, t) for s, t in scratch]
        + [DMA((8, 2)), DMA((8, 2)), DMA((8,)), DMA((8,)), DMA, DMA, DMA((3,)), DMA((2,)), DMA((4,))],
        compiler_params=pltpu.CompilerParams(collective_id=0, has_side_effects=True, vmem_limit_bytes=VMEM_LIMIT),
        cost_estimate=cost(10**10, 3 * 10**7),
    )(tokens, d_out, ids, gates, w1, w3, w2)


def spread_call(d_out, across, key, gate, slot_cap):
    local = key.shape[1]
    out = (local, 8 * slot_cap, d_out.shape[2])
    return pl.pallas_call(
        functools.partial(spread_kernel, slot_cap), name="spread",
        in_specs=[VMEM] * 4, out_specs=ANY, out_shape=jax.ShapeDtypeStruct(out, BF),
        scratch_shapes=[pltpu.VMEM((8,) + d_out.shape, BF), pltpu.VMEM(out, BF), DMA((8, 2)), DMA((8, 2)), DMA((4,))],
        compiler_params=pltpu.CompilerParams(collective_id=1, has_side_effects=True, vmem_limit_bytes=VMEM_LIMIT),
        cost_estimate=cost(10**10, 3 * 10**7),
    )(d_out, across, key, gate)


def solution(mesh):
    tp_size, ep_size = mesh.shape["tp"], mesh.shape["ep"]
    row_spec = P(("dp", "ep", "tp"), None)
    col_spec = P("ep", None, "tp")
    down_spec = P("ep", "tp", None)
    grad_col = P(("dp", "ep"), None, "tp")
    grad_down = P(("dp", "ep"), "tp", None)

    def swap(z, tp_bit, ep_bits):
        pairs = [(t * ep_size + e, (t ^ tp_bit) * ep_size + (e ^ ep_bits)) for t in range(tp_size) for e in range(ep_size)]
        return lax.ppermute(z, ("tp", "ep"), pairs)

    def local_step(tokens, expert_ids, gate_vals, w_one, w_three, w_two, d_out):
        tok_dev, width = tokens.shape
        num_top = expert_ids.shape[1]
        local = w_one.shape[0]
        experts = local * ep_size
        slot_cap = slot_count(num_top, tok_dev, experts)
        half = tp_size * ep_size * slot_cap // 2
        ep_here = lax.axis_index("ep")

        blocked = (2, tok_dev // 2, width)
        d_blocked = d_out.reshape(blocked)
        xs, y_other0, y_spill, key, gate, pack_y, pack_v, aux_all, across = prologue_call(
            tokens.reshape(blocked), d_blocked, expert_ids.T, gate_vals.T, w_one, w_three, w_two, slot_cap)
        y0 = swap(y_other0, 1, 0)
        rest = local - LEAD
        act_one, act_three, hid, y_other1, y_extra, y_mine = expert_call(
            fwd_kernel, 0, local, xs, w_one, w_three, w_two, pack_y, [], [y_spill],
            [F32, F32, BF], (USUAL - Y_FIRST, TOTAL - USUAL, TOTAL), (TOTAL - Y_FIRST,))
        y1 = swap(y_other1, 1, 0)
        across = lax.optimization_barrier((across, hid))[0]
        us = spread_call(d_blocked, across, key, gate, slot_cap)

        every = jnp.arange(experts, dtype=F32)[None, :, None]
        count_all = sum(jnp.sum(aux_all[:, j:j + 1, :] == every, axis=2, dtype=jnp.int32) for j in range(num_top))
        kept = jnp.minimum(count_all, slot_cap).reshape(2, ep_size, ep_size, local).sum(axis=1)
        lead_rows, rest_rows = kept[:, :, :LEAD].sum(axis=2), kept[:, :, LEAD:].sum(axis=2)
        v_rest = jnp.maximum(rest_rows, V_FIRST)
        most = jnp.maximum(jnp.maximum(lead_rows, Y_FIRST) + rest_rows, v_rest + lead_rows)
        more = jnp.any(most > USUAL)
        full = jnp.any((lead_rows > Y_MOST) | (rest_rows > V_MOST) | (most > TOTAL)
                       | (v_rest + lead_rows - kept[:, :, 0] > V_CUTS[2]) | (v_rest + kept[:, :, 1] > V_CUTS[1])
                       | (kept[:, :, LEAD:LEAD + 3].sum(axis=2) > V_FIRST))

        def after(value, *others):
            return lax.optimization_barrier((value,) + others)[0]

        def extra(rows):
            return lax.cond(more, lambda z: swap(z, 1, 0), lambda z: z, rows)

        saved = [act_one, act_three]
        spill = V_MOST - V_FIRST
        tail = TOTAL - V_FIRST
        one1, three1, v_other0, spill_other, v_mine0, spill_mine = expert_call(
            bwd_rest_kernel, LEAD, rest, us, w_one, w_three, w_two, pack_v, saved, [],
            [BF, BF], (V_FIRST, spill, V_FIRST, spill), (V_MOST, V_MOST))
        y2 = extra(after(y_extra, v_mine0))
        v0 = swap(after(v_other0, y2), 1, 0)
        one0, three0, v_other1, v_other2, v_other3, v_extra, v_mine1, v_mine3 = expert_call(
            bwd_lead_kernel, 0, LEAD, us, w_one, w_three, w_two, pack_v, saved,
            [spill_other, spill_mine], [BF, BF],
            tuple(V_CUTS[n + 1] - V_CUTS[n] for n in range(4)) + (V_CUTS[2] - V_FIRST, TOTAL - V_CUTS[2]), (tail, tail))
        v1 = swap(v_other1, 1, 0)
        v2 = swap(v_other2, 1, 0)
        v3 = swap(v_other3, 1, 0)

        grads = grad_call(xs, us, hid, (one0, three0), (one1, three1))

        sources = jnp.stack([ep_here, ep_here ^ 2, ep_here ^ 1, ep_here ^ 3])
        all_ids = (sources[:, None] * local + jnp.arange(local)).reshape(-1)
        eq = expert_ids[:, :, None] == all_ids
        hit = jnp.any(eq, axis=1)
        lower = (jnp.arange(tok_dev)[:, None] > jnp.arange(tok_dev)[None, :]).astype(BF)
        pos = jnp.dot(lower, hit.astype(BF), preferred_element_type=F32)
        own_gate = jnp.sum(jnp.where(eq, gate_vals[:, :, None], 0.0), axis=1)
        own_pick = hit[:, :, None] & (pos[:, :, None] == jnp.arange(slot_cap, dtype=F32))
        own_mul = jnp.where(own_pick, own_gate[:, :, None], 0.0).reshape(tok_dev, ep_size, local, slot_cap)
        own_pick = own_pick.astype(BF).reshape(tok_dev, ep_size, local, slot_cap)

        def send_back(parts):
            back = [parts[0]]
            for n, bits in ((1, 2), (2, 1), (3, 3)):
                back.append(swap(parts[n], 0, bits))
            return back

        def choose(array, ids, axis):
            runs = []
            for e in ids:
                if runs and runs[-1][1] == e:
                    runs[-1][1] = e + 1
                else:
                    runs.append([e, e + 1])
            parts = [lax.slice_in_dim(array, *run, axis=axis) for run in runs]
            return parts[0] if len(parts) == 1 else jnp.concatenate(parts, axis=axis)

        def mix(weights, back, ids):
            flat = jnp.concatenate(back)
            weights = choose(weights, ids, 2).reshape(tok_dev, -1)
            if weights.dtype == BF:
                return jnp.dot(weights, flat, preferred_element_type=F32)
            return jnp.dot(weights, flat.astype(F32), precision=lax.Precision.HIGHEST)

        def slots_of(pack, ids):
            keys = choose(pack, ids, 0)[:, 1].reshape(len(ids), ep_size, slot_cap)
            return keys.transpose(1, 0, 2).reshape(-1, 1)

        def finish(ids, pack, owns, pieces, recvs, known=(), early=(), steps=3):
            keys = [slots_of(pack, i) for i in (ids, early) if i]
            sizes = [len(i) * slot_cap for i in (ids, early) if i for _ in range(ep_size)]
            out = finish_call(owns, pieces, recvs, jnp.concatenate(keys), known, sizes, steps)
            back = send_back(out[:ep_size])
            return back, out[ep_size:]

        y_back, _ = finish(range(local), pack_y, [y_mine],
                           [(0, 0, 0, Y_FIRST), (0, Y_FIRST, Y_FIRST, USUAL - Y_FIRST), (0, USUAL, USUAL, TOTAL - USUAL)],
                           [y0, y1, y2])
        piece = [(0, 0, 0, V_FIRST)] + [(1, V_CUTS[n] - V_FIRST, V_CUTS[n], V_CUTS[n + 1] - V_CUTS[n]) for n in range(2)]
        late = [(0,) + p[1:] for p in piece[1:]]
        last = [(0, V_CUTS[n] - V_CUTS[2], V_CUTS[n], V_CUTS[n + 1] - V_CUTS[n]) for n in (2, 3)]
        whole0, whole1, whole2, whole3 = (3, 4, 5), (6, 7, 1), (2,), (0,)
        back0, _ = finish(whole0, pack_v, [v_mine0], piece[:1], [v0])
        out_sum = mix(own_mul, y_back, range(local))
        back1, _ = finish(whole1, pack_v, [after(v_mine0, back0[0], out_sum), v_mine1], piece[:2], [v0, v1])
        dx_early = mix(own_pick, back0, whole0)
        v4 = extra(after(v_extra, dx_early))
        back2, known = finish(whole2, pack_v, [after(v_mine1, back1[0], v4)], late, [v1, v2], early=whole3)
        back3, _ = finish(whole3, pack_v, [after(v_mine3, back2[0])], last, [v3, v4], known=known, steps=1)
        dx_early = dx_early + mix(own_pick, back1, whole1)
        dx_early = mix(own_pick, back2, whole2) + dx_early
        dx_sum = mix(own_pick, after(tuple(back3), dx_early), whole3) + dx_early

        def exchange_all(args):
            hid, one0, one1, three0, three1, own_mul, own_pick = args
            d_one, d_three = jnp.concatenate([one0, one1]), jnp.concatenate([three0, three1])

            def back(part):
                recv = swap(part[:, :half], 1, 0)
                done = (part[:, half:] + recv).astype(BF).reshape(local, ep_size, slot_cap, width)
                return send_back([done[:, s].reshape(-1, width) for s in range(ep_size)])

            part_out = jnp.einsum("enf,efd->end", hid, w_two, preferred_element_type=F32)
            part_dx = jnp.einsum("enf,edf->end", d_one, w_one, preferred_element_type=F32)
            part_dx += jnp.einsum("enf,edf->end", d_three, w_three, preferred_element_type=F32)
            return mix(own_mul, back(part_out), range(local)), mix(own_pick, back(part_dx), range(local))

        def exchange_none(args):
            zero = jnp.zeros((tok_dev, width), F32)
            return zero, zero

        out_full, dx_full = lax.cond(full, exchange_all, exchange_none, (hid, one0, one1, three0, three1, own_mul, own_pick))
        out_rows = jnp.where(full, out_full, out_sum).astype(BF)
        dx_rows = jnp.where(full, dx_full, dx_sum).astype(BF)
        return out_rows, dx_rows, *grads

    return jax.shard_map(local_step, mesh=mesh,
                         in_specs=(row_spec, row_spec, row_spec, col_spec, col_spec, down_spec, row_spec),
                         out_specs=(row_spec, row_spec, grad_col, grad_col, grad_down), check_vma=False)
```

```python
import functools

import jax
import jax.numpy as jnp
from jax import lax
from jax.experimental import pallas as pl
from jax.experimental.pallas import tpu as pltpu
from jax.sharding import PartitionSpec as P


BF = jnp.bfloat16
F32 = jnp.float32
MESH = pl.DeviceIdType.MESH

LEAD = 3
USUAL, TOTAL = 552, 616
Y_FIRST, Y_MOST = 184, 240
V_FIRST, V_MOST = 280, 376
V_CUTS = (280, 456, 512, 552, 616)
WINDOW = 104
VMEM_LIMIT = 62 * 2**20


def slot_count(num_top, tok_dev, experts):
    return 8 * ((5 * num_top * tok_dev + 32 * experts - 1) // (32 * experts))


def dot(a, b, ca, cb):
    return lax.dot_general(a, b, (((ca,), (cb,)), ((), ())), preferred_element_type=F32)


def place(rows, keys, cap):
    pick = lax.broadcasted_iota(jnp.int32, (cap, keys.shape[1]), 0).astype(F32) == keys
    return dot(jnp.where(pick, 1.0, 0.0).astype(BF), rows, 1, 0).astype(BF)


def add_window(ref, part, keys, shift, terms):
    half = keys.shape[1]
    rows = slice(part * half, (part + 1) * half)
    keys = keys[part:part + 1, :]
    first = jnp.min(jnp.where(keys >= 0.0, keys, float(TOTAL))).astype(jnp.int32)
    start = jnp.clip((first - shift) // 8 * 8, 0, ref.shape[0] - WINDOW)
    at = keys - (start + shift).astype(F32)
    product = sum(dot(place(left[rows], at, WINDOW), right, 1, dim) for left, right, dim in terms)
    ref[pl.ds(pl.multiple_of(start, 8), WINDOW), :] += product


def cut(source, refs):
    row = 0
    for ref in refs:
        ref[...] = source[row:row + ref.shape[0]]
        row += ref.shape[0]


def fwd_kernel(x_ref, w1_ref, w3_ref, w2_ref, key_ref, spill_ref, a_ref, b_ref, h_ref, other_ref, extra_ref, mine_ref, other):
    step = pl.program_id(0)

    @pl.when(step == 0)
    def _():
        mine_ref[...] = jnp.zeros_like(mine_ref)
        other[...] = jnp.zeros_like(other)
        other[:spill_ref.shape[0], :] = spill_ref[...]

    x = x_ref[0]
    a = dot(x, w1_ref[0], 1, 0)
    b = dot(x, w3_ref[0], 1, 0)
    h = (a * jax.nn.sigmoid(a) * b).astype(BF)
    a_ref[0] = a
    b_ref[0] = b
    h_ref[0] = h
    add_window(mine_ref, 1, key_ref[0], 0, [(h, w2_ref[0], 0)])

    @pl.when(step >= LEAD)
    def _():
        add_window(other, 0, key_ref[0], Y_FIRST, [(h_ref[0], w2_ref[0], 0)])

    @pl.when(step == pl.num_programs(0) - 1)
    def _():
        cut(other, (other_ref, extra_ref))


def bwd_step(shift, u_ref, w1_ref, w3_ref, w2_ref, key_ref, a_ref, b_ref, da_ref, db_ref, parts):
    dh = dot(u_ref[0], w2_ref[0], 1, 1)
    a = a_ref[0]
    s = jax.nn.sigmoid(a)
    da = (dh * b_ref[0] * s * (1.0 + a * (1.0 - s))).astype(BF)
    db = (dh * (a * s)).astype(BF)
    da_ref[0] = da
    db_ref[0] = db
    for part, ref in enumerate(parts):
        add_window(ref, part, key_ref[0], shift, [(da, w1_ref[0], 1), (db, w3_ref[0], 1)])


def bwd_rest_kernel(u_ref, w1_ref, w3_ref, w2_ref, key_ref, a_ref, b_ref, da_ref, db_ref,
                    other_ref, spill_other_ref, mine_ref, spill_mine_ref, other, mine):
    step = pl.program_id(0)

    @pl.when(step == 0)
    def _():
        other[...] = jnp.zeros_like(other)
        mine[...] = jnp.zeros_like(mine)

    bwd_step(0, u_ref, w1_ref, w3_ref, w2_ref, key_ref, a_ref, b_ref, da_ref, db_ref, (other, mine))

    @pl.when(step == pl.num_programs(0) - 1)
    def _():
        cut(other, (other_ref, spill_other_ref))
        cut(mine, (mine_ref, spill_mine_ref))


def bwd_lead_kernel(u_ref, w1_ref, w3_ref, w2_ref, key_ref, a_ref, b_ref, spill_other_ref, spill_mine_ref,
                    da_ref, db_ref, other1_ref, other2_ref, other3_ref, extra_ref, mine_ref, mine3_ref, other, mine):
    step = pl.program_id(0)

    @pl.when(step == 0)
    def _():
        for ref, spill_ref in ((other, spill_other_ref), (mine, spill_mine_ref)):
            ref[...] = jnp.zeros_like(ref)
            ref[:spill_ref.shape[0], :] = spill_ref[...]

    bwd_step(V_FIRST, u_ref, w1_ref, w3_ref, w2_ref, key_ref, a_ref, b_ref, da_ref, db_ref, (other, mine))

    @pl.when(step == pl.num_programs(0) - 1)
    def _():
        cut(other, (other1_ref, other2_ref, other3_ref, extra_ref))
        cut(mine, (mine_ref, mine3_ref))


def finish_kernel(pieces, owns, known, *refs):
    own_refs, recv_refs, key_ref = refs[:owns], refs[owns:owns + len(pieces)], refs[owns + len(pieces)]
    known_refs = refs[owns + len(pieces) + 1:][:known]
    out_refs = refs[owns + len(pieces) + 1 + known:]
    done = [(own_refs[i][row:row + count, :] + recv_ref[...]).astype(BF)
            for (i, row, _, count), recv_ref in zip(pieces, recv_refs)]
    total = None
    for (_, _, position, count), values in zip(pieces, done):
        pick = lax.broadcasted_iota(jnp.int32, (key_ref.shape[0], count), 1).astype(F32) == key_ref[...] - float(position)
        term = dot(jnp.where(pick, 1.0, 0.0).astype(BF), values, 1, 0)
        total = term if total is None else total + term
    first = 0
    for i, out_ref in enumerate(out_refs):
        rows = total[first:first + out_ref.shape[0]]
        first += out_ref.shape[0]
        if known:
            rows = rows + known_refs[i][...].astype(F32)
        out_ref[...] = rows.astype(BF)


def grad_kernel(x_ref, u_ref, h_ref, da0_ref, db0_ref, da1_ref, db1_ref, g1_ref, g3_ref, g2_ref):
    x = x_ref[0]
    lead = pl.program_id(0) < LEAD
    g1_ref[0] = dot(x, jnp.where(lead, da0_ref[0], da1_ref[0]), 0, 0).astype(BF)
    g3_ref[0] = dot(x, jnp.where(lead, db0_ref[0], db1_ref[0]), 0, 0).astype(BF)
    g2_ref[0] = dot(h_ref[0], u_ref[0], 0, 0).astype(BF)


def spec(shape, first):
    return pl.BlockSpec((1,) + shape, lambda i: (i + first, 0, 0))


def whole(shape):
    return pl.BlockSpec(shape, lambda i: (0,) * len(shape))


def cost(flops, nbytes):
    return pl.CostEstimate(flops=flops, bytes_accessed=nbytes, transcendentals=0)


PARAMS = pltpu.CompilerParams(dimension_semantics=("arbitrary",), vmem_limit_bytes=VMEM_LIMIT)


def expert_call(body, first, count, rows_in, w1, w3, w2, keys, saved, extra, kinds, outs, scratch):
    rows, d, f = rows_in.shape[1], w1.shape[1], w1.shape[2]
    half = rows // 2
    shapes = [((count, rows, f), t) for t in kinds] + [((n, d), F32) for n in outs]
    return pl.pallas_call(
        body, grid=(count,),
        in_specs=[spec((rows, d), first), spec((d, f), first), spec((d, f), first), spec((f, d), first),
                  spec((2, half), first)] + [spec((rows, f), first)] * len(saved) + [whole(e.shape) for e in extra],
        out_specs=[spec(s[1:], 0) if len(s) == 3 else whole(s) for s, _ in shapes],
        out_shape=[jax.ShapeDtypeStruct(s, t) for s, t in shapes],
        scratch_shapes=[pltpu.VMEM((n, d), F32) for n in scratch],
        compiler_params=PARAMS, cost_estimate=cost(count * 8 * rows * d * f, count * (6 * d * f + 6 * rows * d)),
    )(rows_in, w1, w3, w2, keys, *saved, *extra)


def grad_call(xs, us, h, lead, rest):
    count, rows, d = xs.shape
    f = h.shape[2]
    outs = [((d, f), BF), ((d, f), BF), ((f, d), BF)]
    return pl.pallas_call(
        grad_kernel, grid=(count,), name="wgrad",
        in_specs=[spec((rows, d), 0), spec((rows, d), 0), spec((rows, f), 0)]
        + [pl.BlockSpec((1, rows, f), lambda i: (jnp.minimum(i, LEAD - 1), 0, 0))] * 2
        + [pl.BlockSpec((1, rows, f), lambda i: (jnp.maximum(i - LEAD, 0), 0, 0))] * 2,
        out_specs=[spec(s, 0) for s, _ in outs],
        out_shape=[jax.ShapeDtypeStruct((count,) + s, t) for s, t in outs],
        compiler_params=PARAMS, cost_estimate=cost(count * 6 * rows * d * f, count * (6 * d * f + 4 * rows * d)),
    )(xs, us, h, *lead, *rest)


def finish_call(owns, pieces, recvs, keys, known, sizes, steps):
    d = owns[0].shape[1]
    total = sum(r.shape[0] for r in recvs)

    def columns(rows):
        return pl.BlockSpec((rows, d // steps), lambda i: (0, i))

    return pl.pallas_call(
        functools.partial(finish_kernel, pieces, len(owns), len(known)), name="finish", grid=(steps,),
        in_specs=[columns(r.shape[0]) for r in (*owns, *recvs)] + [whole(keys.shape)] + [columns(r.shape[0]) for r in known],
        out_specs=[columns(rows) for rows in sizes],
        out_shape=[jax.ShapeDtypeStruct((rows, d), BF) for rows in sizes],
        compiler_params=PARAMS,
        cost_estimate=cost(2 * keys.shape[0] * d * total, 8 * total * d),
    )(*owns, *recvs, keys, *known)


ACROSS_Y, ACROSS_XY, OWN, ACROSS_X, CORE = 0, 1, 4, 5, 6
STEPS = ((1, 0), (1, 2), (1, 1), (1, 3), (0, 0), (0, 2), (0, 1), (0, 3))


def find_peers():
    tp, ep = lax.axis_index("tp"), lax.axis_index("ep")
    eps = {0: ep, 2: lax.rem(ep + 2, 4), 1: ep + 1 - 2 * lax.rem(ep, 2), 3: 3 - ep}
    return ep, [{"tp": 1 - tp if a else tp, "ep": eps[b]} for a, b in STEPS]


def meet(peers):
    barrier = pltpu.get_barrier_semaphore()
    for peer in peers:
        pl.semaphore_signal(barrier, inc=1, device_id=peer, device_id_type=MESH)
    pl.semaphore_wait(barrier, len(peers))


def dispatch(slot_cap, blocks, key_ref, gate_ref, out, out_hbm, sem, ready):
    local, width = key_ref.shape[1], key_ref.shape[2]

    @pl.loop(0, 4)
    def _(n):
        for at, step in enumerate(ready):
            pl.when(n == at)(step)
        first = lax.rem(OWN + 4 * n, 8) + 2 * (n // 2)
        one, two = key_ref[first], key_ref[first + 1]
        pair = jnp.concatenate([one, jnp.where(two >= 0.0, two + slot_cap, -1.0)], axis=1)
        index = lax.broadcasted_iota(jnp.int32, (2 * slot_cap, 2 * width), 0).astype(F32)
        picks = [index == pair[e:e + 1, :] for e in range(local)]
        pick = jnp.concatenate([jnp.where(p, 1.0, 0.0) for p in picks], axis=0).astype(BF)
        rows = dot(pick, blocks[pl.ds(first, 2)].reshape(2 * width, out.shape[2]), 1, 0)
        if gate_ref is not None:
            gates = jnp.concatenate([gate_ref[first], gate_ref[first + 1]], axis=1)
            scale = jnp.concatenate([jnp.where(p, gates[e:e + 1, :], 0.0) for e, p in enumerate(picks)], axis=0)
            rows = rows * jnp.sum(scale, axis=1, keepdims=True)
        rows = rows.astype(BF)
        at = pl.ds(pl.multiple_of(first * slot_cap, 2 * slot_cap), 2 * slot_cap)
        for e in range(local):
            out[e, at, :] = rows[e * 2 * slot_cap:(e + 1) * 2 * slot_cap]
        pltpu.make_async_copy(out.at[:, at], out_hbm.at[:, at], sem.at[n]).start()


def dispatch_done(slot_cap, out, out_hbm, sem):
    for n in range(4):
        at = pl.ds(2 * slot_cap * n, 2 * slot_cap)
        pltpu.make_async_copy(out.at[:, at], out_hbm.at[:, at], sem.at[n]).wait()


def prologue_kernel(slot_cap, tok_ref, dout_ref, id_ref, val_ref, w1_hbm, w3_hbm, w2_hbm,
                    xs_hbm, yo_hbm, spill_hbm, key_ref, gate_ref, pack_y_ref, pack_v_ref, aux_all_ref, across_ref,
                    gathered, aux_ref, aux_all, xs, w13, w2, yo,
                    row_send, row_recv, aux_send, aux_recv, side_send, side_recv, in_sem, out_sem, row_out):
    ep, peers = find_peers()
    others = [k for k in range(8) if k != OWN]
    local, width = key_ref.shape[1], key_ref.shape[2]
    num_top, half = id_ref.shape[0], 4 * slot_cap

    aux_ref[...] = jnp.concatenate([id_ref[...].astype(F32), val_ref[...]], axis=0)
    lead, hidden = w2.shape[0], w2.shape[1]
    loads = [pltpu.make_async_copy(w.at[pl.ds(0, lead)], buf, in_sem.at[n]) for n, (w, buf) in enumerate(
        ((w1_hbm, w13.at[:, :, pl.ds(0, hidden)]), (w3_hbm, w13.at[:, :, pl.ds(hidden, hidden)]), (w2_hbm, w2)))]
    for c in loads:
        c.start()
    meet([peers[k] for k in others])

    def aux_copy(k):
        return pltpu.make_async_remote_copy(aux_ref, aux_all.at[k], aux_send.at[k], aux_recv.at[k],
                                            device_id=peers[k], device_id_type=MESH)

    def copy(slot, part):
        if slot in (ACROSS_Y, ACROSS_X, CORE):
            source, peer = tok_ref.at[part], slot
        elif slot == ACROSS_XY:
            source, peer = (gathered.at[ACROSS_Y, 0], ACROSS_X) if part == 0 else (gathered.at[ACROSS_X, 1], ACROSS_Y)
        else:
            source, peer = gathered.at[slot - 2, part], CORE
        return pltpu.make_async_remote_copy(source, gathered.at[slot, part], row_send.at[slot, part],
                                            row_recv.at[slot, part], device_id=peers[peer], device_id_type=MESH)

    def side_copy():
        return pltpu.make_async_remote_copy(dout_ref, across_ref, side_send, side_recv,
                                            device_id=peers[ACROSS_Y], device_id_type=MESH)

    def relay(slot, part):
        copy(slot, part).wait_recv()
        if (slot, part) in ((ACROSS_Y, 0), (ACROSS_X, 1)):
            copy(ACROSS_XY, part).start()
        copy(slot + 2, part).start()

    def arrive(*slots):
        for slot in slots:
            for part in (0, 1):
                copy(slot, part).wait_recv()

    for k in others:
        aux_copy(k).start()
    for slot, part in ((ACROSS_Y, 0), (ACROSS_X, 1), (ACROSS_Y, 1), (ACROSS_X, 0), (CORE, 0), (CORE, 1)):
        copy(slot, part).start()
    gathered[OWN] = tok_ref[...]
    aux_all[OWN] = aux_ref[...]

    for k in others:
        aux_copy(k).wait_recv()
    aux_all_ref[...] = aux_all[...]
    expert = (lax.broadcasted_iota(jnp.int32, (local, width), 0) + ep * local).astype(F32)
    hits = []
    for k in range(8):
        a = aux_all[k]
        hit, gate = jnp.zeros((local, width), F32), jnp.zeros((local, width), F32)
        for j in range(num_top):
            eq = a[j:j + 1, :] == expert
            hit = jnp.where(eq, 1.0, hit)
            gate = jnp.where(eq, a[num_top + j:num_top + j + 1, :], gate)
        hits.append(hit)
        gate_ref[k] = gate
    hit = jnp.concatenate(hits, axis=0)
    upper = lax.broadcasted_iota(jnp.int32, (width, width), 0) < lax.broadcasted_iota(jnp.int32, (width, width), 1)
    pos = dot(hit.astype(BF), jnp.where(upper, 1.0, 0.0).astype(BF), 1, 0)
    kept = jnp.where(pos < slot_cap, hit, 0.0)
    key = jnp.where(kept > 0.0, pos, -1.0)
    number = jnp.broadcast_to(jnp.sum(kept, axis=1, keepdims=True), key.shape)
    total = 8 * local
    row = lax.broadcasted_iota(jnp.int32, (total, total), 0)
    col = lax.broadcasted_iota(jnp.int32, (total, total), 1)
    rb, re, cb, ce = row // local, lax.rem(row, local), col // local, lax.rem(col, local)
    rank_row = jnp.where(re < LEAD, lax.rem(re + LEAD - 1, LEAD), re)
    rank_col = jnp.where(ce < LEAD, lax.rem(ce + LEAD - 1, LEAD), ce)
    before = jnp.logical_and(rb // 4 == cb // 4, (re < LEAD) == (ce < LEAD))
    before = jnp.logical_and(before, jnp.logical_or(rank_col < rank_row, jnp.logical_and(ce == re, cb < rb)))
    base = dot(jnp.where(before, 1.0, 0.0).astype(BF), number.astype(BF), 1, 0)
    source = lax.broadcasted_iota(jnp.int32, key.shape, 0)
    leading = lax.rem(source, local) < LEAD
    is_lead = lax.broadcasted_iota(jnp.int32, (local, width), 0) < LEAD
    lane = lax.broadcasted_iota(jnp.int32, (local, half), 1)
    slot, block = lax.rem(lane, slot_cap).astype(F32), lane // slot_cap
    for k in range(8):
        key_ref[k] = key[k * local:(k + 1) * local]
    for part in range(2):
        here = source // (4 * local) == part
        lead_rows = jnp.sum(jnp.where(jnp.logical_and(here, leading), number, 0.0), axis=0, keepdims=True)
        rest_rows = jnp.sum(jnp.where(jnp.logical_and(here, jnp.logical_not(leading)), number, 0.0), axis=0, keepdims=True)
        shift_y = jnp.where(is_lead, 0.0, jnp.maximum(lead_rows, float(Y_FIRST)))
        shift_v = jnp.where(is_lead, jnp.maximum(rest_rows, float(V_FIRST)), 0.0)
        count, start = jnp.zeros((local, half), F32), jnp.zeros((local, half), F32)
        for n in range(4):
            k = (4 * part + n) * local
            count = jnp.where(block == n, number[k:k + local, :half], count)
            start = jnp.where(block == n, base[k:k + local, :half], start)
        for shift, pack_ref in ((shift_y, pack_y_ref), (shift_v, pack_v_ref)):
            packed = jnp.where(slot < count, start + slot + shift[:, :half], -1.0)
            for e in range(local):
                pack_ref[e, part:part + 1, :] = packed[e:e + 1]

    relay(ACROSS_Y, 0)
    relay(ACROSS_X, 1)
    side_copy().start()

    def second():
        relay(ACROSS_Y, 1)
        relay(ACROSS_X, 0)

    def third():
        relay(ACROSS_XY, 0)
        relay(ACROSS_XY, 1)

    dispatch(slot_cap, gathered, key_ref, None, xs, xs_hbm, row_out,
             [second, third, lambda: arrive(CORE, CORE + 1), lambda: arrive(2, 3)])
    for c in loads:
        c.wait()

    @pl.loop(0, lead)
    def _(e):
        act = dot(xs[e, :half], w13[e], 1, 0)
        a, b = act[:, :hidden], act[:, hidden:]
        h = (a * jax.nn.sigmoid(a) * b).astype(BF)
        packed = dot(place(h, pack_y_ref[e, 0:1, :], Y_MOST), w2[e], 1, 0)

        @pl.when(e == 0)
        def _():
            yo[...] = packed

        @pl.when(e > 0)
        def _():
            yo[...] += packed

    stores = [pltpu.make_async_copy(yo.at[pl.ds(0, Y_FIRST)], yo_hbm, out_sem.at[0]),
              pltpu.make_async_copy(yo.at[pl.ds(Y_FIRST, Y_MOST - Y_FIRST)], spill_hbm, out_sem.at[1])]
    for c in stores:
        c.start()
    for k in others:
        aux_copy(k).wait_send()
        for part in (0, 1):
            copy(k, part).wait_send()
    side_copy().wait()
    dispatch_done(slot_cap, xs, xs_hbm, row_out)
    for c in stores:
        c.wait()


def spread_kernel(slot_cap, dout_ref, across_ref, key_ref, gate_ref, us_hbm, gathered, us, row_send, row_recv, row_out):
    _, peers = find_peers()
    meet([peers[ACROSS_X], peers[CORE]])

    def copy(slot, part):
        if slot in (ACROSS_X, CORE):
            source, peer = dout_ref.at[part], slot
        elif slot in (ACROSS_XY, 2):
            source, peer = across_ref.at[part], ACROSS_X if slot == ACROSS_XY else CORE
        else:
            source, peer = gathered.at[slot - 2, part], CORE
        return pltpu.make_async_remote_copy(source, gathered.at[slot, part], row_send.at[slot, part],
                                            row_recv.at[slot, part], device_id=peers[peer], device_id_type=MESH)

    sent = [ACROSS_X, ACROSS_XY, CORE, 2, CORE + 1, 3]
    for slot in sent[:4]:
        for part in (0, 1):
            copy(slot, part).start()
    gathered[OWN] = dout_ref[...]
    gathered[ACROSS_Y] = across_ref[...]

    def relay(slot):
        for part in (0, 1):
            copy(slot, part).wait_recv()
            copy(slot + 2, part).start()

    def arrive(*slots):
        for slot in slots:
            for part in (0, 1):
                copy(slot, part).wait_recv()

    dispatch(slot_cap, gathered, key_ref, gate_ref, us, us_hbm, row_out,
             [lambda: relay(ACROSS_X), lambda: relay(ACROSS_XY), lambda: arrive(CORE, CORE + 1), lambda: arrive(2, 3)])
    for slot in sent:
        for part in (0, 1):
            copy(slot, part).wait_send()
    dispatch_done(slot_cap, us, us_hbm, row_out)


VMEM = pl.BlockSpec(memory_space=pltpu.VMEM)
ANY = pl.BlockSpec(memory_space=pl.ANY)
DMA = pltpu.SemaphoreType.DMA


def prologue_call(tokens, d_out, ids, gates, w1, w3, w2, slot_cap):
    num_top, tok_dev = ids.shape
    width, local, f = tokens.shape[2], w1.shape[0], w1.shape[2]
    rows, aux = 8 * slot_cap, (2 * num_top, tok_dev)
    large = [((local, rows, width), BF), ((Y_FIRST, width), F32), ((Y_MOST - Y_FIRST, width), F32)]
    small = [((8, local, tok_dev), F32)] * 2 + [((local, 2, rows // 2), F32)] * 2
    small += [((8,) + aux, F32), (tokens.shape, BF)]
    scratch = [((8,) + tokens.shape, BF), (aux, F32), ((8,) + aux, F32), large[0]]
    scratch += [((LEAD, width, 2 * f), BF), ((LEAD, f, width), BF), ((Y_MOST, width), F32)]
    return pl.pallas_call(
        functools.partial(prologue_kernel, slot_cap), name="prologue",
        in_specs=[VMEM] * 4 + [ANY] * 3,
        out_specs=[ANY] * len(large) + [VMEM] * len(small),
        out_shape=[jax.ShapeDtypeStruct(s, t) for s, t in large + small],
        scratch_shapes=[pltpu.VMEM(s, t) for s, t in scratch]
        + [DMA((8, 2)), DMA((8, 2)), DMA((8,)), DMA((8,)), DMA, DMA, DMA((3,)), DMA((2,)), DMA((4,))],
        compiler_params=pltpu.CompilerParams(collective_id=0, has_side_effects=True, vmem_limit_bytes=VMEM_LIMIT),
        cost_estimate=cost(10**10, 3 * 10**7),
    )(tokens, d_out, ids, gates, w1, w3, w2)


def spread_call(d_out, across, key, gate, slot_cap):
    local = key.shape[1]
    out = (local, 8 * slot_cap, d_out.shape[2])
    return pl.pallas_call(
        functools.partial(spread_kernel, slot_cap), name="spread",
        in_specs=[VMEM] * 4, out_specs=ANY, out_shape=jax.ShapeDtypeStruct(out, BF),
        scratch_shapes=[pltpu.VMEM((8,) + d_out.shape, BF), pltpu.VMEM(out, BF), DMA((8, 2)), DMA((8, 2)), DMA((4,))],
        compiler_params=pltpu.CompilerParams(collective_id=1, has_side_effects=True, vmem_limit_bytes=VMEM_LIMIT),
        cost_estimate=cost(10**10, 3 * 10**7),
    )(d_out, across, key, gate)


def solution(mesh):
    tp_size, ep_size = mesh.shape["tp"], mesh.shape["ep"]
    row_spec = P(("dp", "ep", "tp"), None)
    col_spec = P("ep", None, "tp")
    down_spec = P("ep", "tp", None)
    grad_col = P(("dp", "ep"), None, "tp")
    grad_down = P(("dp", "ep"), "tp", None)

    def swap(z, tp_bit, ep_bits):
        pairs = [(t * ep_size + e, (t ^ tp_bit) * ep_size + (e ^ ep_bits)) for t in range(tp_size) for e in range(ep_size)]
        return lax.ppermute(z, ("tp", "ep"), pairs)

    def local_step(tokens, expert_ids, gate_vals, w_one, w_three, w_two, d_out):
        tok_dev, width = tokens.shape
        num_top = expert_ids.shape[1]
        local = w_one.shape[0]
        experts = local * ep_size
        slot_cap = slot_count(num_top, tok_dev, experts)
        half = tp_size * ep_size * slot_cap // 2
        ep_here = lax.axis_index("ep")

        blocked = (2, tok_dev // 2, width)
        d_blocked = d_out.reshape(blocked)
        xs, y_other0, y_spill, key, gate, pack_y, pack_v, aux_all, across = prologue_call(
            tokens.reshape(blocked), d_blocked, expert_ids.T, gate_vals.T, w_one, w_three, w_two, slot_cap)
        y0 = swap(y_other0, 1, 0)
        rest = local - LEAD
        act_one, act_three, hid, y_other1, y_extra, y_mine = expert_call(
            fwd_kernel, 0, local, xs, w_one, w_three, w_two, pack_y, [], [y_spill],
            [F32, F32, BF], (USUAL - Y_FIRST, TOTAL - USUAL, TOTAL), (TOTAL - Y_FIRST,))
        y1 = swap(y_other1, 1, 0)
        across = lax.optimization_barrier((across, hid))[0]
        us = spread_call(d_blocked, across, key, gate, slot_cap)

        every = jnp.arange(experts, dtype=F32)[None, :, None]
        count_all = sum(jnp.sum(aux_all[:, j:j + 1, :] == every, axis=2, dtype=jnp.int32) for j in range(num_top))
        kept = jnp.minimum(count_all, slot_cap).reshape(2, ep_size, ep_size, local).sum(axis=1)
        lead_rows, rest_rows = kept[:, :, :LEAD].sum(axis=2), kept[:, :, LEAD:].sum(axis=2)
        v_rest = jnp.maximum(rest_rows, V_FIRST)
        most = jnp.maximum(jnp.maximum(lead_rows, Y_FIRST) + rest_rows, v_rest + lead_rows)
        more = jnp.any(most > USUAL)
        full = jnp.any((lead_rows > Y_MOST) | (rest_rows > V_MOST) | (most > TOTAL)
                       | (v_rest + lead_rows - kept[:, :, 0] > V_CUTS[2]) | (v_rest + kept[:, :, 1] > V_CUTS[1])
                       | (kept[:, :, LEAD:LEAD + 3].sum(axis=2) > V_FIRST))

        def after(value, *others):
            return lax.optimization_barrier((value,) + others)[0]

        def extra(rows):
            return lax.cond(more, lambda z: swap(z, 1, 0), lambda z: z, rows)

        saved = [act_one, act_three]
        spill = V_MOST - V_FIRST
        tail = TOTAL - V_FIRST
        one1, three1, v_other0, spill_other, v_mine0, spill_mine = expert_call(
            bwd_rest_kernel, LEAD, rest, us, w_one, w_three, w_two, pack_v, saved, [],
            [BF, BF], (V_FIRST, spill, V_FIRST, spill), (V_MOST, V_MOST))
        y2 = extra(after(y_extra, v_mine0))
        v0 = swap(after(v_other0, y2), 1, 0)
        one0, three0, v_other1, v_other2, v_other3, v_extra, v_mine1, v_mine3 = expert_call(
            bwd_lead_kernel, 0, LEAD, us, w_one, w_three, w_two, pack_v, saved,
            [spill_other, spill_mine], [BF, BF],
            tuple(V_CUTS[n + 1] - V_CUTS[n] for n in range(4)) + (V_CUTS[2] - V_FIRST, TOTAL - V_CUTS[2]), (tail, tail))
        v1 = swap(v_other1, 1, 0)
        v2 = swap(v_other2, 1, 0)
        v3 = swap(v_other3, 1, 0)

        grads = grad_call(xs, us, hid, (one0, three0), (one1, three1))

        sources = jnp.stack([ep_here, ep_here ^ 2, ep_here ^ 1, ep_here ^ 3])
        all_ids = (sources[:, None] * local + jnp.arange(local)).reshape(-1)
        eq = expert_ids[:, :, None] == all_ids
        hit = jnp.any(eq, axis=1)
        lower = (jnp.arange(tok_dev)[:, None] > jnp.arange(tok_dev)[None, :]).astype(BF)
        pos = jnp.dot(lower, hit.astype(BF), preferred_element_type=F32)
        own_gate = jnp.sum(jnp.where(eq, gate_vals[:, :, None], 0.0), axis=1)
        own_pick = hit[:, :, None] & (pos[:, :, None] == jnp.arange(slot_cap, dtype=F32))
        own_mul = jnp.where(own_pick, own_gate[:, :, None], 0.0).reshape(tok_dev, ep_size, local, slot_cap)
        own_pick = own_pick.astype(BF).reshape(tok_dev, ep_size, local, slot_cap)

        def send_back(parts):
            back = [parts[0]]
            for n, bits in ((1, 2), (2, 1), (3, 3)):
                back.append(swap(parts[n], 0, bits))
            return back

        def choose(array, ids, axis):
            runs = []
            for e in ids:
                if runs and runs[-1][1] == e:
                    runs[-1][1] = e + 1
                else:
                    runs.append([e, e + 1])
            parts = [lax.slice_in_dim(array, *run, axis=axis) for run in runs]
            return parts[0] if len(parts) == 1 else jnp.concatenate(parts, axis=axis)

        def mix(weights, back, ids):
            flat = jnp.concatenate(back)
            weights = choose(weights, ids, 2).reshape(tok_dev, -1)
            if weights.dtype == BF:
                return jnp.dot(weights, flat, preferred_element_type=F32)
            return jnp.dot(weights, flat.astype(F32), precision=lax.Precision.HIGHEST)

        def slots_of(pack, ids):
            keys = choose(pack, ids, 0)[:, 1].reshape(len(ids), ep_size, slot_cap)
            return keys.transpose(1, 0, 2).reshape(-1, 1)

        def finish(ids, pack, owns, pieces, recvs, known=(), early=(), steps=1):
            keys = [slots_of(pack, i) for i in (ids, early) if i]
            sizes = [len(i) * slot_cap for i in (ids, early) if i for _ in range(ep_size)]
            out = finish_call(owns, pieces, recvs, jnp.concatenate(keys), known, sizes, steps)
            back = send_back(out[:ep_size])
            return back, out[ep_size:]

        y_back, _ = finish(range(local), pack_y, [y_mine],
                           [(0, 0, 0, Y_FIRST), (0, Y_FIRST, Y_FIRST, USUAL - Y_FIRST), (0, USUAL, USUAL, TOTAL - USUAL)],
                           [y0, y1, y2], steps=3)
        piece = [(0, 0, 0, V_FIRST)] + [(1, V_CUTS[n] - V_FIRST, V_CUTS[n], V_CUTS[n + 1] - V_CUTS[n]) for n in range(2)]
        late = [(0,) + p[1:] for p in piece[1:]]
        last = [(0, V_CUTS[n] - V_CUTS[2], V_CUTS[n], V_CUTS[n + 1] - V_CUTS[n]) for n in (2, 3)]
        whole0, whole1, whole2, whole3 = (3, 4, 5), (6, 7, 1), (2,), (0,)
        back0, _ = finish(whole0, pack_v, [v_mine0], piece[:1], [v0])
        out_sum = mix(own_mul, y_back, range(local))
        back1, _ = finish(whole1, pack_v, [after(v_mine0, back0[0], out_sum), v_mine1], piece[:2], [v0, v1])
        v4 = extra(after(v_extra, back1[0]))
        back2, known = finish(whole2, pack_v, [after(v_mine1, back1[0], v4)], late, [v1, v2], early=whole3)
        back3, _ = finish(whole3, pack_v, [after(v_mine3, back2[0])], last, [v3, v4], known=known)
        dx_early = mix(own_pick, after(tuple(back0), back3[0]), whole0)
        dx_early = dx_early + mix(own_pick, back1, whole1)
        dx_early = mix(own_pick, back2, whole2) + dx_early
        dx_sum = mix(own_pick, after(tuple(back3), dx_early), whole3) + dx_early

        def exchange_all(args):
            hid, one0, one1, three0, three1, own_mul, own_pick = args
            d_one, d_three = jnp.concatenate([one0, one1]), jnp.concatenate([three0, three1])

            def back(part):
                recv = swap(part[:, :half], 1, 0)
                done = (part[:, half:] + recv).astype(BF).reshape(local, ep_size, slot_cap, width)
                return send_back([done[:, s].reshape(-1, width) for s in range(ep_size)])

            part_out = jnp.einsum("enf,efd->end", hid, w_two, preferred_element_type=F32)
            part_dx = jnp.einsum("enf,edf->end", d_one, w_one, preferred_element_type=F32)
            part_dx += jnp.einsum("enf,edf->end", d_three, w_three, preferred_element_type=F32)
            return mix(own_mul, back(part_out), range(local)), mix(own_pick, back(part_dx), range(local))

        def exchange_none(args):
            zero = jnp.zeros((tok_dev, width), F32)
            return zero, zero

        out_full, dx_full = lax.cond(full, exchange_all, exchange_none, (hid, one0, one1, three0, three1, own_mul, own_pick))
        out_rows = jnp.where(full, out_full, out_sum).astype(BF)
        dx_rows = jnp.where(full, dx_full, dx_sum).astype(BF)
        return out_rows, dx_rows, *grads

    return jax.shard_map(local_step, mesh=mesh,
                         in_specs=(row_spec, row_spec, row_spec, col_spec, col_spec, down_spec, row_spec),
                         out_specs=(row_spec, row_spec, grad_col, grad_col, grad_down), check_vma=False)
```

```python
import functools

import jax
import jax.numpy as jnp
from jax import lax
from jax.experimental import pallas as pl
from jax.experimental.pallas import tpu as pltpu
from jax.sharding import PartitionSpec as P


BF = jnp.bfloat16
F32 = jnp.float32
MESH = pl.DeviceIdType.MESH

LEAD = 3
USUAL, TOTAL = 552, 584
Y_FIRST, Y_MOST = 184, 240
V_FIRST, V_MOST = 280, 376
V_CUTS = (280, 384, 456, 512, 552, 584)
WINDOW = 104
VMEM_LIMIT = 62 * 2**20


def slot_count(num_top, tok_dev, experts):
    return 8 * ((5 * num_top * tok_dev + 32 * experts - 1) // (32 * experts))


def dot(a, b, ca, cb):
    return lax.dot_general(a, b, (((ca,), (cb,)), ((), ())), preferred_element_type=F32)


def place(rows, keys, cap):
    pick = lax.broadcasted_iota(jnp.int32, (cap, keys.shape[1]), 0).astype(F32) == keys
    return dot(jnp.where(pick, 1.0, 0.0).astype(BF), rows, 1, 0).astype(BF)


def add_window(ref, part, keys, shift, terms):
    half = keys.shape[1]
    rows = slice(part * half, (part + 1) * half)
    keys = keys[part:part + 1, :]
    first = jnp.min(jnp.where(keys >= 0.0, keys, float(TOTAL))).astype(jnp.int32)
    start = jnp.clip((first - shift) // 8 * 8, 0, ref.shape[0] - WINDOW)
    at = keys - (start + shift).astype(F32)
    product = sum(dot(place(left[rows], at, WINDOW), right, 1, dim) for left, right, dim in terms)
    ref[pl.ds(pl.multiple_of(start, 8), WINDOW), :] += product


def cut(source, refs):
    row = 0
    for ref in refs:
        ref[...] = source[row:row + ref.shape[0]]
        row += ref.shape[0]


def fwd_kernel(x_ref, w1_ref, w3_ref, w2_ref, key_ref, spill_ref, a_ref, b_ref, h_ref, other_ref, extra_ref, mine_ref, other):
    step = pl.program_id(0)

    @pl.when(step == 0)
    def _():
        mine_ref[...] = jnp.zeros_like(mine_ref)
        other[...] = jnp.zeros_like(other)
        other[:spill_ref.shape[0], :] = spill_ref[...]

    x = x_ref[0]
    a = dot(x, w1_ref[0], 1, 0)
    b = dot(x, w3_ref[0], 1, 0)
    h = (a * jax.nn.sigmoid(a) * b).astype(BF)
    a_ref[0] = a
    b_ref[0] = b
    h_ref[0] = h
    add_window(mine_ref, 1, key_ref[0], 0, [(h, w2_ref[0], 0)])

    @pl.when(step >= LEAD)
    def _():
        add_window(other, 0, key_ref[0], Y_FIRST, [(h_ref[0], w2_ref[0], 0)])

    @pl.when(step == pl.num_programs(0) - 1)
    def _():
        cut(other, (other_ref, extra_ref))


def bwd_step(shift, u_ref, w1_ref, w3_ref, w2_ref, key_ref, a_ref, b_ref, da_ref, db_ref, parts):
    dh = dot(u_ref[0], w2_ref[0], 1, 1)
    a = a_ref[0]
    s = jax.nn.sigmoid(a)
    da = (dh * b_ref[0] * s * (1.0 + a * (1.0 - s))).astype(BF)
    db = (dh * (a * s)).astype(BF)
    da_ref[0] = da
    db_ref[0] = db
    for part, ref in enumerate(parts):
        add_window(ref, part, key_ref[0], shift, [(da, w1_ref[0], 1), (db, w3_ref[0], 1)])


def bwd_rest_kernel(u_ref, w1_ref, w3_ref, w2_ref, key_ref, a_ref, b_ref, da_ref, db_ref,
                    other_ref, spill_other_ref, mine_ref, spill_mine_ref, other, mine):
    step = pl.program_id(0)

    @pl.when(step == 0)
    def _():
        other[...] = jnp.zeros_like(other)
        mine[...] = jnp.zeros_like(mine)

    bwd_step(0, u_ref, w1_ref, w3_ref, w2_ref, key_ref, a_ref, b_ref, da_ref, db_ref, (other, mine))

    @pl.when(step == pl.num_programs(0) - 1)
    def _():
        cut(other, (other_ref, spill_other_ref))
        cut(mine, (mine_ref, spill_mine_ref))


def bwd_lead_kernel(u_ref, w1_ref, w3_ref, w2_ref, key_ref, a_ref, b_ref, spill_other_ref, spill_mine_ref,
                    da_ref, db_ref, other1_ref, other2_ref, other3_ref, other4_ref, extra_ref, mine_ref, mine4_ref, other, mine):
    step = pl.program_id(0)

    @pl.when(step == 0)
    def _():
        for ref, spill_ref in ((other, spill_other_ref), (mine, spill_mine_ref)):
            ref[...] = jnp.zeros_like(ref)
            ref[:spill_ref.shape[0], :] = spill_ref[...]

    bwd_step(V_FIRST, u_ref, w1_ref, w3_ref, w2_ref, key_ref, a_ref, b_ref, da_ref, db_ref, (other, mine))

    @pl.when(step == pl.num_programs(0) - 1)
    def _():
        cut(other, (other1_ref, other2_ref, other3_ref, other4_ref, extra_ref))
        cut(mine, (mine_ref, mine4_ref))


def finish_kernel(pieces, owns, known, ranges, *refs):
    own_refs, recv_refs, key_ref = refs[:owns], refs[owns:owns + len(pieces)], refs[owns + len(pieces)]
    known_refs = refs[owns + len(pieces) + 1:][:known]
    out_refs = refs[owns + len(pieces) + 1 + known:]
    done = [(own_refs[i][row:row + count, :] + recv_ref[...]).astype(BF)
            for (i, row, _, count), recv_ref in zip(pieces, recv_refs)]
    keys = jnp.concatenate([key_ref[start:stop, :] for start, stop in ranges], axis=0)
    total = None
    for (_, _, position, count), values in zip(pieces, done):
        pick = lax.broadcasted_iota(jnp.int32, (keys.shape[0], count), 1).astype(F32) == keys - float(position)
        term = dot(jnp.where(pick, 1.0, 0.0).astype(BF), values, 1, 0)
        total = term if total is None else total + term
    first = 0
    for i, out_ref in enumerate(out_refs):
        rows = total[first:first + out_ref.shape[0]]
        first += out_ref.shape[0]
        if known:
            rows = rows + known_refs[i][...].astype(F32)
        out_ref[...] = rows.astype(BF)


def grad_kernel(x_ref, u_ref, h_ref, da0_ref, db0_ref, da1_ref, db1_ref, g1_ref, g3_ref, g2_ref):
    x = x_ref[0]
    lead = pl.program_id(0) < LEAD
    g1_ref[0] = dot(x, jnp.where(lead, da0_ref[0], da1_ref[0]), 0, 0).astype(BF)
    g3_ref[0] = dot(x, jnp.where(lead, db0_ref[0], db1_ref[0]), 0, 0).astype(BF)
    g2_ref[0] = dot(h_ref[0], u_ref[0], 0, 0).astype(BF)


def spec(shape, first):
    return pl.BlockSpec((1,) + shape, lambda i: (i + first, 0, 0))


def whole(shape):
    return pl.BlockSpec(shape, lambda i: (0,) * len(shape))


def cost(flops, nbytes):
    return pl.CostEstimate(flops=flops, bytes_accessed=nbytes, transcendentals=0)


PARAMS = pltpu.CompilerParams(dimension_semantics=("arbitrary",), vmem_limit_bytes=VMEM_LIMIT)


def expert_call(body, first, count, rows_in, w1, w3, w2, keys, saved, extra, kinds, outs, scratch):
    rows, d, f = rows_in.shape[1], w1.shape[1], w1.shape[2]
    half = rows // 2
    shapes = [((count, rows, f), t) for t in kinds] + [((n, d), F32) for n in outs]
    return pl.pallas_call(
        body, grid=(count,),
        in_specs=[spec((rows, d), first), spec((d, f), first), spec((d, f), first), spec((f, d), first),
                  spec((2, half), first)] + [spec((rows, f), first)] * len(saved) + [whole(e.shape) for e in extra],
        out_specs=[spec(s[1:], 0) if len(s) == 3 else whole(s) for s, _ in shapes],
        out_shape=[jax.ShapeDtypeStruct(s, t) for s, t in shapes],
        scratch_shapes=[pltpu.VMEM((n, d), F32) for n in scratch],
        compiler_params=PARAMS, cost_estimate=cost(count * 8 * rows * d * f, count * (6 * d * f + 6 * rows * d)),
    )(rows_in, w1, w3, w2, keys, *saved, *extra)


def grad_call(xs, us, h, lead, rest):
    count, rows, d = xs.shape
    f = h.shape[2]
    outs = [((d, f), BF), ((d, f), BF), ((f, d), BF)]
    return pl.pallas_call(
        grad_kernel, grid=(count,), name="wgrad",
        in_specs=[spec((rows, d), 0), spec((rows, d), 0), spec((rows, f), 0)]
        + [pl.BlockSpec((1, rows, f), lambda i: (jnp.minimum(i, LEAD - 1), 0, 0))] * 2
        + [pl.BlockSpec((1, rows, f), lambda i: (jnp.maximum(i - LEAD, 0), 0, 0))] * 2,
        out_specs=[spec(s, 0) for s, _ in outs],
        out_shape=[jax.ShapeDtypeStruct((count,) + s, t) for s, t in outs],
        compiler_params=PARAMS, cost_estimate=cost(count * 6 * rows * d * f, count * (6 * d * f + 4 * rows * d)),
    )(xs, us, h, *lead, *rest)


def finish_call(owns, pieces, recvs, keys, ranges, known, sizes, steps):
    d = owns[0].shape[1]
    total = sum(r.shape[0] for r in recvs)

    def columns(rows):
        return pl.BlockSpec((rows, d // steps), lambda i: (0, i))

    return pl.pallas_call(
        functools.partial(finish_kernel, pieces, len(owns), len(known), ranges), name="finish", grid=(steps,),
        in_specs=[columns(r.shape[0]) for r in (*owns, *recvs)] + [whole(keys.shape)] + [columns(r.shape[0]) for r in known],
        out_specs=[columns(rows) for rows in sizes],
        out_shape=[jax.ShapeDtypeStruct((rows, d), BF) for rows in sizes],
        compiler_params=PARAMS,
        cost_estimate=cost(2 * sum(sizes) * d * total, 8 * total * d),
    )(*owns, *recvs, keys, *known)


ACROSS_Y, ACROSS_XY, OWN, ACROSS_X, CORE = 0, 1, 4, 5, 6
STEPS = ((1, 0), (1, 2), (1, 1), (1, 3), (0, 0), (0, 2), (0, 1), (0, 3))


def find_peers():
    tp, ep = lax.axis_index("tp"), lax.axis_index("ep")
    eps = {0: ep, 2: lax.rem(ep + 2, 4), 1: ep + 1 - 2 * lax.rem(ep, 2), 3: 3 - ep}
    return ep, [{"tp": 1 - tp if a else tp, "ep": eps[b]} for a, b in STEPS]


def meet(peers):
    barrier = pltpu.get_barrier_semaphore()
    for peer in peers:
        pl.semaphore_signal(barrier, inc=1, device_id=peer, device_id_type=MESH)
    pl.semaphore_wait(barrier, len(peers))


def dispatch(slot_cap, blocks, key_ref, gate_ref, out, out_hbm, sem, ready):
    local, width = key_ref.shape[1], key_ref.shape[2]

    @pl.loop(0, 4)
    def _(n):
        for at, step in enumerate(ready):
            pl.when(n == at)(step)
        first = lax.rem(OWN + 4 * n, 8) + 2 * (n // 2)
        one, two = key_ref[first], key_ref[first + 1]
        pair = jnp.concatenate([one, jnp.where(two >= 0.0, two + slot_cap, -1.0)], axis=1)
        index = lax.broadcasted_iota(jnp.int32, (2 * slot_cap, 2 * width), 0).astype(F32)
        picks = [index == pair[e:e + 1, :] for e in range(local)]
        pick = jnp.concatenate([jnp.where(p, 1.0, 0.0) for p in picks], axis=0).astype(BF)
        rows = dot(pick, blocks[pl.ds(first, 2)].reshape(2 * width, out.shape[2]), 1, 0)
        if gate_ref is not None:
            gates = jnp.concatenate([gate_ref[first], gate_ref[first + 1]], axis=1)
            scale = jnp.concatenate([jnp.where(p, gates[e:e + 1, :], 0.0) for e, p in enumerate(picks)], axis=0)
            rows = rows * jnp.sum(scale, axis=1, keepdims=True)
        rows = rows.astype(BF)
        at = pl.ds(pl.multiple_of(first * slot_cap, 2 * slot_cap), 2 * slot_cap)
        for e in range(local):
            out[e, at, :] = rows[e * 2 * slot_cap:(e + 1) * 2 * slot_cap]
        pltpu.make_async_copy(out.at[:, at], out_hbm.at[:, at], sem.at[n]).start()


def dispatch_done(slot_cap, out, out_hbm, sem):
    for n in range(4):
        at = pl.ds(2 * slot_cap * n, 2 * slot_cap)
        pltpu.make_async_copy(out.at[:, at], out_hbm.at[:, at], sem.at[n]).wait()


def prologue_kernel(slot_cap, tok_ref, dout_ref, id_ref, val_ref, w1_hbm, w3_hbm, w2_hbm,
                    xs_hbm, yo_hbm, spill_hbm, key_ref, gate_ref, pack_y_ref, pack_v_ref, aux_all_ref, across_ref,
                    gathered, aux_ref, aux_all, xs, w13, w2, yo,
                    row_send, row_recv, aux_send, aux_recv, side_send, side_recv, in_sem, out_sem, row_out):
    ep, peers = find_peers()
    others = [k for k in range(8) if k != OWN]
    local, width = key_ref.shape[1], key_ref.shape[2]
    num_top, half = id_ref.shape[0], 4 * slot_cap

    aux_ref[...] = jnp.concatenate([id_ref[...].astype(F32), val_ref[...]], axis=0)
    lead, hidden = w2.shape[0], w2.shape[1]
    loads = [pltpu.make_async_copy(w.at[pl.ds(0, lead)], buf, in_sem.at[n]) for n, (w, buf) in enumerate(
        ((w1_hbm, w13.at[:, :, pl.ds(0, hidden)]), (w3_hbm, w13.at[:, :, pl.ds(hidden, hidden)]), (w2_hbm, w2)))]
    for c in loads:
        c.start()
    meet([peers[k] for k in others])

    def aux_copy(k):
        return pltpu.make_async_remote_copy(aux_ref, aux_all.at[k], aux_send.at[k], aux_recv.at[k],
                                            device_id=peers[k], device_id_type=MESH)

    def copy(slot, part):
        if slot in (ACROSS_Y, ACROSS_X, CORE):
            source, peer = tok_ref.at[part], slot
        elif slot == ACROSS_XY:
            source, peer = (gathered.at[ACROSS_Y, 0], ACROSS_X) if part == 0 else (gathered.at[ACROSS_X, 1], ACROSS_Y)
        else:
            source, peer = gathered.at[slot - 2, part], CORE
        return pltpu.make_async_remote_copy(source, gathered.at[slot, part], row_send.at[slot, part],
                                            row_recv.at[slot, part], device_id=peers[peer], device_id_type=MESH)

    def side_copy():
        return pltpu.make_async_remote_copy(dout_ref, across_ref, side_send, side_recv,
                                            device_id=peers[ACROSS_Y], device_id_type=MESH)

    def relay(slot, part):
        copy(slot, part).wait_recv()
        if (slot, part) in ((ACROSS_Y, 0), (ACROSS_X, 1)):
            copy(ACROSS_XY, part).start()
        copy(slot + 2, part).start()

    def arrive(*slots):
        for slot in slots:
            for part in (0, 1):
                copy(slot, part).wait_recv()

    for k in others:
        aux_copy(k).start()
    for slot, part in ((ACROSS_Y, 0), (ACROSS_X, 1), (ACROSS_Y, 1), (ACROSS_X, 0), (CORE, 0), (CORE, 1)):
        copy(slot, part).start()
    gathered[OWN] = tok_ref[...]
    aux_all[OWN] = aux_ref[...]

    for k in others:
        aux_copy(k).wait_recv()
    aux_all_ref[...] = aux_all[...]
    expert = (lax.broadcasted_iota(jnp.int32, (local, width), 0) + ep * local).astype(F32)
    hits = []
    for k in range(8):
        a = aux_all[k]
        hit, gate = jnp.zeros((local, width), F32), jnp.zeros((local, width), F32)
        for j in range(num_top):
            eq = a[j:j + 1, :] == expert
            hit = jnp.where(eq, 1.0, hit)
            gate = jnp.where(eq, a[num_top + j:num_top + j + 1, :], gate)
        hits.append(hit)
        gate_ref[k] = gate
    hit = jnp.concatenate(hits, axis=0)
    upper = lax.broadcasted_iota(jnp.int32, (width, width), 0) < lax.broadcasted_iota(jnp.int32, (width, width), 1)
    pos = dot(hit.astype(BF), jnp.where(upper, 1.0, 0.0).astype(BF), 1, 0)
    kept = jnp.where(pos < slot_cap, hit, 0.0)
    key = jnp.where(kept > 0.0, pos, -1.0)
    number = jnp.broadcast_to(jnp.sum(kept, axis=1, keepdims=True), key.shape)
    total = 8 * local
    row = lax.broadcasted_iota(jnp.int32, (total, total), 0)
    col = lax.broadcasted_iota(jnp.int32, (total, total), 1)
    rb, re, cb, ce = row // local, lax.rem(row, local), col // local, lax.rem(col, local)
    rank_row = jnp.where(re < LEAD, lax.rem(re + LEAD - 1, LEAD), re)
    rank_col = jnp.where(ce < LEAD, lax.rem(ce + LEAD - 1, LEAD), ce)
    before = jnp.logical_and(rb // 4 == cb // 4, (re < LEAD) == (ce < LEAD))
    before = jnp.logical_and(before, jnp.logical_or(rank_col < rank_row, jnp.logical_and(ce == re, cb < rb)))
    base = dot(jnp.where(before, 1.0, 0.0).astype(BF), number.astype(BF), 1, 0)
    source = lax.broadcasted_iota(jnp.int32, key.shape, 0)
    leading = lax.rem(source, local) < LEAD
    is_lead = lax.broadcasted_iota(jnp.int32, (local, width), 0) < LEAD
    lane = lax.broadcasted_iota(jnp.int32, (local, half), 1)
    slot, block = lax.rem(lane, slot_cap).astype(F32), lane // slot_cap
    for k in range(8):
        key_ref[k] = key[k * local:(k + 1) * local]
    for part in range(2):
        here = source // (4 * local) == part
        lead_rows = jnp.sum(jnp.where(jnp.logical_and(here, leading), number, 0.0), axis=0, keepdims=True)
        rest_rows = jnp.sum(jnp.where(jnp.logical_and(here, jnp.logical_not(leading)), number, 0.0), axis=0, keepdims=True)
        shift_y = jnp.where(is_lead, 0.0, jnp.maximum(lead_rows, float(Y_FIRST)))
        shift_v = jnp.where(is_lead, jnp.maximum(rest_rows, float(V_FIRST)), 0.0)
        count, start = jnp.zeros((local, half), F32), jnp.zeros((local, half), F32)
        for n in range(4):
            k = (4 * part + n) * local
            count = jnp.where(block == n, number[k:k + local, :half], count)
            start = jnp.where(block == n, base[k:k + local, :half], start)
        for shift, pack_ref in ((shift_y, pack_y_ref), (shift_v, pack_v_ref)):
            packed = jnp.where(slot < count, start + slot + shift[:, :half], -1.0)
            for e in range(local):
                pack_ref[e, part:part + 1, :] = packed[e:e + 1]

    relay(ACROSS_Y, 0)
    relay(ACROSS_X, 1)
    side_copy().start()

    def second():
        relay(ACROSS_Y, 1)
        relay(ACROSS_X, 0)

    def third():
        relay(ACROSS_XY, 0)
        relay(ACROSS_XY, 1)

    dispatch(slot_cap, gathered, key_ref, None, xs, xs_hbm, row_out,
             [second, third, lambda: arrive(CORE, CORE + 1), lambda: arrive(2, 3)])
    for c in loads:
        c.wait()

    @pl.loop(0, lead)
    def _(e):
        act = dot(xs[e, :half], w13[e], 1, 0)
        a, b = act[:, :hidden], act[:, hidden:]
        h = (a * jax.nn.sigmoid(a) * b).astype(BF)
        packed = dot(place(h, pack_y_ref[e, 0:1, :], Y_MOST), w2[e], 1, 0)

        @pl.when(e == 0)
        def _():
            yo[...] = packed

        @pl.when(e > 0)
        def _():
            yo[...] += packed

    stores = [pltpu.make_async_copy(yo.at[pl.ds(0, Y_FIRST)], yo_hbm, out_sem.at[0]),
              pltpu.make_async_copy(yo.at[pl.ds(Y_FIRST, Y_MOST - Y_FIRST)], spill_hbm, out_sem.at[1])]
    for c in stores:
        c.start()
    for k in others:
        aux_copy(k).wait_send()
        for part in (0, 1):
            copy(k, part).wait_send()
    side_copy().wait()
    dispatch_done(slot_cap, xs, xs_hbm, row_out)
    for c in stores:
        c.wait()


def spread_kernel(slot_cap, dout_ref, across_ref, key_ref, gate_ref, us_hbm, gathered, us, row_send, row_recv, row_out):
    _, peers = find_peers()
    meet([peers[ACROSS_X], peers[CORE]])

    def copy(slot, part):
        if slot in (ACROSS_X, CORE):
            source, peer = dout_ref.at[part], slot
        elif slot in (ACROSS_XY, 2):
            source, peer = across_ref.at[part], ACROSS_X if slot == ACROSS_XY else CORE
        else:
            source, peer = gathered.at[slot - 2, part], CORE
        return pltpu.make_async_remote_copy(source, gathered.at[slot, part], row_send.at[slot, part],
                                            row_recv.at[slot, part], device_id=peers[peer], device_id_type=MESH)

    sent = [ACROSS_X, ACROSS_XY, CORE, 2, CORE + 1, 3]
    for slot in sent[:4]:
        for part in (0, 1):
            copy(slot, part).start()
    gathered[OWN] = dout_ref[...]
    gathered[ACROSS_Y] = across_ref[...]

    def relay(slot):
        for part in (0, 1):
            copy(slot, part).wait_recv()
            copy(slot + 2, part).start()

    def arrive(*slots):
        for slot in slots:
            for part in (0, 1):
                copy(slot, part).wait_recv()

    dispatch(slot_cap, gathered, key_ref, gate_ref, us, us_hbm, row_out,
             [lambda: relay(ACROSS_X), lambda: relay(ACROSS_XY), lambda: arrive(CORE, CORE + 1), lambda: arrive(2, 3)])
    for slot in sent:
        for part in (0, 1):
            copy(slot, part).wait_send()
    dispatch_done(slot_cap, us, us_hbm, row_out)


VMEM = pl.BlockSpec(memory_space=pltpu.VMEM)
ANY = pl.BlockSpec(memory_space=pl.ANY)
DMA = pltpu.SemaphoreType.DMA


def prologue_call(tokens, d_out, ids, gates, w1, w3, w2, slot_cap):
    num_top, tok_dev = ids.shape
    width, local, f = tokens.shape[2], w1.shape[0], w1.shape[2]
    rows, aux = 8 * slot_cap, (2 * num_top, tok_dev)
    large = [((local, rows, width), BF), ((Y_FIRST, width), F32), ((Y_MOST - Y_FIRST, width), F32)]
    small = [((8, local, tok_dev), F32)] * 2 + [((local, 2, rows // 2), F32)] * 2
    small += [((8,) + aux, F32), (tokens.shape, BF)]
    scratch = [((8,) + tokens.shape, BF), (aux, F32), ((8,) + aux, F32), large[0]]
    scratch += [((LEAD, width, 2 * f), BF), ((LEAD, f, width), BF), ((Y_MOST, width), F32)]
    return pl.pallas_call(
        functools.partial(prologue_kernel, slot_cap), name="prologue",
        in_specs=[VMEM] * 4 + [ANY] * 3,
        out_specs=[ANY] * len(large) + [VMEM] * len(small),
        out_shape=[jax.ShapeDtypeStruct(s, t) for s, t in large + small],
        scratch_shapes=[pltpu.VMEM(s, t) for s, t in scratch]
        + [DMA((8, 2)), DMA((8, 2)), DMA((8,)), DMA((8,)), DMA, DMA, DMA((3,)), DMA((2,)), DMA((4,))],
        compiler_params=pltpu.CompilerParams(collective_id=0, has_side_effects=True, vmem_limit_bytes=VMEM_LIMIT),
        cost_estimate=cost(10**10, 3 * 10**7),
    )(tokens, d_out, ids, gates, w1, w3, w2)


def spread_call(d_out, across, key, gate, slot_cap):
    local = key.shape[1]
    out = (local, 8 * slot_cap, d_out.shape[2])
    return pl.pallas_call(
        functools.partial(spread_kernel, slot_cap), name="spread",
        in_specs=[VMEM] * 4, out_specs=ANY, out_shape=jax.ShapeDtypeStruct(out, BF),
        scratch_shapes=[pltpu.VMEM((8,) + d_out.shape, BF), pltpu.VMEM(out, BF), DMA((8, 2)), DMA((8, 2)), DMA((4,))],
        compiler_params=pltpu.CompilerParams(collective_id=1, has_side_effects=True, vmem_limit_bytes=VMEM_LIMIT),
        cost_estimate=cost(10**10, 3 * 10**7),
    )(d_out, across, key, gate)


def solution(mesh):
    tp_size, ep_size = mesh.shape["tp"], mesh.shape["ep"]
    row_spec = P(("dp", "ep", "tp"), None)
    col_spec = P("ep", None, "tp")
    down_spec = P("ep", "tp", None)
    grad_col = P(("dp", "ep"), None, "tp")
    grad_down = P(("dp", "ep"), "tp", None)

    def swap(z, tp_bit, ep_bits):
        pairs = [(t * ep_size + e, (t ^ tp_bit) * ep_size + (e ^ ep_bits)) for t in range(tp_size) for e in range(ep_size)]
        return lax.ppermute(z, ("tp", "ep"), pairs)

    def local_step(tokens, expert_ids, gate_vals, w_one, w_three, w_two, d_out):
        tok_dev, width = tokens.shape
        num_top = expert_ids.shape[1]
        local = w_one.shape[0]
        experts = local * ep_size
        slot_cap = slot_count(num_top, tok_dev, experts)
        half = tp_size * ep_size * slot_cap // 2
        ep_here = lax.axis_index("ep")

        blocked = (2, tok_dev // 2, width)
        d_blocked = d_out.reshape(blocked)
        xs, y_other0, y_spill, key, gate, pack_y, pack_v, aux_all, across = prologue_call(
            tokens.reshape(blocked), d_blocked, expert_ids.T, gate_vals.T, w_one, w_three, w_two, slot_cap)
        y0 = swap(y_other0, 1, 0)
        rest = local - LEAD
        act_one, act_three, hid, y_other1, y_extra, y_mine = expert_call(
            fwd_kernel, 0, local, xs, w_one, w_three, w_two, pack_y, [], [y_spill],
            [F32, F32, BF], (USUAL - Y_FIRST, TOTAL - USUAL, TOTAL), (TOTAL - Y_FIRST,))
        y1 = swap(y_other1, 1, 0)
        across = lax.optimization_barrier((across, hid))[0]
        us = spread_call(d_blocked, across, key, gate, slot_cap)

        every = jnp.arange(experts, dtype=F32)[None, :, None]
        count_all = sum(jnp.sum(aux_all[:, j:j + 1, :] == every, axis=2, dtype=jnp.int32) for j in range(num_top))
        kept = jnp.minimum(count_all, slot_cap).reshape(2, ep_size, ep_size, local).sum(axis=1)
        lead_rows, rest_rows = kept[:, :, :LEAD].sum(axis=2), kept[:, :, LEAD:].sum(axis=2)
        v_rest = jnp.maximum(rest_rows, V_FIRST)
        most = jnp.maximum(jnp.maximum(lead_rows, Y_FIRST) + rest_rows, v_rest + lead_rows)
        more = jnp.any(most > USUAL)
        full = jnp.any((lead_rows > Y_MOST) | (rest_rows > V_MOST) | (most > TOTAL)
                       | (v_rest + lead_rows - kept[:, :, 0] > V_CUTS[3]) | (v_rest + kept[:, :, 1] > V_CUTS[2])
                       | (kept[:, :, LEAD:LEAD + 3].sum(axis=2) > V_FIRST))

        def after(value, *others):
            return lax.optimization_barrier((value,) + others)[0]

        def extra(rows):
            return lax.cond(more, lambda z: swap(z, 1, 0), lambda z: z, rows)

        saved = [act_one, act_three]
        spill = V_MOST - V_FIRST
        tail = TOTAL - V_FIRST
        one1, three1, v_other0, spill_other, v_mine0, spill_mine = expert_call(
            bwd_rest_kernel, LEAD, rest, us, w_one, w_three, w_two, pack_v, saved, [],
            [BF, BF], (V_FIRST, spill, V_FIRST, spill), (V_MOST, V_MOST))
        y2 = extra(after(y_extra, v_mine0))
        v0 = swap(after(v_other0, y2), 1, 0)
        one0, three0, v_other1, v_other2, v_other3, v_other4, v_extra, v_mine1, v_mine4 = expert_call(
            bwd_lead_kernel, 0, LEAD, us, w_one, w_three, w_two, pack_v, saved,
            [spill_other, spill_mine], [BF, BF],
            tuple(V_CUTS[n + 1] - V_CUTS[n] for n in range(5)) + (V_CUTS[3] - V_FIRST, TOTAL - V_CUTS[3]), (tail, tail))
        v1 = swap(v_other1, 1, 0)
        v2 = swap(v_other2, 1, 0)
        v3 = swap(v_other3, 1, 0)
        v4 = swap(v_other4, 1, 0)

        grads = grad_call(xs, us, hid, (one0, three0), (one1, three1))

        sources = jnp.stack([ep_here, ep_here ^ 2, ep_here ^ 1, ep_here ^ 3])
        all_ids = (sources[:, None] * local + jnp.arange(local)).reshape(-1)
        eq = expert_ids[:, :, None] == all_ids
        hit = jnp.any(eq, axis=1)
        lower = (jnp.arange(tok_dev)[:, None] > jnp.arange(tok_dev)[None, :]).astype(BF)
        pos = jnp.dot(lower, hit.astype(BF), preferred_element_type=F32)
        own_gate = jnp.sum(jnp.where(eq, gate_vals[:, :, None], 0.0), axis=1)
        own_pick = hit[:, :, None] & (pos[:, :, None] == jnp.arange(slot_cap, dtype=F32))
        own_mul = jnp.where(own_pick, own_gate[:, :, None], 0.0).reshape(tok_dev, ep_size, local, slot_cap)
        own_pick = own_pick.astype(BF).reshape(tok_dev, ep_size, local, slot_cap)

        def send_back(parts):
            back = [parts[0]]
            for n, bits in ((1, 2), (2, 1), (3, 3)):
                back.append(swap(parts[n], 0, bits))
            return back

        def choose(array, ids, axis):
            runs = []
            for e in ids:
                if runs and runs[-1][1] == e:
                    runs[-1][1] = e + 1
                else:
                    runs.append([e, e + 1])
            parts = [lax.slice_in_dim(array, *run, axis=axis) for run in runs]
            return parts[0] if len(parts) == 1 else jnp.concatenate(parts, axis=axis)

        def mix(weights, back, ids):
            flat = jnp.concatenate(back)
            weights = choose(weights, ids, 2).reshape(tok_dev, -1)
            if weights.dtype == BF:
                return jnp.dot(weights, flat, preferred_element_type=F32)
            return jnp.dot(weights, flat.astype(F32), precision=lax.Precision.HIGHEST)

        def column(pack):
            return pack[:, 1].reshape(local, ep_size, slot_cap).transpose(1, 0, 2).reshape(-1, 1)

        def finish(ids, keys, owns, pieces, recvs, known=(), early=(), steps=1):
            ranges, sizes = [], []
            for group in (ids, early):
                for owner in range(ep_size if group else 0):
                    ranges += [((owner * local + e) * slot_cap, (owner * local + e + 1) * slot_cap) for e in group]
                    sizes.append(len(group) * slot_cap)
            out = finish_call(owns, pieces, recvs, keys, tuple(ranges), known, sizes, steps)
            back = send_back(out[:ep_size])
            return back, out[ep_size:]

        y_back, _ = finish(range(local), column(pack_y), [y_mine],
                           [(0, 0, 0, Y_FIRST), (0, Y_FIRST, Y_FIRST, USUAL - Y_FIRST), (0, USUAL, USUAL, TOTAL - USUAL)],
                           [y0, y1, y2], steps=3)
        keys = column(pack_v)
        piece0 = [(0, 0, 0, V_FIRST)]
        late = [(0, V_CUTS[n] - V_FIRST, V_CUTS[n], V_CUTS[n + 1] - V_CUTS[n]) for n in range(3)]
        last = [(0, V_CUTS[n] - V_CUTS[3], V_CUTS[n], V_CUTS[n + 1] - V_CUTS[n]) for n in (3, 4)]
        whole0, whole1, whole2, whole3, whole4 = (3, 4, 5), (6, 7), (1,), (2,), (0,)
        back0, _ = finish(whole0, keys, [v_mine0], piece0, [v0])
        back1, _ = finish(whole1, keys, [after(v_mine0, back0[0]), v_mine1], piece0 + [(1,) + late[0][1:]], [v0, v1])
        y_back = after(tuple(y_back), back1[0])
        out_sum = mix(own_mul, y_back, range(local))
        back2, _ = finish(whole2, keys, [after(v_mine1, back1[0], out_sum)], late[:2], [v1, v2])
        v5 = extra(after(v_extra, back2[0]))
        back3, known = finish(whole3, keys, [after(v_mine1, back2[0], v5)], late, [v1, v2, v3], early=whole4)
        back4, _ = finish(whole4, keys, [after(v_mine4, back3[0])], last, [v4, v5], known=known)
        dx_early = mix(own_pick, after(tuple(back0), back4[0]), whole0)
        dx_early = dx_early + mix(own_pick, back1, whole1)
        dx_early = dx_early + mix(own_pick, back2, whole2)
        dx_early = mix(own_pick, back3, whole3) + dx_early
        dx_sum = mix(own_pick, after(tuple(back4), dx_early), whole4) + dx_early

        def exchange_all(args):
            hid, one0, one1, three0, three1, own_mul, own_pick = args
            d_one, d_three = jnp.concatenate([one0, one1]), jnp.concatenate([three0, three1])

            def back(part):
                recv = swap(part[:, :half], 1, 0)
                done = (part[:, half:] + recv).astype(BF).reshape(local, ep_size, slot_cap, width)
                return send_back([done[:, s].reshape(-1, width) for s in range(ep_size)])

            part_out = jnp.einsum("enf,efd->end", hid, w_two, preferred_element_type=F32)
            part_dx = jnp.einsum("enf,edf->end", d_one, w_one, preferred_element_type=F32)
            part_dx += jnp.einsum("enf,edf->end", d_three, w_three, preferred_element_type=F32)
            return mix(own_mul, back(part_out), range(local)), mix(own_pick, back(part_dx), range(local))

        def exchange_none(args):
            zero = jnp.zeros((tok_dev, width), F32)
            return zero, zero

        out_full, dx_full = lax.cond(full, exchange_all, exchange_none, (hid, one0, one1, three0, three1, own_mul, own_pick))
        out_rows = jnp.where(full, out_full, out_sum).astype(BF)
        dx_rows = jnp.where(full, dx_full, dx_sum).astype(BF)
        return out_rows, dx_rows, *grads

    return jax.shard_map(local_step, mesh=mesh,
                         in_specs=(row_spec, row_spec, row_spec, col_spec, col_spec, down_spec, row_spec),
                         out_specs=(row_spec, row_spec, grad_col, grad_col, grad_down), check_vma=False)
```
